32 devices in a mesh: gx: 4 (over y, x), gy: 4 (over z), gz: 2 (over core).
Axes of the slice: x: 2, y: 2, z: 4, core: 2. Of those that a mesh axis runs over, the one named last changes fastest.
Arguments:
- provisional: float32 [9, 128, 64, 256], P(None, 'gx', 'gy', 'gz'), may hold values from -6 to 6
- cut_flag: int32 [128, 64, 256], P('gx', 'gy', 'gz'), may hold values from 0 to 1, as said below
- cut_code: int32 [128, 64, 256], P('gx', 'gy', 'gz'), may hold values from 0 to 134217727
- volume_level: int32 [128, 64, 256], P('gx', 'gy', 'gz'), may hold values from 1 to 256
- area_level: int32 [128, 64, 256], P('gx', 'gy', 'gz'), may hold values from 64 to 256
Outputs:
- redistributed: float32 [9, 128, 64, 256], P(None, 'gx', 'gy', 'gz')
- species_change: float32 [9], replicated
The draws below stay inside these ranges and needn't reach their ends.
Inputs may be any that keep to these rules, and one draw needn't show every extreme that they name: cut_flag marks the cells crossed by one closed embedded surface.
All inputs are finite; a program needn't handle non-finite values.
Results may differ from the reference program's by a relative error of at most 0.00002.
Values sent between devices are 32-bit elements; how exact they have to be, the bound alone decides.
A program may use at most 128 MiB of HBM per device.

```python
import math
import jax
import jax.numpy as jnp
from jax import lax

NSPEC = 9
NX = 128
NY = 64
NZ = 256


def draw_cut_flag(key, part):
    keys = jax.random.split(jax.random.fold_in(key, 7), 2)
    centre = jax.random.randint(keys[0], (3,), -128, 129)
    radius = jax.random.randint(keys[1], (), 200, 360)
    coord_x = (2 * jnp.arange(NX, dtype=jnp.int32) + 1) * 512 // NX - 512 - centre[0]
    coord_y = (2 * jnp.arange(NY, dtype=jnp.int32) + 1) * 512 // NY - 512 - centre[1]
    coord_z = (2 * jnp.arange(NZ, dtype=jnp.int32) + 1) * 512 // NZ - 512 - centre[2]
    distance = coord_x[:, None, None] * coord_x[:, None, None] + coord_y[None, :, None] * coord_y[None, :, None] + coord_z[None, None, :] * coord_z[None, None, :]
    spacing = max(max(1024 // NX, 1024 // NY), max(1024 // NZ, 1))
    band_width = 2 * radius * spacing
    shell = jnp.abs(distance - radius * radius) <= band_width
    return shell.astype(jnp.int32)


def set_ends(drawn, stream_key, least, high):
    index_at = [jax.random.randint(jax.random.fold_in(stream_key, axis), (), 0, length) for axis, length in enumerate(drawn.shape)]
    main_axis = drawn.shape.index(max(drawn.shape))
    beside = index_at[:main_axis] + [(index_at[main_axis] + 1) % drawn.shape[main_axis]] + index_at[main_axis + 1:]
    return drawn.at[tuple(index_at)].set(least).at[tuple(beside)].set(high)


def levels(key, shape, pieces, least, high):
    level, own = 1.0, jax.random.fold_in(key, 6)
    for dim, parts in pieces:
        steps = jnp.exp(jax.random.uniform(jax.random.fold_in(own, dim), (parts,), jnp.float32, least / len(pieces), high / len(pieces)))
        level = level * jnp.repeat(steps, shape[dim] // parts).reshape([-1 if axis == dim else 1 for axis in range(len(shape))])
    return level


def gaussian(key, dims, deviation, reach, pieces=(), kind=jnp.bfloat16):
    array = deviation * jax.random.normal(key, dims, jnp.float32)
    if pieces:
        array = array * levels(key, dims, pieces, -0.22, 0.18)
    return jnp.clip(array, -reach, reach).astype(kind)


def setup_inputs(seed: int = 0) -> dict:
    arg_keys = jax.random.split(jax.random.key(seed), 6)
    return {
        "provisional": gaussian(arg_keys[0], (NSPEC, NX, NY, NZ), 1.0, 6.0, ((1, 4), (2, 4), (3, 2)), jnp.float32),
        "cut_flag": draw_cut_flag(jax.random.fold_in(arg_keys[5], 71), 0),
        "cut_code": set_ends(jax.random.randint(arg_keys[2], (NX, NY, NZ), 0, 134217728), jax.random.fold_in(arg_keys[2], 1), 0, 134217727).astype(jnp.int32),
        "volume_level": set_ends(jax.random.randint(arg_keys[3], (NX, NY, NZ), 1, 257), jax.random.fold_in(arg_keys[3], 1), 1, 256).astype(jnp.int32),
        "area_level": set_ends(jax.random.randint(arg_keys[4], (NX, NY, NZ), 64, 257), jax.random.fold_in(arg_keys[4], 1), 64, 256).astype(jnp.int32),
    }


CENTER = 8192
OFFSETS = [(a, b, c) for a in (-1, 0, 1) for b in (-1, 0, 1) for c in (-1, 0, 1)]

def window(values, a, b, c, margin, border):
    extent_x = values.shape[-3] - 2 * border + 2 * margin
    extent_y = values.shape[-2] - 2 * border + 2 * margin
    extent_z = values.shape[-1] - 2 * border + 2 * margin
    start_x = border - margin + a
    start_y = border - margin + b
    start_z = border - margin + c
    return values[..., start_x:start_x + extent_x, start_y:start_y + extent_y, start_z:start_z + extent_z]

def member(codes, position):
    return (codes >> position & 1).astype(jnp.float32)

def reference(provisional, cut_flag, cut_code, volume_level, area_level):
    is_cut = cut_flag == 1
    codes = jnp.where(is_cut, cut_code | CENTER, CENTER)
    volume_frac = jnp.where(is_cut, volume_level, 256).astype(jnp.float32) / 256.0
    face_frac = jnp.where(is_cut, area_level, 256).astype(jnp.float32) / 256.0
    code_pad = jnp.pad(codes, 1) | CENTER
    counted = jnp.zeros(codes.shape, jnp.float32)
    for position, (a, b, c) in enumerate(OFFSETS):
        counted = counted + member(window(code_pad, -a, -b, -c, 0, 1), position)
    weights = volume_frac / counted
    portions = volume_frac * face_frac / counted
    portion_pad = jnp.pad(portions, 1)
    gathered = jnp.zeros(codes.shape, jnp.float32)
    for position, (a, b, c) in enumerate(OFFSETS):
        gathered = gathered + member(codes, position) * window(portion_pad, a, b, c, 0, 1)
    scaling = face_frac / counted

    def spread_species(values):
        carried = jnp.pad(weights * values, 1)
        amounts = jnp.zeros(codes.shape, jnp.float32)
        for position, (a, b, c) in enumerate(OFFSETS):
            amounts = amounts + member(codes, position) * window(carried, a, b, c, 0, 1)
        quotas = jnp.pad(amounts / gathered, 1)
        summed = jnp.zeros(codes.shape, jnp.float32)
        for position, (a, b, c) in enumerate(OFFSETS):
            summed = summed + member(window(code_pad, -a, -b, -c, 0, 1), position) * window(quotas, -a, -b, -c, 0, 1)
        return scaling * summed
    redistributed = lax.map(spread_species, provisional)
    species_change = lax.optimization_barrier(jnp.sum(volume_frac[None] * redistributed, axis=(1, 2, 3))) / math.sqrt(NX * NY * NZ)
    return (redistributed, species_change)
```

```python
import functools
import math

import jax
import jax.numpy as jnp
from jax import lax
from jax.experimental import pallas as pl
from jax.experimental.pallas import tpu as pltpu
from jax.sharding import PartitionSpec as P

CENTER = 8192
BLOCK = [(a, b, 9 * (a + 1) + 3 * (b + 1)) for a in (-1, 0, 1) for b in (-1, 0, 1)]
AXES = ("gx", "gy", "gz")
WAYS = [(1, 0), (-1, 0), (0, 1), (0, -1), (1, 1), (1, -1), (-1, 1), (-1, -1)]
MESH = pl.DeviceIdType.MESH
LANES = 128
TILE = 8


def pipelined(stages, count, hook=None):
    depth = len(stages)

    def step(i, lowest, highest):
        for k in reversed(range(lowest, highest)):
            stages[k](i - k)

    for i in range(min(depth - 1, count)):
        step(i, 0, i + 1)

    def body(i, carry):
        if hook is not None:
            at, action = hook
            pl.when(i == at)(action)
        step(i, 0, depth)
        return carry

    lax.fori_loop(depth - 1, count, body, 0)
    for i in range(count, count + depth - 1):
        step(i, i - count + 1, depth)


def kernel(
    nx, ny, scale,
    prov_h, flag_h, code_h, vol_h, area_h,
    out_h, change,
    prov, flag, code, vol, area, out,
    codes, wbuf, qbuf, shifted, edge,
    zs_i, zl_i, zr_i, zs_f, zl_f, zr_f,
    ys_i, yr_i, cs_i, cr_i, ys_w, yr_w, cs_w, cr_w, ys_q, yr_q, cs_q, cr_q,
    weights, scaling, ends, parts_i, parts_f, peers,
    load, store, z_send, z_recv, send, recv, peer_send, peer_recv,
):
    nspec = prov.shape[0]
    pitch = ny + TILE
    tiles = ny // TILE
    count = nx * tiles
    here = {axis: lax.axis_index(axis) for axis in AXES}
    size = {axis: lax.axis_size(axis) for axis in AXES}
    lane = lax.broadcasted_iota(jnp.int32, (TILE, LANES), 1)
    odd = (lane & 1) == 1
    first_lane = lane == 0
    last_lane = lane == LANES - 1
    both_ends = first_lane | last_lane
    cut = nspec // 2
    flux = cut
    fields = nspec + 1
    group_a, group_b = list(range(cut)), list(range(cut, nspec))

    inputs = [(flag_h, flag), (code_h, code), (vol_h, vol), (area_h, area), (prov_h, prov)]
    loads = [pltpu.make_async_copy(src, dst, load.at[k]) for k, (src, dst) in enumerate(inputs)]
    for copy in loads:
        copy.start()

    def moved(axis, step):
        return lax.rem(here[axis] + (step + size[axis]), size[axis])

    barrier = pltpu.get_barrier_semaphore()
    others = set()
    for dx, dy in WAYS:
        others.add((dx % size["gx"], dy % size["gy"], 0))
    for number, axis in enumerate(AXES):
        for k in range(1, size[axis]):
            others.add(tuple(k if i == number else 0 for i in range(3)))
    others.discard((0, 0, 0))
    for shift in sorted(others):
        pl.semaphore_signal(
            barrier, inc=1,
            device_id={axis: lax.rem(here[axis] + shift[i], size[axis]) for i, axis in enumerate(AXES)},
            device_id_type=MESH,
        )

    def first(x):
        return TILE + x * pitch

    def own_tile(t):
        row = TILE + (t // tiles + 1) * pitch + lax.rem(t, tiles) * TILE
        return pl.multiple_of(row, TILE), pl.multiple_of(t * TILE, TILE)

    def side(axis, step):
        return here[axis] < size[axis] - 1 if step > 0 else here[axis] > 0

    def exists(dx, dy):
        found = None
        for axis, step in (("gx", dx), ("gy", dy)):
            if step:
                there = side(axis, step)
                found = there if found is None else jnp.logical_and(found, there)
        return found

    below_z, above_z = side("gz", -1), side("gz", 1)

    def edge_row(step):
        return ny - 1 if step > 0 else 0

    def halo_row(step):
        return ny if step > 0 else -1

    def blank(buf, low, high):
        zeros = jnp.zeros((ny, LANES), buf.dtype)
        row_zeros = jnp.zeros((TILE, LANES), buf.dtype)
        one = jnp.zeros((1, LANES), buf.dtype)

        def plane(step):
            def body(f, carry):
                buf[f, pl.ds(first(nx + 1 if step > 0 else 0), ny), :] = zeros
                return carry
            lax.fori_loop(low, high, body, 0)

        def row(step):
            def body(f, carry):
                for x in range(0, nx, TILE):
                    buf[f, pl.ds(first(x + 1) + halo_row(step), TILE, stride=pitch), :] = row_zeros
                return carry
            lax.fori_loop(low, high, body, 0)

        def corner(dx, dy):
            def body(f, carry):
                buf[f, pl.ds(first(nx + 1 if dx > 0 else 0) + halo_row(dy), 1), :] = one
                return carry
            lax.fori_loop(low, high, body, 0)

        for dx, dy in WAYS:
            action = functools.partial(plane, dx) if dy == 0 else (
                functools.partial(row, dy) if dx == 0 else functools.partial(corner, dx, dy))
            pl.when(jnp.logical_not(exists(dx, dy)))(action)

    class Unit:
        def __init__(self, number, buf, low, high, ys, yr, cs, cr, corner):
            self.buf, self.low, self.high = buf, low, high
            self.ys, self.yr, self.cs, self.cr, self.corner = ys, yr, cs, cr, corner
            n = high - low
            ends_of = {1: (nx, 0), -1: (1, nx + 1)}
            self.copies = []
            for k, (dx, dy) in enumerate(WAYS):
                if dy == 0:
                    here_x, there_x = ends_of[dx]
                    source = buf.at[pl.ds(low, n), pl.ds(first(here_x), ny), :]
                    landing = buf.at[pl.ds(low, n), pl.ds(first(there_x), ny), :]
                elif dx == 0:
                    way = 0 if dy > 0 else 1
                    source, landing = ys.at[way, pl.ds(low, n)], yr.at[way, pl.ds(low, n)]
                else:
                    source, landing = cs.at[corner, k - 4], cr.at[corner, k - 4]
                self.copies.append(
                    pltpu.make_async_remote_copy(
                        src_ref=source, dst_ref=landing,
                        send_sem=send.at[number, k], recv_sem=recv.at[number, k],
                        device_id={"gx": moved("gx", dx), "gy": moved("gy", dy)}, device_id_type=MESH,
                    )
                )

        def start(self):
            buf = self.buf
            for k, (dx, dy) in enumerate(WAYS):
                if dy == 0:
                    pl.when(exists(dx, dy))(self.copies[k].start)

            def gather(f, carry):
                for x in range(0, nx, TILE):
                    for way, step in ((0, 1), (1, -1)):
                        self.ys[way, f, pl.ds(x, TILE), :] = buf[f, pl.ds(first(x + 1) + edge_row(step), TILE, stride=pitch), :]
                for k, (dx, dy) in enumerate(WAYS[4:]):
                    row = first(nx if dx > 0 else 1) + edge_row(dy)
                    self.cs[self.corner, k, pl.ds(f - self.low, 1), :] = buf[f, pl.ds(row, 1), :]
                return carry

            lax.fori_loop(self.low, self.high, gather, 0)
            for k, (dx, dy) in enumerate(WAYS):
                if dy != 0:
                    pl.when(exists(dx, dy))(self.copies[k].start)

        def receive(self):
            buf = self.buf
            for k, (dx, dy) in enumerate(WAYS):
                pl.when(exists(-dx, -dy))(self.copies[k].wait_recv)

            def rows(way, step):
                def body(f, carry):
                    for x in range(0, nx, TILE):
                        buf[f, pl.ds(first(x + 1) + halo_row(-step), TILE, stride=pitch), :] = self.yr[way, f, pl.ds(x, TILE), :]
                    return carry
                lax.fori_loop(self.low, self.high, body, 0)

            def corner(k, dx, dy):
                def body(f, carry):
                    row = first(0 if dx > 0 else nx + 1) + halo_row(-dy)
                    buf[f, pl.ds(row, 1), :] = self.cr[self.corner, k, pl.ds(f - self.low, 1), :]
                    return carry
                lax.fori_loop(self.low, self.high, body, 0)

            for way, step in ((0, 1), (1, -1)):
                pl.when(exists(0, -step))(functools.partial(rows, way, step))
            for k, (dx, dy) in enumerate(WAYS[4:]):
                pl.when(exists(-dx, -dy))(functools.partial(corner, k, dx, dy))

        def finish(self):
            for k, (dx, dy) in enumerate(WAYS):
                pl.when(exists(dx, dy))(self.copies[k].wait_send)

    class Depth:
        def __init__(self, number, zs, zl, zr, buf, plane):
            self.zl, self.zr, self.buf, self.plane = zl, zr, buf, plane
            self.copies = [
                pltpu.make_async_remote_copy(
                    src_ref=zs, dst_ref=landing,
                    send_sem=z_send.at[number, way], recv_sem=z_recv.at[number, way],
                    device_id={"gz": moved("gz", step)}, device_id_type=MESH,
                )
                for way, (landing, step) in enumerate(((zl, 1), (zr, -1)))
            ]

        def start(self):
            pl.when(above_z)(self.copies[0].start)
            pl.when(below_z)(self.copies[1].start)

        def receive(self):
            pl.when(below_z)(self.copies[0].wait_recv)
            pl.when(above_z)(self.copies[1].wait_recv)
            zero = jnp.zeros((TILE, LANES), self.buf.dtype)

            def place(t, carry):
                row, at = own_tile(t)
                low = jnp.where(below_z, self.zl[pl.ds(at, TILE), :], zero)
                high = jnp.where(above_z, self.zr[pl.ds(at, TILE), :], zero)
                self.buf[self.plane, pl.ds(row, TILE), :] = jnp.where(odd, low, high)
                return carry

            lax.fori_loop(0, count, place, 0, unroll=8)

        def finish(self):
            pl.when(above_z)(self.copies[0].wait_send)
            pl.when(below_z)(self.copies[1].wait_send)

    code_z = Depth(0, zs_i, zl_i, zr_i, codes, 1)
    code_own = Unit(0, codes, 0, 1, ys_i, yr_i, cs_i, cr_i, 0)
    code_packed = Unit(1, codes, 1, 2, ys_i, yr_i, cs_i, cr_i, 1)
    w_z = Depth(1, zs_f.at[0], zl_f.at[0], zr_f.at[0], wbuf, fields)
    w_a = Unit(2, wbuf, 0, cut + 1, ys_w, yr_w, cs_w, cr_w, 0)
    w_b = Unit(3, wbuf, cut + 1, fields, ys_w, yr_w, cs_w, cr_w, 1)
    w_packed = Unit(4, wbuf, fields, fields + 1, ys_w, yr_w, cs_w, cr_w, 2)
    qa_z = Depth(2, zs_f.at[1], zl_f.at[1], zr_f.at[1], qbuf, nspec)
    q_a = Unit(5, qbuf, 0, cut, ys_q, yr_q, cs_q, cr_q, 0)
    qa_packed = Unit(6, qbuf, nspec, nspec + 1, ys_q, yr_q, cs_q, cr_q, 1)
    qb_z = Depth(3, zs_f.at[2], zl_f.at[2], zr_f.at[2], qbuf, nspec + 1)
    q_b = Unit(7, qbuf, cut, nspec, ys_q, yr_q, cs_q, cr_q, 2)
    qb_packed = Unit(8, qbuf, nspec + 1, nspec + 2, ys_q, yr_q, cs_q, cr_q, 3)
    everything = [code_z, code_own, code_packed, w_z, w_a, w_b, w_packed, qa_z, q_a, qa_packed, qb_z, q_b, qb_packed]

    def peer_copies(axis):
        number = AXES.index(axis)
        return [
            pltpu.make_async_remote_copy(
                src_ref=peers.at[number, here[axis]], dst_ref=peers.at[number, here[axis]],
                send_sem=peer_send.at[number, k], recv_sem=peer_recv.at[number, k],
                device_id={axis: lax.rem(here[axis] + k, size[axis])}, device_id_type=MESH,
            )
            for k in range(1, size[axis])
        ]

    def reduce_start(axis, value):
        peers[AXES.index(axis), here[axis]] = value
        for copy in peer_copies(axis):
            copy.start()

    def reduce_finish(axis):
        number = AXES.index(axis)
        for copy in peer_copies(axis):
            copy.wait()
        value = peers[number, 0]
        for k in range(1, size[axis]):
            value = value + peers[number, k]
        return value

    def fractions(own):
        is_cut = flag[own, :] == 1
        volume = jnp.where(is_cut, vol[own, :], 256).astype(jnp.float32) * (1.0 / 256.0)
        face = jnp.where(is_cut, area[own, :], 256).astype(jnp.float32) * (1.0 / 256.0)
        return volume, face

    def fill(t, carry):
        row, at = own_tile(t)
        own = pl.ds(at, TILE)
        value = jnp.where(flag[own, :] == 1, code[own, :] | CENTER, CENTER)
        codes[0, pl.ds(row, TILE), :] = value
        shifted[0, own, :] = jnp.where(first_lane, 0, pltpu.roll(value, 1, 1))
        shifted[1, own, :] = jnp.where(last_lane, 0, pltpu.roll(value, LANES - 1, 1))
        low = jnp.broadcast_to(value[:, :1], (TILE, LANES))
        high = lax.shift_right_logical(jnp.broadcast_to(value[:, LANES - 1:], (TILE, LANES)), 2)
        zs_i[own, :] = jnp.where(odd, high, low)
        edge[own, :] = jnp.where(odd, low, high)
        return carry

    def add_up(t, totals):
        _, at = own_tile(t)
        own = pl.ds(at, TILE)
        volume, _ = fractions(own)
        return tuple(totals[s] + volume * prov[s, own, :] for s in range(nspec))

    def taps(row, step, left, middle, right, buf, low, high):
        zero = jnp.zeros((TILE, LANES), jnp.float32)
        sums = [[None] * (high - low) for _ in range(3)]
        for a, b, position in BLOCK:
            near = pl.ds(row + step * (a * pitch + b), TILE)
            present = []
            for k, source in enumerate((left, middle, right)):
                if step > 0 and position + k == 13:
                    present.append(None)
                else:
                    present.append((source(near) & (1 << (position + k))) != 0)
            for f in range(low, high):
                value = buf[f, near, :]
                for k in range(3):
                    term = value if present[k] is None else jnp.where(present[k], value, zero)
                    old = sums[k][f - low]
                    sums[k][f - low] = term if old is None else old + term
        return sums

    def packed_taps(row, step, source, buf, plane):
        zero = jnp.zeros((TILE, LANES), jnp.float32)
        total = None
        for a, b, position in BLOCK:
            near = pl.ds(row + step * (a * pitch + b), TILE)
            term = jnp.where((source(near) & (1 << position)) != 0, buf[plane, near, :], zero)
            total = term if total is None else total + term
        return total

    def pack(values, lowest):
        packed = jnp.zeros((TILE, LANES), jnp.float32)
        for k, value in enumerate(values):
            f = lowest + k
            start = value if f == 0 else pltpu.roll(value, 2 * f, 1)
            packed = jnp.where(lane == 2 * f, start, packed)
            packed = jnp.where(lane == 2 * f + 1, pltpu.roll(value, 2 * f + 2, 1), packed)
        return packed

    quad = 4

    def count_taps(g):
        for k in range(quad):
            row, at = own_tile(g * quad + k)
            sums = [None] * 3
            total = None
            for a, b, position in BLOCK:
                near = pl.ds(row - a * pitch - b, TILE)
                value = codes[0, near, :]
                value = value if position == 0 else lax.shift_right_logical(value, position)
                for m in range(3):
                    term = value & (1 << m)
                    sums[m] = term if sums[m] is None else sums[m] + term
                value = codes[1, near, :]
                value = value if position == 0 else lax.shift_right_logical(value, position)
                total = value & 1 if total is None else total + (value & 1)
            for m in range(3):
                parts_i[k, m] = sums[m]
            parts_i[k, 3] = total

    def weigh(g):
        for k in range(quad):
            row, at = own_tile(g * quad + k)
            own = pl.ds(at, TILE)
            from_end = pltpu.roll(parts_i[k, 3], LANES - 1, 1)
            from_left = pltpu.roll(lax.shift_right_logical(parts_i[k, 2], 2), 1, 1)
            from_right = pltpu.roll(parts_i[k, 0], LANES - 1, 1)
            counted = lax.shift_right_logical(parts_i[k, 1], 1)
            counted = counted + jnp.where(first_lane, from_end, from_left) + jnp.where(last_lane, from_end, from_right)
            volume, face = fractions(own)
            share = 1.0 / counted.astype(jnp.float32)
            scaling[own, :] = face * share
            weight = volume * share
            for s in range(nspec):
                f = s if s < cut else s + 1
                wbuf[f, pl.ds(row, TILE), :] = weight * prov[s, own, :]
            wbuf[flux, pl.ds(row, TILE), :] = weight * face

    def weigh_pack(g):
        for k in range(quad):
            row, at = own_tile(g * quad + k)
            zs_f[0, pl.ds(at, TILE), :] = pack([wbuf[f, pl.ds(row, TILE), :] for f in range(fields)], 0)

    def quota_stages(low, high, with_ends):
        n = high - low
        base = low if low == 0 else low - 1

        def main(x):
            for k in range(tiles):
                row, at = own_tile(x * tiles + k)
                own = pl.ds(at, TILE)
                right, left, middle = shifted[0, own, :], shifted[1, own, :], codes[0, pl.ds(row, TILE), :]
                sums = taps(row, 1, lambda near: left, lambda near: middle, lambda near: right, wbuf, low, high)
                for m in range(3):
                    for f in range(n):
                        parts_f[k, m, f] = sums[m][f]
                if with_ends:
                    value = edge[own, :]
                    ends[own, :] = packed_taps(row, 1, lambda near: value, wbuf, fields)

        def close(x):
            for k in range(tiles):
                row, at = own_tile(x * tiles + k)
                own = pl.ds(at, TILE)
                packed = ends[own, :]
                found = []
                for f in range(n):
                    spread = pltpu.roll(packed, LANES - 1 - 2 * (low + f), 1)
                    total = parts_f[k, 1, f] + pltpu.roll(parts_f[k, 2, f], LANES - 1, 1)
                    total = total + pltpu.roll(parts_f[k, 0, f], 1, 1)
                    found.append(total + jnp.where(both_ends, spread, 0.0))
                if with_ends:
                    inverted = 1.0 / found[flux]
                    weights[own, :] = inverted
                    found = found[:flux]
                else:
                    inverted = weights[own, :]
                for f, value in enumerate(found):
                    qbuf[base + f, pl.ds(row, TILE), :] = value * inverted

        def send_pack(x):
            for k in range(tiles):
                row, at = own_tile(x * tiles + k)
                group = group_a if with_ends else group_b
                zs_f[1 if with_ends else 2, pl.ds(at, TILE), :] = pack([qbuf[s, pl.ds(row, TILE), :] for s in group], 0)

        return [main, close, send_pack]

    def scatter_stages(group, plane):
        n = len(group)
        low = group[0]

        def main(x):
            for k in range(tiles):
                row, at = own_tile(x * tiles + k)
                own_code = {}

                def source(near):
                    return codes[0, near, :]

                sums = taps(row, -1, source, source, source, qbuf, low, low + n)
                for m in range(3):
                    for f in range(n):
                        parts_f[k, m, f] = sums[m][f]
                parts_f[k, 0, n] = packed_taps(row, -1, lambda near: codes[1, near, :], qbuf, plane)

        def close(x):
            for k in range(tiles):
                row, at = own_tile(x * tiles + k)
                own = pl.ds(at, TILE)
                packed = parts_f[k, 0, n]
                factor = scaling[own, :]
                for f, s in enumerate(group):
                    spread = pltpu.roll(packed, LANES - 1 - 2 * f, 1)
                    total = parts_f[k, 1, f]
                    total = total + jnp.where(first_lane, spread, pltpu.roll(parts_f[k, 2, f], 1, 1))
                    total = total + jnp.where(last_lane, spread, pltpu.roll(parts_f[k, 0, f], LANES - 1, 1))
                    out[s, own, :] = factor * total

        return [main, close]

    blank(codes, 0, 2)
    blank(wbuf, 0, fields + 1)
    blank(qbuf, 0, nspec + 2)
    loads[0].wait()
    loads[1].wait()
    lax.fori_loop(0, count, fill, 0, unroll=8)
    pl.semaphore_wait(barrier, len(others))
    code_z.start()
    code_own.start()
    for copy in loads[2:]:
        copy.wait()
    totals = tuple(jnp.zeros((TILE, LANES), jnp.float32) for _ in range(nspec))
    totals = lax.fori_loop(0, count // 8 * 4, add_up, totals, unroll=4)
    code_z.receive()
    code_packed.start()
    totals = lax.fori_loop(count // 8 * 4, count, add_up, totals, unroll=4)
    local = jnp.concatenate(
        [jnp.sum(total, axis=0, keepdims=True) for total in totals]
        + [jnp.zeros((peers.shape[2] - nspec, LANES), jnp.float32)],
        axis=0,
    )
    reduce_start("gx", local)
    code_own.receive()
    code_packed.receive()
    pipelined([count_taps, weigh, weigh_pack], count // quad)
    w_z.start()
    w_a.start()
    w_b.start()
    reduce_start("gy", reduce_finish("gx"))
    w_z.receive()
    w_packed.start()
    w_a.receive()
    w_packed.receive()
    pipelined(quota_stages(0, cut + 1, True), nx)
    qa_z.start()
    q_a.start()
    w_b.receive()
    reduce_start("gz", reduce_finish("gy"))

    def middle_a():
        qa_z.receive()
        qa_packed.start()

    pipelined(quota_stages(cut + 1, fields, False), nx, (nx // 3, middle_a))
    qb_z.start()
    q_b.start()
    summed = reduce_finish("gz")
    change[...] = jnp.broadcast_to(jnp.sum(summed, axis=1, keepdims=True) * scale, change.shape)
    q_a.receive()
    qa_packed.receive()

    def middle_b():
        qb_z.receive()
        qb_packed.start()

    pipelined(scatter_stages(group_a, nspec), nx, (nx // 3, middle_b))
    save_a = pltpu.make_async_copy(out.at[pl.ds(0, cut)], out_h.at[pl.ds(0, cut)], store.at[0])
    save_a.start()
    q_b.receive()
    qb_packed.receive()
    pipelined(scatter_stages(group_b, nspec + 1), nx)
    save_b = pltpu.make_async_copy(out.at[pl.ds(cut, nspec - cut)], out_h.at[pl.ds(cut, nspec - cut)], store.at[1])
    save_b.start()
    for part in everything:
        part.finish()
    save_a.wait()
    save_b.wait()


def per_device(provisional, cut_flag, cut_code, volume_level, area_level):
    nspec, nx, ny, nz = provisional.shape
    assert nz == LANES and ny % TILE == 0 and nx % TILE == 0
    own = nx * ny
    tiles = ny // TILE
    rows = TILE + (nx + 2) * (ny + TILE)
    most = max(lax.axis_size(axis) for axis in AXES)
    cells = own * nz * math.prod(lax.axis_size(axis) for axis in AXES)
    high = -(-nspec // TILE) * TILE
    cut = nspec // 2
    fields = nspec + 1
    group = max(cut + 1, nspec - cut)
    wide = -(-group // TILE) * TILE
    f32, i32 = jnp.float32, jnp.int32
    vmem = pl.BlockSpec(memory_space=pltpu.VMEM)
    hbm = pl.BlockSpec(memory_space=pl.ANY)
    shapes = [
        ((nspec, own, nz), f32), ((own, nz), i32), ((own, nz), i32), ((own, nz), i32), ((own, nz), i32),
        ((nspec, own, nz), f32),
        ((2, rows, nz), i32), ((fields + 1, rows, nz), f32), ((nspec + 2, rows, nz), f32),
        ((2, own, nz), i32), ((own, nz), i32),
        ((own, nz), i32), ((own, nz), i32), ((own, nz), i32),
        ((3, own, nz), f32), ((3, own, nz), f32), ((3, own, nz), f32),
        ((2, 2, nx, nz), i32), ((2, 2, nx, nz), i32), ((2, 4, TILE, nz), i32), ((2, 4, TILE, nz), i32),
        ((2, fields + 1, nx, nz), f32), ((2, fields + 1, nx, nz), f32), ((3, 4, wide, nz), f32), ((3, 4, wide, nz), f32),
        ((2, nspec + 2, nx, nz), f32), ((2, nspec + 2, nx, nz), f32), ((4, 4, wide, nz), f32), ((4, 4, wide, nz), f32),
        ((own, nz), f32), ((own, nz), f32), ((own, nz), f32),
        ((4, 4, TILE, nz), i32), ((tiles, 3, group + 1, TILE, nz), f32),
        ((3, most, high, nz), f32),
    ]
    dma = pltpu.SemaphoreType.DMA
    out, change = pl.pallas_call(
        functools.partial(kernel, nx, ny, 1.0 / math.sqrt(cells)),
        out_shape=(
            jax.ShapeDtypeStruct((nspec, own, nz), f32),
            jax.ShapeDtypeStruct((high, nz), f32),
        ),
        in_specs=[hbm] * 5,
        out_specs=(hbm, vmem),
        scratch_shapes=[pltpu.VMEM(shape, kind) for shape, kind in shapes]
        + [
            dma((5,)), dma((2,)), dma((4, 2)), dma((4, 2)), dma((9, 8)), dma((9, 8)), dma((3, most)), dma((3, most)),
        ],
        compiler_params=pltpu.CompilerParams(
            collective_id=0, has_side_effects=True, vmem_limit_bytes=60 * 1024 * 1024
        ),
    )(
        provisional.reshape(nspec, own, nz),
        cut_flag.reshape(own, nz),
        cut_code.reshape(own, nz),
        volume_level.reshape(own, nz),
        area_level.reshape(own, nz),
    )
    return out.reshape(provisional.shape), change[:nspec, 0]


def solution(mesh):
    spec = P("gx", "gy", "gz")
    wide = P(None, "gx", "gy", "gz")
    return jax.shard_map(
        per_device, mesh=mesh, in_specs=(wide, spec, spec, spec, spec), out_specs=(wide, P()), check_vma=False
    )
```

```python
import functools
import math

import jax
import jax.numpy as jnp
from jax import lax
from jax.experimental import pallas as pl
from jax.experimental.pallas import tpu as pltpu
from jax.sharding import PartitionSpec as P

CENTER = 8192
BLOCK = [(a, b, 9 * (a + 1) + 3 * (b + 1)) for a in (-1, 0, 1) for b in (-1, 0, 1)]
AXES = ("gx", "gy", "gz")
WAYS = [(1, 0), (-1, 0), (0, 1), (0, -1), (1, 1), (1, -1), (-1, 1), (-1, -1)]
MESH = pl.DeviceIdType.MESH
LANES = 128
TILE = 8


def pipelined(stages, count, hook=None):
    depth = len(stages)

    def step(i, lowest, highest):
        for k in reversed(range(lowest, highest)):
            stages[k](i - k)

    for i in range(min(depth - 1, count)):
        step(i, 0, i + 1)

    def body(i, carry):
        step(i, 0, depth)
        return carry

    low = depth - 1
    if hook is not None:
        at, action = hook
        lax.fori_loop(low, at, body, 0)
        action()
        low = at
    lax.fori_loop(low, count, body, 0)
    for i in range(count, count + depth - 1):
        step(i, i - count + 1, depth)


def kernel(
    nx, ny, scale,
    prov_h, flag_h, code_h, vol_h, area_h,
    out, change,
    prov, flag, code, vol, area,
    codes, wbuf, qbuf, shifted, edge,
    zs_i, zl_i, zr_i, zs_f, zl_f, zr_f,
    ys_i, yr_i, cs_i, cr_i, ys_w, yr_w, cs_w, cr_w, ys_q, yr_q, cs_q, cr_q,
    weights, scaling, ends, parts_i, parts_f, peers,
    load, z_send, z_recv, send, recv, peer_send, peer_recv,
):
    nspec = prov.shape[0]
    pitch = ny + TILE
    tiles = ny // TILE
    here = {axis: lax.axis_index(axis) for axis in AXES}
    size = {axis: lax.axis_size(axis) for axis in AXES}
    lane = lax.broadcasted_iota(jnp.int32, (TILE, LANES), 1)
    odd = (lane & 1) == 1
    first_lane = lane == 0
    last_lane = lane == LANES - 1
    both_ends = first_lane | last_lane
    cut = nspec // 2
    flux = cut
    fields = nspec + 1
    group_a, group_b = list(range(cut)), list(range(cut, nspec))

    inputs = [(flag_h, flag), (code_h, code), (vol_h, vol), (area_h, area), (prov_h, prov)]
    loads = [pltpu.make_async_copy(src, dst, load.at[k]) for k, (src, dst) in enumerate(inputs)]
    for copy in loads:
        copy.start()

    def moved(axis, step):
        return lax.rem(here[axis] + (step + size[axis]), size[axis])

    barrier = pltpu.get_barrier_semaphore()
    others = set()
    for dx, dy in WAYS:
        others.add((dx % size["gx"], dy % size["gy"], 0))
    for number, axis in enumerate(AXES):
        for k in range(1, size[axis]):
            others.add(tuple(k if i == number else 0 for i in range(3)))
    others.discard((0, 0, 0))
    for shift in sorted(others):
        pl.semaphore_signal(
            barrier, inc=1,
            device_id={axis: lax.rem(here[axis] + shift[i], size[axis]) for i, axis in enumerate(AXES)},
            device_id_type=MESH,
        )

    def first(x):
        return TILE + x * pitch

    def own_tile(x, k):
        row = (TILE + pitch + k * TILE) + x * pitch
        at = x * ny + k * TILE
        if isinstance(x, int):
            return row, at
        return pl.multiple_of(row, TILE), pl.multiple_of(at, TILE)

    def side(axis, step):
        return here[axis] < size[axis] - 1 if step > 0 else here[axis] > 0

    def exists(dx, dy):
        found = None
        for axis, step in (("gx", dx), ("gy", dy)):
            if step:
                there = side(axis, step)
                found = there if found is None else jnp.logical_and(found, there)
        return found

    below_z, above_z = side("gz", -1), side("gz", 1)

    def edge_row(step):
        return ny - 1 if step > 0 else 0

    def halo_row(step):
        return ny if step > 0 else -1

    def blank(buf, low, high):
        zeros = jnp.zeros((ny, LANES), buf.dtype)
        row_zeros = jnp.zeros((TILE, LANES), buf.dtype)
        one = jnp.zeros((1, LANES), buf.dtype)

        def plane(step):
            def body(f, carry):
                buf[f, pl.ds(first(nx + 1 if step > 0 else 0), ny), :] = zeros
                return carry
            lax.fori_loop(low, high, body, 0)

        def row(step):
            def body(f, carry):
                for x in range(0, nx, TILE):
                    buf[f, pl.ds(first(x + 1) + halo_row(step), TILE, stride=pitch), :] = row_zeros
                return carry
            lax.fori_loop(low, high, body, 0)

        def corner(dx, dy):
            def body(f, carry):
                buf[f, pl.ds(first(nx + 1 if dx > 0 else 0) + halo_row(dy), 1), :] = one
                return carry
            lax.fori_loop(low, high, body, 0)

        for dx, dy in WAYS:
            action = functools.partial(plane, dx) if dy == 0 else (
                functools.partial(row, dy) if dx == 0 else functools.partial(corner, dx, dy))
            pl.when(jnp.logical_not(exists(dx, dy)))(action)

    class Unit:
        def __init__(self, number, buf, low, high, ys, yr, cs, cr, corner):
            self.buf, self.low, self.high = buf, low, high
            self.ys, self.yr, self.cs, self.cr, self.corner = ys, yr, cs, cr, corner
            n = high - low
            ends_of = {1: (nx, 0), -1: (1, nx + 1)}
            self.copies = []
            for k, (dx, dy) in enumerate(WAYS):
                if dy == 0:
                    here_x, there_x = ends_of[dx]
                    source = buf.at[pl.ds(low, n), pl.ds(first(here_x), ny), :]
                    landing = buf.at[pl.ds(low, n), pl.ds(first(there_x), ny), :]
                elif dx == 0:
                    way = 0 if dy > 0 else 1
                    source, landing = ys.at[way, pl.ds(low, n)], yr.at[way, pl.ds(low, n)]
                else:
                    source, landing = cs.at[corner, k - 4], cr.at[corner, k - 4]
                self.copies.append(
                    pltpu.make_async_remote_copy(
                        src_ref=source, dst_ref=landing,
                        send_sem=send.at[number, k], recv_sem=recv.at[number, k],
                        device_id={"gx": moved("gx", dx), "gy": moved("gy", dy)}, device_id_type=MESH,
                    )
                )

        def start(self):
            buf = self.buf
            for k, (dx, dy) in enumerate(WAYS):
                if dy == 0:
                    pl.when(exists(dx, dy))(self.copies[k].start)

            def gather(f, carry):
                for x in range(0, nx, TILE):
                    for way, step in ((0, 1), (1, -1)):
                        self.ys[way, f, pl.ds(x, TILE), :] = buf[f, pl.ds(first(x + 1) + edge_row(step), TILE, stride=pitch), :]
                for k, (dx, dy) in enumerate(WAYS[4:]):
                    row = first(nx if dx > 0 else 1) + edge_row(dy)
                    self.cs[self.corner, k, pl.ds(f - self.low, 1), :] = buf[f, pl.ds(row, 1), :]
                return carry

            lax.fori_loop(self.low, self.high, gather, 0)
            for k, (dx, dy) in enumerate(WAYS):
                if dy != 0:
                    pl.when(exists(dx, dy))(self.copies[k].start)

        def receive(self):
            buf = self.buf
            for k, (dx, dy) in enumerate(WAYS):
                pl.when(exists(-dx, -dy))(self.copies[k].wait_recv)

            def rows(way, step):
                def body(f, carry):
                    for x in range(0, nx, TILE):
                        buf[f, pl.ds(first(x + 1) + halo_row(-step), TILE, stride=pitch), :] = self.yr[way, f, pl.ds(x, TILE), :]
                    return carry
                lax.fori_loop(self.low, self.high, body, 0)

            def corner(k, dx, dy):
                def body(f, carry):
                    row = first(0 if dx > 0 else nx + 1) + halo_row(-dy)
                    buf[f, pl.ds(row, 1), :] = self.cr[self.corner, k, pl.ds(f - self.low, 1), :]
                    return carry
                lax.fori_loop(self.low, self.high, body, 0)

            for way, step in ((0, 1), (1, -1)):
                pl.when(exists(0, -step))(functools.partial(rows, way, step))
            for k, (dx, dy) in enumerate(WAYS[4:]):
                pl.when(exists(-dx, -dy))(functools.partial(corner, k, dx, dy))

        def finish(self):
            for k, (dx, dy) in enumerate(WAYS):
                pl.when(exists(dx, dy))(self.copies[k].wait_send)

    class Depth:
        def __init__(self, number, zs, zl, zr, buf, plane):
            self.zl, self.zr, self.buf, self.plane = zl, zr, buf, plane
            self.copies = [
                pltpu.make_async_remote_copy(
                    src_ref=zs, dst_ref=landing,
                    send_sem=z_send.at[number, way], recv_sem=z_recv.at[number, way],
                    device_id={"gz": moved("gz", step)}, device_id_type=MESH,
                )
                for way, (landing, step) in enumerate(((zl, 1), (zr, -1)))
            ]

        def start(self):
            pl.when(above_z)(self.copies[0].start)
            pl.when(below_z)(self.copies[1].start)

        def receive(self):
            pl.when(below_z)(self.copies[0].wait_recv)
            pl.when(above_z)(self.copies[1].wait_recv)
            zero = jnp.zeros((TILE, LANES), self.buf.dtype)

            def place(x, carry):
                for k in range(tiles):
                    row, at = own_tile(x, k)
                    low = jnp.where(below_z, self.zl[pl.ds(at, TILE), :], zero)
                    high = jnp.where(above_z, self.zr[pl.ds(at, TILE), :], zero)
                    self.buf[self.plane, pl.ds(row, TILE), :] = jnp.where(odd, low, high)
                return carry

            lax.fori_loop(0, nx, place, 0, unroll=8)

        def finish(self):
            pl.when(above_z)(self.copies[0].wait_send)
            pl.when(below_z)(self.copies[1].wait_send)

    code_z = Depth(0, zs_i, zl_i, zr_i, codes, 1)
    code_own = Unit(0, codes, 0, 1, ys_i, yr_i, cs_i, cr_i, 0)
    code_packed = Unit(1, codes, 1, 2, ys_i, yr_i, cs_i, cr_i, 1)
    w_z = Depth(1, zs_f.at[0], zl_f.at[0], zr_f.at[0], wbuf, fields)
    w_a = Unit(2, wbuf, 0, cut + 1, ys_w, yr_w, cs_w, cr_w, 0)
    w_b = Unit(3, wbuf, cut + 1, fields, ys_w, yr_w, cs_w, cr_w, 1)
    w_packed = Unit(4, wbuf, fields, fields + 1, ys_w, yr_w, cs_w, cr_w, 2)
    qa_z = Depth(2, zs_f.at[1], zl_f.at[1], zr_f.at[1], qbuf, nspec)
    q_a = Unit(5, qbuf, 0, cut, ys_q, yr_q, cs_q, cr_q, 0)
    qa_packed = Unit(6, qbuf, nspec, nspec + 1, ys_q, yr_q, cs_q, cr_q, 1)
    qb_z = Depth(3, zs_f.at[2], zl_f.at[2], zr_f.at[2], qbuf, nspec + 1)
    q_b = Unit(7, qbuf, cut, nspec, ys_q, yr_q, cs_q, cr_q, 2)
    qb_packed = Unit(8, qbuf, nspec + 1, nspec + 2, ys_q, yr_q, cs_q, cr_q, 3)
    everything = [code_z, code_own, code_packed, w_z, w_a, w_b, w_packed, qa_z, q_a, qa_packed, qb_z, q_b, qb_packed]

    def peer_copies(axis):
        number = AXES.index(axis)
        return [
            pltpu.make_async_remote_copy(
                src_ref=peers.at[number, here[axis]], dst_ref=peers.at[number, here[axis]],
                send_sem=peer_send.at[number, k], recv_sem=peer_recv.at[number, k],
                device_id={axis: lax.rem(here[axis] + k, size[axis])}, device_id_type=MESH,
            )
            for k in range(1, size[axis])
        ]

    def reduce_start(axis, value):
        peers[AXES.index(axis), here[axis]] = value
        for copy in peer_copies(axis):
            copy.start()

    def reduce_finish(axis):
        number = AXES.index(axis)
        for copy in peer_copies(axis):
            copy.wait()
        value = peers[number, 0]
        for k in range(1, size[axis]):
            value = value + peers[number, k]
        return value

    def fractions(own):
        is_cut = flag[own, :] == 1
        volume = jnp.where(is_cut, vol[own, :], 256).astype(jnp.float32) * (1.0 / 256.0)
        face = jnp.where(is_cut, area[own, :], 256).astype(jnp.float32) * (1.0 / 256.0)
        return volume, face

    def fill(x, carry):
        for k in range(tiles):
            row, at = own_tile(x, k)
            own = pl.ds(at, TILE)
            value = jnp.where(flag[own, :] == 1, code[own, :] | CENTER, CENTER)
            codes[0, pl.ds(row, TILE), :] = value
            shifted[0, own, :] = jnp.where(first_lane, 0, pltpu.roll(value, 1, 1))
            shifted[1, own, :] = jnp.where(last_lane, 0, pltpu.roll(value, LANES - 1, 1))
            low = jnp.broadcast_to(value[:, :1], (TILE, LANES))
            high = lax.shift_right_logical(jnp.broadcast_to(value[:, LANES - 1:], (TILE, LANES)), 2)
            zs_i[own, :] = jnp.where(odd, high, low)
            edge[own, :] = jnp.where(odd, low, high)
        return carry

    def add_up(x, totals):
        for k in range(tiles):
            _, at = own_tile(x, k)
            own = pl.ds(at, TILE)
            volume, _ = fractions(own)
            totals = tuple(totals[s] + volume * prov[s, own, :] for s in range(nspec))
        return totals

    def taps(row, step, left, middle, right, buf, low, high):
        zero = jnp.zeros((TILE, LANES), jnp.float32)
        sums = [[None] * (high - low) for _ in range(3)]
        for a, b, position in BLOCK:
            near = pl.ds(row + step * (a * pitch + b), TILE)
            present = []
            for k, source in enumerate((left, middle, right)):
                if step > 0 and position + k == 13:
                    present.append(None)
                else:
                    present.append((source(near) & (1 << (position + k))) != 0)
            for f in range(low, high):
                value = buf[f, near, :]
                for k in range(3):
                    term = value if present[k] is None else jnp.where(present[k], value, zero)
                    old = sums[k][f - low]
                    sums[k][f - low] = term if old is None else old + term
        return sums

    def packed_taps(row, step, source, buf, plane):
        zero = jnp.zeros((TILE, LANES), jnp.float32)
        total = None
        for a, b, position in BLOCK:
            near = pl.ds(row + step * (a * pitch + b), TILE)
            term = jnp.where((source(near) & (1 << position)) != 0, buf[plane, near, :], zero)
            total = term if total is None else total + term
        return total

    def pack(values, lowest):
        packed = jnp.zeros((TILE, LANES), jnp.float32)
        for k, value in enumerate(values):
            f = lowest + k
            start = value if f == 0 else pltpu.roll(value, 2 * f, 1)
            packed = jnp.where(lane == 2 * f, start, packed)
            packed = jnp.where(lane == 2 * f + 1, pltpu.roll(value, 2 * f + 2, 1), packed)
        return packed

    quad = 2
    members = [(k, k // tiles, k % tiles) for k in range(quad * tiles)]

    def count_taps(g):
        for k, x, y in members:
            row, at = own_tile(g * quad + x, y)
            sums = [None] * 3
            total = None
            for a, b, position in BLOCK:
                near = pl.ds(row - a * pitch - b, TILE)
                value = codes[0, near, :]
                value = value if position == 0 else lax.shift_right_logical(value, position)
                for m in range(3):
                    term = value & (1 << m)
                    sums[m] = term if sums[m] is None else sums[m] + term
                value = codes[1, near, :]
                value = value if position == 0 else lax.shift_right_logical(value, position)
                total = value & 1 if total is None else total + (value & 1)
            for m in range(3):
                parts_i[k, m] = sums[m]
            parts_i[k, 3] = total

    def weigh(g):
        for k, x, y in members:
            row, at = own_tile(g * quad + x, y)
            own = pl.ds(at, TILE)
            from_end = pltpu.roll(parts_i[k, 3], LANES - 1, 1)
            from_left = pltpu.roll(lax.shift_right_logical(parts_i[k, 2], 2), 1, 1)
            from_right = pltpu.roll(parts_i[k, 0], LANES - 1, 1)
            counted = lax.shift_right_logical(parts_i[k, 1], 1)
            counted = counted + jnp.where(first_lane, from_end, from_left) + jnp.where(last_lane, from_end, from_right)
            volume, face = fractions(own)
            share = 1.0 / counted.astype(jnp.float32)
            scaling[own, :] = face * share
            weight = volume * share
            for s in range(nspec):
                f = s if s < cut else s + 1
                wbuf[f, pl.ds(row, TILE), :] = weight * prov[s, own, :]
            wbuf[flux, pl.ds(row, TILE), :] = weight * face

    def weigh_pack(g):
        for k, x, y in members:
            row, at = own_tile(g * quad + x, y)
            zs_f[0, pl.ds(at, TILE), :] = pack([wbuf[f, pl.ds(row, TILE), :] for f in range(fields)], 0)

    def quota_stages(low, high, with_ends):
        n = high - low
        base = low if low == 0 else low - 1

        def main(x):
            for k in range(tiles):
                row, at = own_tile(x, k)
                own = pl.ds(at, TILE)
                right, left, middle = shifted[0, own, :], shifted[1, own, :], codes[0, pl.ds(row, TILE), :]
                sums = taps(row, 1, lambda near: left, lambda near: middle, lambda near: right, wbuf, low, high)
                for m in range(3):
                    for f in range(n):
                        parts_f[k, m, f] = sums[m][f]
                if with_ends:
                    value = edge[own, :]
                    ends[own, :] = packed_taps(row, 1, lambda near: value, wbuf, fields)

        def close(x):
            for k in range(tiles):
                row, at = own_tile(x, k)
                own = pl.ds(at, TILE)
                packed = ends[own, :]
                found = []
                for f in range(n):
                    spread = pltpu.roll(packed, LANES - 1 - 2 * (low + f), 1)
                    total = parts_f[k, 1, f] + pltpu.roll(parts_f[k, 2, f], LANES - 1, 1)
                    total = total + pltpu.roll(parts_f[k, 0, f], 1, 1)
                    found.append(total + jnp.where(both_ends, spread, 0.0))
                if with_ends:
                    inverted = 1.0 / found[flux]
                    weights[own, :] = inverted
                    found = found[:flux]
                else:
                    inverted = weights[own, :]
                for f, value in enumerate(found):
                    qbuf[base + f, pl.ds(row, TILE), :] = value * inverted

        def send_pack(x):
            for k in range(tiles):
                row, at = own_tile(x, k)
                group = group_a if with_ends else group_b
                zs_f[1 if with_ends else 2, pl.ds(at, TILE), :] = pack([qbuf[s, pl.ds(row, TILE), :] for s in group], 0)

        return [main, close, send_pack]

    def scatter_stages(group, plane):
        n = len(group)
        low = group[0]

        def main(x):
            for k in range(tiles):
                row, at = own_tile(x, k)

                def source(near):
                    return codes[0, near, :]

                sums = taps(row, -1, source, source, source, qbuf, low, low + n)
                for m in range(3):
                    for f in range(n):
                        parts_f[k, m, f] = sums[m][f]
                parts_f[k, 0, n] = packed_taps(row, -1, lambda near: codes[1, near, :], qbuf, plane)

        def close(x):
            for k in range(tiles):
                row, at = own_tile(x, k)
                own = pl.ds(at, TILE)
                packed = parts_f[k, 0, n]
                factor = scaling[own, :]
                for f, s in enumerate(group):
                    spread = pltpu.roll(packed, LANES - 1 - 2 * f, 1)
                    total = parts_f[k, 1, f]
                    total = total + jnp.where(first_lane, spread, pltpu.roll(parts_f[k, 2, f], 1, 1))
                    total = total + jnp.where(last_lane, spread, pltpu.roll(parts_f[k, 0, f], LANES - 1, 1))
                    out[s, own, :] = factor * total

        return [main, close]

    blank(codes, 0, 2)
    blank(wbuf, 0, fields + 1)
    blank(qbuf, 0, nspec + 2)
    loads[0].wait()
    loads[1].wait()
    lax.fori_loop(0, nx, fill, 0, unroll=8)
    pl.semaphore_wait(barrier, len(others))
    code_z.start()
    code_own.start()
    for copy in loads[2:]:
        copy.wait()
    totals = tuple(jnp.zeros((TILE, LANES), jnp.float32) for _ in range(nspec))
    totals = lax.fori_loop(0, nx // 2, add_up, totals, unroll=2)
    code_z.receive()
    code_packed.start()
    totals = lax.fori_loop(nx // 2, nx, add_up, totals, unroll=2)
    local = jnp.concatenate(
        [jnp.sum(total, axis=0, keepdims=True) for total in totals]
        + [jnp.zeros((peers.shape[2] - nspec, LANES), jnp.float32)],
        axis=0,
    )
    reduce_start("gx", local)
    code_own.receive()
    code_packed.receive()
    pipelined([count_taps, weigh, weigh_pack], nx // quad)
    w_z.start()
    w_a.start()
    w_b.start()
    reduce_start("gy", reduce_finish("gx"))
    w_z.receive()
    w_packed.start()
    w_a.receive()
    w_packed.receive()
    pipelined(quota_stages(0, cut + 1, True), nx)
    qa_z.start()
    q_a.start()
    w_b.receive()
    reduce_start("gz", reduce_finish("gy"))

    def middle_a():
        qa_z.receive()
        qa_packed.start()

    pipelined(quota_stages(cut + 1, fields, False), nx, (nx // 3, middle_a))
    qb_z.start()
    q_b.start()
    summed = reduce_finish("gz")
    change[...] = jnp.broadcast_to(jnp.sum(summed, axis=1, keepdims=True) * scale, change.shape)
    q_a.receive()
    qa_packed.receive()

    def middle_b():
        qb_z.receive()
        qb_packed.start()

    pipelined(scatter_stages(group_a, nspec), nx, (nx // 3, middle_b))
    q_b.receive()
    qb_packed.receive()
    pipelined(scatter_stages(group_b, nspec + 1), nx)
    for part in everything:
        part.finish()


def per_device(provisional, cut_flag, cut_code, volume_level, area_level):
    nspec, nx, ny, nz = provisional.shape
    assert nz == LANES and ny % TILE == 0 and nx % TILE == 0
    own = nx * ny
    tiles = ny // TILE
    rows = TILE + (nx + 2) * (ny + TILE)
    most = max(lax.axis_size(axis) for axis in AXES)
    cells = own * nz * math.prod(lax.axis_size(axis) for axis in AXES)
    high = -(-nspec // TILE) * TILE
    cut = nspec // 2
    fields = nspec + 1
    group = max(cut + 1, nspec - cut)
    wide = -(-group // TILE) * TILE
    f32, i32 = jnp.float32, jnp.int32
    vmem = pl.BlockSpec(memory_space=pltpu.VMEM)
    hbm = pl.BlockSpec(memory_space=pltpu.HBM)
    shapes = [
        ((nspec, own, nz), f32), ((own, nz), i32), ((own, nz), i32), ((own, nz), i32), ((own, nz), i32),
        ((2, rows, nz), i32), ((fields + 1, rows, nz), f32), ((nspec + 2, rows, nz), f32),
        ((2, own, nz), i32), ((own, nz), i32),
        ((own, nz), i32), ((own, nz), i32), ((own, nz), i32),
        ((3, own, nz), f32), ((3, own, nz), f32), ((3, own, nz), f32),
        ((2, 2, nx, nz), i32), ((2, 2, nx, nz), i32), ((2, 4, TILE, nz), i32), ((2, 4, TILE, nz), i32),
        ((2, fields + 1, nx, nz), f32), ((2, fields + 1, nx, nz), f32), ((3, 4, wide, nz), f32), ((3, 4, wide, nz), f32),
        ((2, nspec + 2, nx, nz), f32), ((2, nspec + 2, nx, nz), f32), ((4, 4, wide, nz), f32), ((4, 4, wide, nz), f32),
        ((own, nz), f32), ((own, nz), f32), ((own, nz), f32),
        ((2 * tiles, 4, TILE, nz), i32), ((tiles, 3, group + 1, TILE, nz), f32),
        ((3, most, high, nz), f32),
    ]
    dma = pltpu.SemaphoreType.DMA
    out, change = pl.pallas_call(
        functools.partial(kernel, nx, ny, 1.0 / math.sqrt(cells)),
        out_shape=(
            jax.ShapeDtypeStruct((nspec, own, nz), f32),
            jax.ShapeDtypeStruct((high, nz), f32),
        ),
        in_specs=[hbm] * 5,
        out_specs=(vmem, vmem),
        scratch_shapes=[pltpu.VMEM(shape, kind) for shape, kind in shapes]
        + [
            dma((5,)), dma((4, 2)), dma((4, 2)), dma((9, 8)), dma((9, 8)), dma((3, most)), dma((3, most)),
        ],
        compiler_params=pltpu.CompilerParams(
            collective_id=0, has_side_effects=True, vmem_limit_bytes=26 * 1024 * 1024
        ),
    )(
        *[pltpu.with_memory_space_constraint(x, pltpu.HBM) for x in (
        provisional.reshape(nspec, own, nz),
        cut_flag.reshape(own, nz),
        cut_code.reshape(own, nz),
        volume_level.reshape(own, nz),
        area_level.reshape(own, nz))]
    )
    return out.reshape(provisional.shape), change[:nspec, 0]


def solution(mesh):
    spec = P("gx", "gy", "gz")
    wide = P(None, "gx", "gy", "gz")
    return jax.shard_map(
        per_device, mesh=mesh, in_specs=(wide, spec, spec, spec, spec), out_specs=(wide, P()), check_vma=False
    )
```

```python
import functools
import math

import jax
import jax.numpy as jnp
from jax import lax
from jax.experimental import pallas as pl
from jax.experimental.pallas import tpu as pltpu
from jax.sharding import PartitionSpec as P

CENTER = 8192
BLOCK = [(a, b, 9 * (a + 1) + 3 * (b + 1)) for a in (-1, 0, 1) for b in (-1, 0, 1)]
AXES = ("gx", "gy", "gz")
WAYS = [(1, 0), (-1, 0), (0, 1), (0, -1), (1, 1), (1, -1), (-1, 1), (-1, -1)]
MESH = pl.DeviceIdType.MESH
LANES = 128
TILE = 8


def pipelined(stages, count, hook=None):
    depth = len(stages)

    def step(i, lowest, highest):
        for k in reversed(range(lowest, highest)):
            stages[k](i - k)

    for i in range(min(depth - 1, count)):
        step(i, 0, i + 1)

    def body(i, carry):
        step(i, 0, depth)
        return carry

    low = depth - 1
    if hook is not None:
        at, action = hook
        lax.fori_loop(low, at, body, 0)
        action()
        low = at
    lax.fori_loop(low, count, body, 0)
    for i in range(count, count + depth - 1):
        step(i, i - count + 1, depth)


def kernel(
    nx, ny, scale,
    prov_h, flag_h, code_h, vol_h, area_h,
    out, change,
    prov, flag, code, vol, area,
    codes, wbuf, qbuf, packed, shifted, edge,
    zs_i, zl_i, zr_i, zs_f, zl_f, zr_f,
    ys_i, yr_i, cs_i, cr_i, ys_p, yr_p, cs_p, cr_p,
    xr, ys, yr, cs, cr,
    gathered, scaling, parts_i, parts_f, parts_e, peers,
    load, z_send, z_recv, send, recv, peer_send, peer_recv,
):
    nspec = prov.shape[0]
    pitch = ny + TILE
    tiles = ny // TILE
    here = {axis: lax.axis_index(axis) for axis in AXES}
    size = {axis: lax.axis_size(axis) for axis in AXES}
    lane = lax.broadcasted_iota(jnp.int32, (TILE, LANES), 1)
    odd = (lane & 1) == 1
    first_lane = lane == 0
    last_lane = lane == LANES - 1
    both_ends = first_lane | last_lane
    fields = nspec + 1
    flux = nspec

    inputs = [(flag_h, flag), (code_h, code), (vol_h, vol), (area_h, area), (prov_h, prov)]
    loads = [pltpu.make_async_copy(src, dst, load.at[k]) for k, (src, dst) in enumerate(inputs)]
    for copy in loads:
        copy.start()

    def moved(axis, step):
        return lax.rem(here[axis] + (step + size[axis]), size[axis])

    barrier = pltpu.get_barrier_semaphore()
    others = set()
    for dx, dy in WAYS:
        others.add((dx % size["gx"], dy % size["gy"], 0))
    for number, axis in enumerate(AXES):
        for k in range(1, size[axis]):
            others.add(tuple(k if i == number else 0 for i in range(3)))
    others.discard((0, 0, 0))
    for shift in sorted(others):
        pl.semaphore_signal(
            barrier, inc=1,
            device_id={axis: lax.rem(here[axis] + shift[i], size[axis]) for i, axis in enumerate(AXES)},
            device_id_type=MESH,
        )

    def first(x):
        return TILE + x * pitch

    def own_tile(x, k):
        row = (TILE + pitch + k * TILE) + x * pitch
        at = x * ny + k * TILE
        if isinstance(x, int):
            return row, at
        return pl.multiple_of(row, TILE), pl.multiple_of(at, TILE)

    def side(axis, step):
        return here[axis] < size[axis] - 1 if step > 0 else here[axis] > 0

    def exists(dx, dy):
        found = None
        for axis, step in (("gx", dx), ("gy", dy)):
            if step:
                there = side(axis, step)
                found = there if found is None else jnp.logical_and(found, there)
        return found

    below_z, above_z = side("gz", -1), side("gz", 1)

    def edge_row(step):
        return ny - 1 if step > 0 else 0

    def halo_row(step):
        return ny if step > 0 else -1

    def blank(buf, low, high):
        zeros = jnp.zeros((ny, LANES), buf.dtype)
        row_zeros = jnp.zeros((TILE, LANES), buf.dtype)
        one = jnp.zeros((1, LANES), buf.dtype)

        def plane(step):
            def body(f, carry):
                buf[f, pl.ds(first(nx + 1 if step > 0 else 0), ny), :] = zeros
                return carry
            lax.fori_loop(low, high, body, 0)

        def row(step):
            def body(f, carry):
                for x in range(0, nx, TILE):
                    buf[f, pl.ds(first(x + 1) + halo_row(step), TILE, stride=pitch), :] = row_zeros
                return carry
            lax.fori_loop(low, high, body, 0)

        def corner(dx, dy):
            def body(f, carry):
                buf[f, pl.ds(first(nx + 1 if dx > 0 else 0) + halo_row(dy), 1), :] = one
                return carry
            lax.fori_loop(low, high, body, 0)

        for dx, dy in WAYS:
            action = functools.partial(plane, dx) if dy == 0 else (
                functools.partial(row, dy) if dx == 0 else functools.partial(corner, dx, dy))
            pl.when(jnp.logical_not(exists(dx, dy)))(action)

    class Unit:
        def __init__(self, number, buf, low, high, ys, yr, cs, cr, corner):
            self.buf, self.low, self.high = buf, low, high
            self.ys, self.yr, self.cs, self.cr, self.corner = ys, yr, cs, cr, corner
            n = high - low
            ends_of = {1: (nx, 0), -1: (1, nx + 1)}
            self.copies = []
            for k, (dx, dy) in enumerate(WAYS):
                if dy == 0:
                    here_x, there_x = ends_of[dx]
                    source = buf.at[pl.ds(low, n), pl.ds(first(here_x), ny), :]
                    landing = buf.at[pl.ds(low, n), pl.ds(first(there_x), ny), :]
                elif dx == 0:
                    way = 0 if dy > 0 else 1
                    source, landing = ys.at[way, pl.ds(low, n)], yr.at[way, pl.ds(low, n)]
                else:
                    source, landing = cs.at[corner, k - 4], cr.at[corner, k - 4]
                self.copies.append(
                    pltpu.make_async_remote_copy(
                        src_ref=source, dst_ref=landing,
                        send_sem=send.at[number, k], recv_sem=recv.at[number, k],
                        device_id={"gx": moved("gx", dx), "gy": moved("gy", dy)}, device_id_type=MESH,
                    )
                )

        def start(self):
            buf = self.buf
            for k, (dx, dy) in enumerate(WAYS):
                if dy == 0:
                    pl.when(exists(dx, dy))(self.copies[k].start)

            def gather(f, carry):
                for x in range(0, nx, TILE):
                    for way, step in ((0, 1), (1, -1)):
                        self.ys[way, f, pl.ds(x, TILE), :] = buf[f, pl.ds(first(x + 1) + edge_row(step), TILE, stride=pitch), :]
                for k, (dx, dy) in enumerate(WAYS[4:]):
                    row = first(nx if dx > 0 else 1) + edge_row(dy)
                    self.cs[self.corner, k, pl.ds(f - self.low, 1), :] = buf[f, pl.ds(row, 1), :]
                return carry

            lax.fori_loop(self.low, self.high, gather, 0)
            for k, (dx, dy) in enumerate(WAYS):
                if dy != 0:
                    pl.when(exists(dx, dy))(self.copies[k].start)

        def receive(self):
            buf = self.buf
            for k, (dx, dy) in enumerate(WAYS):
                pl.when(exists(-dx, -dy))(self.copies[k].wait_recv)

            def rows(way, step):
                def body(f, carry):
                    for x in range(0, nx, TILE):
                        buf[f, pl.ds(first(x + 1) + halo_row(-step), TILE, stride=pitch), :] = self.yr[way, f, pl.ds(x, TILE), :]
                    return carry
                lax.fori_loop(self.low, self.high, body, 0)

            def corner(k, dx, dy):
                def body(f, carry):
                    row = first(0 if dx > 0 else nx + 1) + halo_row(-dy)
                    buf[f, pl.ds(row, 1), :] = self.cr[self.corner, k, pl.ds(f - self.low, 1), :]
                    return carry
                lax.fori_loop(self.low, self.high, body, 0)

            for way, step in ((0, 1), (1, -1)):
                pl.when(exists(0, -step))(functools.partial(rows, way, step))
            for k, (dx, dy) in enumerate(WAYS[4:]):
                pl.when(exists(-dx, -dy))(functools.partial(corner, k, dx, dy))

        def finish(self):
            for k, (dx, dy) in enumerate(WAYS):
                pl.when(exists(dx, dy))(self.copies[k].wait_send)

    class Depth:
        def __init__(self, number, zs, zl, zr, buf, plane):
            self.zl, self.zr, self.buf, self.plane = zl, zr, buf, plane
            self.copies = [
                pltpu.make_async_remote_copy(
                    src_ref=zs, dst_ref=landing,
                    send_sem=z_send.at[number, way], recv_sem=z_recv.at[number, way],
                    device_id={"gz": moved("gz", step)}, device_id_type=MESH,
                )
                for way, (landing, step) in enumerate(((zl, 1), (zr, -1)))
            ]

        def start(self):
            pl.when(above_z)(self.copies[0].start)
            pl.when(below_z)(self.copies[1].start)

        def receive(self):
            pl.when(below_z)(self.copies[0].wait_recv)
            pl.when(above_z)(self.copies[1].wait_recv)
            zero = jnp.zeros((TILE, LANES), self.buf.dtype)

            def place(x, carry):
                for k in range(tiles):
                    row, at = own_tile(x, k)
                    low = jnp.where(below_z, self.zl[pl.ds(at, TILE), :], zero)
                    high = jnp.where(above_z, self.zr[pl.ds(at, TILE), :], zero)
                    self.buf[self.plane, pl.ds(row, TILE), :] = jnp.where(odd, low, high)
                return carry

            lax.fori_loop(0, nx, place, 0, unroll=8)

        def finish(self):
            pl.when(above_z)(self.copies[0].wait_send)
            pl.when(below_z)(self.copies[1].wait_send)

    class Faces:
        def __init__(self, number, buf, n, which):
            self.buf, self.n = buf, n
            self.xr, self.ys, self.yr, self.cs, self.cr = xr.at[which], ys.at[which], yr.at[which], cs.at[which], cr.at[which]
            self.copies = []
            for k, (dx, dy) in enumerate(WAYS):
                way = 0 if dx + dy > 0 else 1
                if dy == 0:
                    source = buf.at[pl.ds(0, n), pl.ds(first(nx if dx > 0 else 1), ny), :]
                    landing = self.xr.at[way, pl.ds(0, n), pl.ds(TILE, ny), :]
                elif dx == 0:
                    source = self.ys.at[way, pl.ds(0, n)]
                    landing = self.yr.at[way, pl.ds(0, n), pl.ds(TILE, nx), :]
                else:
                    source, landing = self.cs.at[k - 4], self.cr.at[k - 4]
                self.copies.append(
                    pltpu.make_async_remote_copy(
                        src_ref=source, dst_ref=landing,
                        send_sem=send.at[number, k], recv_sem=recv.at[number, k],
                        device_id={"gx": moved("gx", dx), "gy": moved("gy", dy)}, device_id_type=MESH,
                    )
                )

        def blank(self):
            def low(f, carry):
                zeros = jnp.zeros((TILE, LANES), jnp.float32)
                for p in range(nx + 3):
                    self.buf[f, pl.ds(p * pitch, TILE), :] = zeros
                for p in (0, nx + 1):
                    for k in range(tiles):
                        self.buf[f, pl.ds(first(p) + k * TILE, TILE), :] = zeros
                for way in range(2):
                    for at in (0, TILE + ny):
                        self.xr[way, f, pl.ds(at, TILE), :] = zeros
                    for at in (0, TILE + nx):
                        self.yr[way, f, pl.ds(at, TILE), :] = zeros
                return carry

            lax.fori_loop(0, self.n, low, 0)

            def clear(ref, way, extent):
                def body(f, carry):
                    ref[way, f, pl.ds(TILE, extent), :] = jnp.zeros((extent, LANES), jnp.float32)
                    return carry
                lax.fori_loop(0, self.n, body, 0)

            for way, step in ((0, 1), (1, -1)):
                pl.when(jnp.logical_not(exists(-step, 0)))(functools.partial(clear, self.xr, way, ny))
                pl.when(jnp.logical_not(exists(0, -step)))(functools.partial(clear, self.yr, way, nx))

        def start(self):
            buf = self.buf

            def gather(f, carry):
                for x in range(0, nx, TILE):
                    for way, step in ((0, 1), (1, -1)):
                        self.ys[way, f, pl.ds(x, TILE), :] = buf[f, pl.ds(first(x + 1) + edge_row(step), TILE, stride=pitch), :]
                for k, (dx, dy) in enumerate(WAYS[4:]):
                    row = first(nx if dx > 0 else 1) + edge_row(dy)
                    self.cs[k, pl.ds(f, 1), :] = buf[f, pl.ds(row, 1), :]
                return carry

            for k in range(2):
                pl.when(exists(*WAYS[k]))(self.copies[k].start)
            lax.fori_loop(0, self.n, gather, 0)
            for k in range(2, 8):
                pl.when(exists(*WAYS[k]))(self.copies[k].start)

        def receive(self):
            for k, (dx, dy) in enumerate(WAYS):
                pl.when(exists(-dx, -dy))(self.copies[k].wait_recv)

            def corner(k, dx, dy):
                way = 0 if dy > 0 else 1
                at = TILE - 1 if dx > 0 else TILE + nx

                def body(f, carry):
                    self.yr[way, f, pl.ds(at, 1), :] = self.cr[k, pl.ds(f, 1), :]
                    return carry
                lax.fori_loop(0, self.n, body, 0)

            for k, (dx, dy) in enumerate(WAYS[4:]):
                pl.when(exists(-dx, -dy))(functools.partial(corner, k, dx, dy))

        def finish(self):
            for k, (dx, dy) in enumerate(WAYS):
                pl.when(exists(dx, dy))(self.copies[k].wait_send)

    code_z = Depth(0, zs_i, zl_i, zr_i, codes, 1)
    code_own = Unit(0, codes, 0, 1, ys_i, yr_i, cs_i, cr_i, 0)
    code_packed = Unit(1, codes, 1, 2, ys_i, yr_i, cs_i, cr_i, 1)
    w_z = Depth(1, zs_f.at[0], zl_f.at[0], zr_f.at[0], packed, 0)
    w_all = Faces(2, wbuf, fields, 0)
    w_packed = Unit(3, packed, 0, 1, ys_p, yr_p, cs_p, cr_p, 0)
    q_z = Depth(2, zs_f.at[1], zl_f.at[1], zr_f.at[1], packed, 1)
    q_all = Faces(4, qbuf, nspec, 1)
    q_packed = Unit(5, packed, 1, 2, ys_p, yr_p, cs_p, cr_p, 1)
    everything = [code_z, code_own, code_packed, w_z, w_all, w_packed, q_z, q_all, q_packed]

    def peer_copies(axis):
        number = AXES.index(axis)
        return [
            pltpu.make_async_remote_copy(
                src_ref=peers.at[number, here[axis]], dst_ref=peers.at[number, here[axis]],
                send_sem=peer_send.at[number, k], recv_sem=peer_recv.at[number, k],
                device_id={axis: lax.rem(here[axis] + k, size[axis])}, device_id_type=MESH,
            )
            for k in range(1, size[axis])
        ]

    def reduce_start(axis, value):
        peers[AXES.index(axis), here[axis]] = value
        for copy in peer_copies(axis):
            copy.start()

    def reduce_finish(axis):
        number = AXES.index(axis)
        for copy in peer_copies(axis):
            copy.wait()
        value = peers[number, 0]
        for k in range(1, size[axis]):
            value = value + peers[number, k]
        return value

    def fractions(own):
        is_cut = flag[own, :] == 1
        volume = jnp.where(is_cut, vol[own, :], 256).astype(jnp.float32) * (1.0 / 256.0)
        face = jnp.where(is_cut, area[own, :], 256).astype(jnp.float32) * (1.0 / 256.0)
        return volume, face

    def fill(x, carry):
        for k in range(tiles):
            row, at = own_tile(x, k)
            own = pl.ds(at, TILE)
            value = jnp.where(flag[own, :] == 1, code[own, :] | CENTER, CENTER)
            codes[0, pl.ds(row, TILE), :] = value
            shifted[0, own, :] = jnp.where(first_lane, 0, pltpu.roll(value, 1, 1))
            shifted[1, own, :] = jnp.where(last_lane, 0, pltpu.roll(value, LANES - 1, 1))
            low = jnp.broadcast_to(value[:, :1], (TILE, LANES))
            high = lax.shift_right_logical(jnp.broadcast_to(value[:, LANES - 1:], (TILE, LANES)), 2)
            zs_i[own, :] = jnp.where(odd, high, low)
            edge[own, :] = jnp.where(odd, low, high)
        return carry

    def add_up(x, totals):
        for k in range(tiles):
            _, at = own_tile(x, k)
            own = pl.ds(at, TILE)
            volume, _ = fractions(own)
            totals = tuple(totals[s] + volume * prov[s, own, :] for s in range(nspec))
        return totals

    def masked_sums(taps, low, high):
        zero = jnp.zeros((TILE, LANES), jnp.float32)
        sums = [[None] * (high - low) for _ in range(3)]
        for sources, position, value_of in taps:
            present = [
                None if source is None else (source & (1 << (position + k))) != 0 for k, source in enumerate(sources)
            ]
            for f in range(low, high):
                value = value_of(f)
                for k in range(3):
                    term = value if present[k] is None else jnp.where(present[k], value, zero)
                    old = sums[k][f - low]
                    sums[k][f - low] = term if old is None else old + term
        return sums

    def keep_sums(slot, sums, low):
        for m in range(3):
            for f, value in enumerate(sums[m]):
                parts_f[slot, m, low + f] = value

    def merged(slot, f, wrap):
        if wrap:
            up, down = pltpu.roll(parts_f[slot, 2, f], 1, 1), pltpu.roll(parts_f[slot, 0, f], LANES - 1, 1)
            up, down = jnp.where(first_lane, 0.0, up), jnp.where(last_lane, 0.0, down)
        else:
            up, down = pltpu.roll(parts_f[slot, 2, f], LANES - 1, 1), pltpu.roll(parts_f[slot, 0, f], 1, 1)
        return parts_f[slot, 1, f] + up + down

    def packed_taps(row, step, source, buf, plane):
        zero = jnp.zeros((TILE, LANES), jnp.float32)
        total = None
        for a, b, position in BLOCK:
            near = pl.ds(row + step * (a * pitch + b), TILE)
            term = jnp.where((source(near) & (1 << position)) != 0, buf[plane, near, :], zero)
            total = term if total is None else total + term
        return total

    def pack(values, lowest):
        packed = jnp.zeros((TILE, LANES), jnp.float32)
        for k, value in enumerate(values):
            f = lowest + k
            start = value if f == 0 else pltpu.roll(value, 2 * f, 1)
            packed = jnp.where(lane == 2 * f, start, packed)
            packed = jnp.where(lane == 2 * f + 1, pltpu.roll(value, 2 * f + 2, 1), packed)
        return packed

    quad = 2
    members = [(k, k // tiles, k % tiles) for k in range(quad * tiles)]

    def count_taps(g):
        for k, x, y in members:
            row, at = own_tile(g * quad + x, y)
            sums = [None] * 3
            total = None
            for a, b, position in BLOCK:
                near = pl.ds(row - a * pitch - b, TILE)
                value = codes[0, near, :]
                value = value if position == 0 else lax.shift_right_logical(value, position)
                for m in range(3):
                    term = value & (1 << m)
                    sums[m] = term if sums[m] is None else sums[m] + term
                value = codes[1, near, :]
                value = value if position == 0 else lax.shift_right_logical(value, position)
                total = value & 1 if total is None else total + (value & 1)
            for m in range(3):
                parts_i[k, m] = sums[m]
            parts_i[k, 3] = total

    def weigh(g):
        for k, x, y in members:
            row, at = own_tile(g * quad + x, y)
            own = pl.ds(at, TILE)
            from_end = pltpu.roll(parts_i[k, 3], LANES - 1, 1)
            from_left = pltpu.roll(lax.shift_right_logical(parts_i[k, 2], 2), 1, 1)
            from_right = pltpu.roll(parts_i[k, 0], LANES - 1, 1)
            counted = lax.shift_right_logical(parts_i[k, 1], 1)
            counted = counted + jnp.where(first_lane, from_end, from_left) + jnp.where(last_lane, from_end, from_right)
            volume, face = fractions(own)
            share = 1.0 / counted.astype(jnp.float32)
            scaling[own, :] = face * share
            weight = volume * share
            for s in range(nspec):
                wbuf[s, pl.ds(row, TILE), :] = weight * prov[s, own, :]
            wbuf[flux, pl.ds(row, TILE), :] = weight * face

    def weigh_pack(g):
        for k, x, y in members:
            row, at = own_tile(g * quad + x, y)
            zs_f[0, pl.ds(at, TILE), :] = pack([wbuf[f, pl.ds(row, TILE), :] for f in range(fields)], 0)

    def own_row(t):
        x, k = lax.div(t, tiles), lax.rem(t, tiles)
        row = (TILE + pitch) + x * pitch + k * TILE
        if isinstance(t, int):
            return int(row), t * TILE
        return pl.multiple_of(row, TILE), pl.multiple_of(t * TILE, TILE)

    def reader(buf, near):
        return lambda f: buf[f, near, :]

    def gather_main(t):
        row, at = own_tile(t // tiles, t % tiles) if isinstance(t, int) else own_row(t)
        own = pl.ds(at, TILE)
        right, left, middle = shifted[0, own, :], shifted[1, own, :], codes[0, pl.ds(row, TILE), :]
        taps = []
        for a, b, position in BLOCK:
            center = None if position == 12 else middle
            taps.append(((left, center, right), position, reader(wbuf, pl.ds(row + a * pitch + b, TILE))))
        keep_sums(0, masked_sums(taps, 0, fields), 0)

    def gather_close(t):
        row, at = own_tile(t // tiles, t % tiles) if isinstance(t, int) else own_row(t)
        for f in range(nspec):
            qbuf[f, pl.ds(row, TILE), :] = merged(0, f, False)
        gathered[pl.ds(at, TILE), :] = merged(0, flux, False)

    def gather_strip(j):
        x = j * TILE
        for way, (b, y) in enumerate(((-1, 0), (1, ny - 1))):
            where = pl.ds(x * ny + y, TILE, stride=ny)
            right, left = shifted[0, where, :], shifted[1, where, :]
            middle = codes[0, pl.ds(first(1) + x * pitch + y, TILE, stride=pitch), :]
            taps = []
            for a in (-1, 0, 1):
                taps.append(((left, middle, right), 9 * (a + 1) + 3 * (b + 1), reader(yr.at[0, way], pl.ds(TILE + x + a, TILE))))
            keep_sums(way, masked_sums(taps, 0, fields), 0)

    def gather_strip_close(j):
        x = j * TILE
        for way, y in enumerate((0, ny - 1)):
            rows = pl.ds(first(1) + x * pitch + y, TILE, stride=pitch)
            for f in range(nspec):
                qbuf[f, rows, :] = qbuf[f, rows, :] + merged(way, f, False)
            where = pl.ds(x * ny + y, TILE, stride=ny)
            gathered[where, :] = gathered[where, :] + merged(way, flux, False)

    def gather_plane(way):
        a, x = ((-1, 0), (1, nx - 1))[way]
        for k in range(tiles):
            row, at = own_tile(x, k)
            own = pl.ds(at, TILE)
            right, left, middle = shifted[0, own, :], shifted[1, own, :], codes[0, pl.ds(row, TILE), :]
            taps = []
            for b in (-1, 0, 1):
                taps.append(((left, middle, right), 9 * (a + 1) + 3 * (b + 1), reader(xr.at[0, way], pl.ds(TILE + k * TILE + b, TILE))))
            keep_sums(way * tiles + k, masked_sums(taps, 0, fields), 0)

    def gather_plane_close(way):
        x = (0, nx - 1)[way]
        for k in range(tiles):
            row, at = own_tile(x, k)
            for f in range(nspec):
                qbuf[f, pl.ds(row, TILE), :] = qbuf[f, pl.ds(row, TILE), :] + merged(way * tiles + k, f, False)
            own = pl.ds(at, TILE)
            gathered[own, :] = gathered[own, :] + merged(way * tiles + k, flux, False)

    def gather_ends(g):
        for k, x, y in members:
            row, at = own_tile(g * quad + x, y)
            value = edge[pl.ds(at, TILE), :]
            parts_e[k] = packed_taps(row, 1, lambda near: value, packed, 0)

    def quotas(g):
        for k, x, y in members:
            row, at = own_tile(g * quad + x, y)
            value = parts_e[k]

            def spread(f):
                return jnp.where(both_ends, pltpu.roll(value, LANES - 1 - 2 * f, 1), 0.0)

            inverted = 1.0 / (gathered[pl.ds(at, TILE), :] + spread(flux))
            for f in range(nspec):
                qbuf[f, pl.ds(row, TILE), :] = (qbuf[f, pl.ds(row, TILE), :] + spread(f)) * inverted

    def quota_pack(g):
        for k, x, y in members:
            row, at = own_tile(g * quad + x, y)
            zs_f[1, pl.ds(at, TILE), :] = pack([qbuf[f, pl.ds(row, TILE), :] for f in range(nspec)], 0)

    def scatter_main(t):
        row, at = own_tile(t // tiles, t % tiles) if isinstance(t, int) else own_row(t)
        taps = []
        for a, b, position in BLOCK:
            near = pl.ds(row - a * pitch - b, TILE)
            source = codes[0, near, :]
            center = None if position == 12 else source
            taps.append(((source, center, source), position, reader(qbuf, near)))
        keep_sums(0, masked_sums(taps, 0, nspec), 0)

    def scatter_close(t):
        row, at = own_tile(t // tiles, t % tiles) if isinstance(t, int) else own_row(t)
        for f in range(nspec):
            out[f, pl.ds(at, TILE), :] = merged(0, f, True)

    def scatter_strip(j):
        x = j * TILE
        for way, (b, y) in enumerate(((1, -1), (-1, ny))):
            taps = []
            for a in (-1, 0, 1):
                source = codes[0, pl.ds(first(1) + (x - a) * pitch + y, TILE, stride=pitch), :]
                taps.append(((source, source, source), 9 * (a + 1) + 3 * (b + 1), reader(yr.at[1, way], pl.ds(TILE + x - a, TILE))))
            keep_sums(way, masked_sums(taps, 0, nspec), 0)

    def scatter_strip_close(j):
        for way, y in enumerate((0, ny - 1)):
            where = pl.ds(j * TILE * ny + y, TILE, stride=ny)
            for f in range(nspec):
                out[f, where, :] = out[f, where, :] + merged(way, f, True)

    def scatter_plane(way):
        a, x = ((1, 0), (-1, nx + 1))[way]
        for k in range(tiles):
            taps = []
            for b in (-1, 0, 1):
                source = codes[0, pl.ds(first(x) + k * TILE - b, TILE), :]
                taps.append(((source, source, source), 9 * (a + 1) + 3 * (b + 1), reader(xr.at[1, way], pl.ds(TILE + k * TILE - b, TILE))))
            keep_sums(way * tiles + k, masked_sums(taps, 0, nspec), 0)

    def scatter_plane_close(way):
        x = (0, nx - 1)[way]
        for k in range(tiles):
            row, at = own_tile(x, k)
            for f in range(nspec):
                out[f, pl.ds(at, TILE), :] = out[f, pl.ds(at, TILE), :] + merged(way * tiles + k, f, True)

    def scatter_ends(g):
        for k, x, y in members:
            row, at = own_tile(g * quad + x, y)
            parts_e[k] = packed_taps(row, -1, lambda near: codes[1, near, :], packed, 1)

    def finals(g):
        for k, x, y in members:
            row, at = own_tile(g * quad + x, y)
            own = pl.ds(at, TILE)
            value, factor = parts_e[k], scaling[own, :]
            for f in range(nspec):
                spread = jnp.where(both_ends, pltpu.roll(value, LANES - 1 - 2 * f, 1), 0.0)
                out[f, own, :] = factor * (out[f, own, :] + spread)

    blank(codes, 0, 2)
    blank(packed, 0, 2)
    w_all.blank()
    q_all.blank()
    loads[0].wait()
    loads[1].wait()
    lax.fori_loop(0, nx, fill, 0, unroll=8)
    pl.semaphore_wait(barrier, len(others))
    code_z.start()
    code_own.start()
    for copy in loads[2:]:
        copy.wait()
    totals = tuple(jnp.zeros((TILE, LANES), jnp.float32) for _ in range(nspec))
    totals = lax.fori_loop(0, nx // 2, add_up, totals, unroll=2)
    code_z.receive()
    code_packed.start()
    totals = lax.fori_loop(nx // 2, nx, add_up, totals, unroll=2)
    local = jnp.concatenate(
        [jnp.sum(total, axis=0, keepdims=True) for total in totals]
        + [jnp.zeros((peers.shape[2] - nspec, LANES), jnp.float32)],
        axis=0,
    )
    reduce_start("gx", local)
    code_own.receive()
    code_packed.receive()
    pipelined([count_taps, weigh, weigh_pack], nx // quad)
    w_z.start()
    w_all.start()

    def relay_w():
        w_z.receive()
        w_packed.start()
        reduce_start("gy", reduce_finish("gx"))

    pipelined([gather_main, gather_close], nx * tiles, (nx * tiles // 3, relay_w))
    w_all.receive()
    w_packed.receive()
    pipelined([gather_strip, gather_strip_close], nx // TILE)
    for stage in (gather_plane, gather_plane_close):
        stage(0)
        stage(1)
    pipelined([gather_ends, quotas, quota_pack], nx // quad)
    q_z.start()
    q_all.start()
    reduce_start("gz", reduce_finish("gy"))

    def relay_q():
        q_z.receive()
        q_packed.start()
        summed = reduce_finish("gz")
        change[...] = jnp.broadcast_to(jnp.sum(summed, axis=1, keepdims=True) * scale, change.shape)

    pipelined([scatter_main, scatter_close], nx * tiles, (nx * tiles // 3, relay_q))
    q_all.receive()
    q_packed.receive()
    pipelined([scatter_strip, scatter_strip_close], nx // TILE)
    for stage in (scatter_plane, scatter_plane_close):
        stage(0)
        stage(1)
    pipelined([scatter_ends, finals], nx // quad)
    for part in everything:
        part.finish()


def per_device(provisional, cut_flag, cut_code, volume_level, area_level):
    nspec, nx, ny, nz = provisional.shape
    assert nz == LANES and ny % TILE == 0 and nx % TILE == 0
    own = nx * ny
    tiles = ny // TILE
    rows = 2 * TILE + (nx + 2) * (ny + TILE)
    most = max(lax.axis_size(axis) for axis in AXES)
    cells = own * nz * math.prod(lax.axis_size(axis) for axis in AXES)
    high = -(-nspec // TILE) * TILE
    fields = nspec + 1
    wide = -(-fields // TILE) * TILE
    f32, i32 = jnp.float32, jnp.int32
    vmem = pl.BlockSpec(memory_space=pltpu.VMEM)
    hbm = pl.BlockSpec(memory_space=pltpu.HBM)
    shapes = [
        ((nspec, own, nz), f32), ((own, nz), i32), ((own, nz), i32), ((own, nz), i32), ((own, nz), i32),
        ((2, rows, nz), i32), ((fields, rows, nz), f32), ((nspec, rows, nz), f32), ((2, rows, nz), f32),
        ((2, own, nz), i32), ((own, nz), i32),
        ((own, nz), i32), ((own, nz), i32), ((own, nz), i32),
        ((2, own, nz), f32), ((2, own, nz), f32), ((2, own, nz), f32),
        ((2, 2, nx, nz), i32), ((2, 2, nx, nz), i32), ((2, 4, TILE, nz), i32), ((2, 4, TILE, nz), i32),
        ((2, 2, nx, nz), f32), ((2, 2, nx, nz), f32), ((2, 4, TILE, nz), f32), ((2, 4, TILE, nz), f32),
        ((2, 2, fields, ny + 2 * TILE, nz), f32), ((2, 2, fields, nx, nz), f32),
        ((2, 2, fields, nx + 2 * TILE, nz), f32), ((2, 4, wide, nz), f32), ((2, 4, wide, nz), f32),
        ((own, nz), f32), ((own, nz), f32),
        ((2 * tiles, 4, TILE, nz), i32), ((2 * tiles, 3, fields, TILE, nz), f32), ((2 * tiles, TILE, nz), f32),
        ((3, most, high, nz), f32),
    ]
    dma = pltpu.SemaphoreType.DMA
    out, change = pl.pallas_call(
        functools.partial(kernel, nx, ny, 1.0 / math.sqrt(cells)),
        out_shape=(
            jax.ShapeDtypeStruct((nspec, own, nz), f32),
            jax.ShapeDtypeStruct((high, nz), f32),
        ),
        in_specs=[hbm] * 5,
        out_specs=(vmem, vmem),
        scratch_shapes=[pltpu.VMEM(shape, kind) for shape, kind in shapes]
        + [
            dma((5,)), dma((3, 2)), dma((3, 2)), dma((6, 8)), dma((6, 8)), dma((3, most)), dma((3, most)),
        ],
        compiler_params=pltpu.CompilerParams(
            collective_id=0, has_side_effects=True, vmem_limit_bytes=26 * 1024 * 1024
        ),
    )(
        *[pltpu.with_memory_space_constraint(x, pltpu.HBM) for x in (
        provisional.reshape(nspec, own, nz),
        cut_flag.reshape(own, nz),
        cut_code.reshape(own, nz),
        volume_level.reshape(own, nz),
        area_level.reshape(own, nz))]
    )
    return out.reshape(provisional.shape), change[:nspec, 0]


def solution(mesh):
    spec = P("gx", "gy", "gz")
    wide = P(None, "gx", "gy", "gz")
    return jax.shard_map(
        per_device, mesh=mesh, in_specs=(wide, spec, spec, spec, spec), out_specs=(wide, P()), check_vma=False
    )
```

```python
import functools
import math

import jax
import jax.numpy as jnp
from jax import lax
from jax.experimental import pallas as pl
from jax.experimental.pallas import tpu as pltpu
from jax.sharding import PartitionSpec as P

CENTER = 8192
BLOCK = [(a, b, 9 * (a + 1) + 3 * (b + 1)) for a in (-1, 0, 1) for b in (-1, 0, 1)]
AXES = ("gx", "gy", "gz")
WAYS = [(1, 0), (-1, 0), (0, 1), (0, -1), (1, 1), (1, -1), (-1, 1), (-1, -1)]
MESH = pl.DeviceIdType.MESH
LANES = 128
TILE = 8


def pipelined(stages, count, hook=None):
    depth = len(stages)

    def step(i, lowest, highest):
        for k in reversed(range(lowest, highest)):
            stages[k](i - k)

    for i in range(min(depth - 1, count)):
        step(i, 0, i + 1)

    def body(i, carry):
        step(i, 0, depth)
        return carry

    low = depth - 1
    if hook is not None:
        at, action = hook
        lax.fori_loop(low, at, body, 0)
        action()
        low = at
    lax.fori_loop(low, count, body, 0)
    for i in range(count, count + depth - 1):
        step(i, i - count + 1, depth)


def kernel(
    nx, ny, scale,
    prov_h, flag_h, code_h, vol_h, area_h,
    out, change,
    raw, flag, code, vol, area,
    codes, wbuf, qbuf, packed, shifted, edge,
    zl_i, zr_i, zs_f, zl_f, zr_f,
    ys_i, yr_i, cs_i, cr_i, ys_p, yr_p, cs_p, cr_p,
    xr_r, ys_r, yr_r, cs_r, cr_r, xr_w, ys_w, yr_w, cs_w, cr_w, xr_q, ys_q, yr_q, cs_q, cr_q,
    volumes, weights, gathered, scaling, parts_i, parts_f, parts_e, peers,
    load, z_send, z_recv, send, recv, peer_send, peer_recv,
):
    nspec = prov_h.shape[0]
    pitch = ny + TILE
    tiles = ny // TILE
    here = {axis: lax.axis_index(axis) for axis in AXES}
    size = {axis: lax.axis_size(axis) for axis in AXES}
    lane = lax.broadcasted_iota(jnp.int32, (TILE, LANES), 1)
    odd = (lane & 1) == 1
    first_lane = lane == 0
    last_lane = lane == LANES - 1
    both_ends = first_lane | last_lane
    fields = nspec + 1
    flux = nspec

    inputs = [(flag_h, flag), (code_h, code), (vol_h, vol), (area_h, area), (prov_h, raw.at[pl.ds(0, nspec)])]
    loads = [pltpu.make_async_copy(src, dst, load.at[k]) for k, (src, dst) in enumerate(inputs)]
    for copy in loads:
        copy.start()

    def moved(axis, step):
        return lax.rem(here[axis] + (step + size[axis]), size[axis])

    barrier = pltpu.get_barrier_semaphore()
    near_x = lax.min(here["gx"], 1) + lax.min(size["gx"] - 1 - here["gx"], 1)
    near_y = lax.min(here["gy"], 1) + lax.min(size["gy"] - 1 - here["gy"], 1)
    near_z = lax.min(here["gz"], 1) + lax.min(size["gz"] - 1 - here["gz"], 1)
    greeted = (near_x + 1) * (near_y + 1) - 1 + near_z

    def greet(target):
        pl.semaphore_signal(barrier, inc=1, device_id=target, device_id_type=MESH)

    def first(x):
        return TILE + x * pitch

    def own_tile(x, k):
        row = (TILE + pitch + k * TILE) + x * pitch
        at = x * ny + k * TILE
        if isinstance(x, int):
            return row, at
        return pl.multiple_of(row, TILE), pl.multiple_of(at, TILE)

    def side(axis, step):
        return here[axis] < size[axis] - 1 if step > 0 else here[axis] > 0

    def exists(dx, dy):
        found = None
        for axis, step in (("gx", dx), ("gy", dy)):
            if step:
                there = side(axis, step)
                found = there if found is None else jnp.logical_and(found, there)
        return found

    below_z, above_z = side("gz", -1), side("gz", 1)
    for dx, dy in WAYS:
        pl.when(exists(dx, dy))(functools.partial(greet, {"gx": moved("gx", dx), "gy": moved("gy", dy)}))
    pl.when(below_z)(functools.partial(greet, {"gz": moved("gz", -1)}))
    pl.when(above_z)(functools.partial(greet, {"gz": moved("gz", 1)}))

    def edge_row(step):
        return ny - 1 if step > 0 else 0

    def halo_row(step):
        return ny if step > 0 else -1

    def blank(buf, low, high):
        zeros = jnp.zeros((ny, LANES), buf.dtype)
        row_zeros = jnp.zeros((TILE, LANES), buf.dtype)
        one = jnp.zeros((1, LANES), buf.dtype)

        def plane(step):
            def body(f, carry):
                buf[f, pl.ds(first(nx + 1 if step > 0 else 0), ny), :] = zeros
                return carry
            lax.fori_loop(low, high, body, 0)

        def row(step):
            def body(f, carry):
                for x in range(0, nx, TILE):
                    buf[f, pl.ds(first(x + 1) + halo_row(step), TILE, stride=pitch), :] = row_zeros
                return carry
            lax.fori_loop(low, high, body, 0)

        def corner(dx, dy):
            def body(f, carry):
                buf[f, pl.ds(first(nx + 1 if dx > 0 else 0) + halo_row(dy), 1), :] = one
                return carry
            lax.fori_loop(low, high, body, 0)

        for dx, dy in WAYS:
            action = functools.partial(plane, dx) if dy == 0 else (
                functools.partial(row, dy) if dx == 0 else functools.partial(corner, dx, dy))
            pl.when(jnp.logical_not(exists(dx, dy)))(action)

    class Unit:
        def __init__(self, number, buf, low, high, ys, yr, cs, cr, corner):
            self.buf, self.low, self.high = buf, low, high
            self.ys, self.yr, self.cs, self.cr, self.corner = ys, yr, cs, cr, corner
            n = high - low
            ends_of = {1: (nx, 0), -1: (1, nx + 1)}
            self.copies = []
            for k, (dx, dy) in enumerate(WAYS):
                if dy == 0:
                    here_x, there_x = ends_of[dx]
                    source = buf.at[pl.ds(low, n), pl.ds(first(here_x), ny), :]
                    landing = buf.at[pl.ds(low, n), pl.ds(first(there_x), ny), :]
                elif dx == 0:
                    way = 0 if dy > 0 else 1
                    source, landing = ys.at[way, pl.ds(low, n)], yr.at[way, pl.ds(low, n)]
                else:
                    source, landing = cs.at[corner, k - 4], cr.at[corner, k - 4]
                self.copies.append(
                    pltpu.make_async_remote_copy(
                        src_ref=source, dst_ref=landing,
                        send_sem=send.at[number, k], recv_sem=recv.at[number, k],
                        device_id={"gx": moved("gx", dx), "gy": moved("gy", dy)}, device_id_type=MESH,
                    )
                )

        def start(self):
            buf = self.buf
            for k, (dx, dy) in enumerate(WAYS):
                if dy == 0:
                    pl.when(exists(dx, dy))(self.copies[k].start)

            def gather(f, carry):
                for x in range(0, nx, TILE):
                    for way, step in ((0, 1), (1, -1)):
                        self.ys[way, f, pl.ds(x, TILE), :] = buf[f, pl.ds(first(x + 1) + edge_row(step), TILE, stride=pitch), :]
                for k, (dx, dy) in enumerate(WAYS[4:]):
                    row = first(nx if dx > 0 else 1) + edge_row(dy)
                    self.cs[self.corner, k, pl.ds(f - self.low, 1), :] = buf[f, pl.ds(row, 1), :]
                return carry

            lax.fori_loop(self.low, self.high, gather, 0)
            for k, (dx, dy) in enumerate(WAYS):
                if dy != 0:
                    pl.when(exists(dx, dy))(self.copies[k].start)

        def receive(self):
            buf = self.buf
            for k, (dx, dy) in enumerate(WAYS):
                pl.when(exists(-dx, -dy))(self.copies[k].wait_recv)

            def rows(way, step):
                def body(f, carry):
                    for x in range(0, nx, TILE):
                        buf[f, pl.ds(first(x + 1) + halo_row(-step), TILE, stride=pitch), :] = self.yr[way, f, pl.ds(x, TILE), :]
                    return carry
                lax.fori_loop(self.low, self.high, body, 0)

            def corner(k, dx, dy):
                def body(f, carry):
                    row = first(0 if dx > 0 else nx + 1) + halo_row(-dy)
                    buf[f, pl.ds(row, 1), :] = self.cr[self.corner, k, pl.ds(f - self.low, 1), :]
                    return carry
                lax.fori_loop(self.low, self.high, body, 0)

            for way, step in ((0, 1), (1, -1)):
                pl.when(exists(0, -step))(functools.partial(rows, way, step))
            for k, (dx, dy) in enumerate(WAYS[4:]):
                pl.when(exists(-dx, -dy))(functools.partial(corner, k, dx, dy))

        def finish(self):
            for k, (dx, dy) in enumerate(WAYS):
                pl.when(exists(dx, dy))(self.copies[k].wait_send)

    class Depth:
        def __init__(self, number, zs, zl, zr, buf, plane):
            self.zl, self.zr, self.buf, self.plane = zl, zr, buf, plane
            self.copies = [
                pltpu.make_async_remote_copy(
                    src_ref=zs, dst_ref=landing,
                    send_sem=z_send.at[number, way], recv_sem=z_recv.at[number, way],
                    device_id={"gz": moved("gz", step)}, device_id_type=MESH,
                )
                for way, (landing, step) in enumerate(((zl, 1), (zr, -1)))
            ]

        def start(self):
            pl.when(above_z)(self.copies[0].start)
            pl.when(below_z)(self.copies[1].start)

        def receive(self):
            pl.when(below_z)(self.copies[0].wait_recv)
            pl.when(above_z)(self.copies[1].wait_recv)
            zero = jnp.zeros((TILE, LANES), self.buf.dtype)

            def place(x, carry):
                for k in range(tiles):
                    row, at = own_tile(x, k)
                    low = jnp.where(below_z, pltpu.roll(self.zl[pl.ds(at, TILE), :], 1, 1), zero)
                    high = jnp.where(above_z, pltpu.roll(self.zr[pl.ds(at, TILE), :], LANES - 1, 1), zero)
                    self.buf[self.plane, pl.ds(row, TILE), :] = jnp.where(odd, low, high)
                return carry

            lax.fori_loop(0, nx, place, 0, unroll=8)

        def finish(self):
            pl.when(above_z)(self.copies[0].wait_send)
            pl.when(below_z)(self.copies[1].wait_send)

    class Faces:
        def __init__(self, number, buf, n, start, step, landing):
            self.buf, self.n, self.first_row, self.step = buf, n, start, step
            self.xr, self.ys, self.yr, self.cs, self.cr = landing
            self.copies = []
            for k, (dx, dy) in enumerate(WAYS):
                way = 0 if dx + dy > 0 else 1
                if dy == 0:
                    source = buf.at[pl.ds(0, n), pl.ds(start + (nx - 1 if dx > 0 else 0) * step, ny), :]
                    target = self.xr.at[way, pl.ds(0, n), pl.ds(TILE, ny), :]
                elif dx == 0:
                    source, target = self.ys.at[way], self.yr.at[way, pl.ds(0, n), pl.ds(TILE, nx), :]
                else:
                    source, target = self.cs.at[k - 4], self.cr.at[k - 4]
                self.copies.append(
                    pltpu.make_async_remote_copy(
                        src_ref=source, dst_ref=target,
                        send_sem=send.at[number, k], recv_sem=recv.at[number, k],
                        device_id={"gx": moved("gx", dx), "gy": moved("gy", dy)}, device_id_type=MESH,
                    )
                )

        def blank(self):
            zeros = jnp.zeros((TILE, LANES), jnp.float32)

            def borders(f, carry):
                for way in range(2):
                    for at in (0, TILE + ny):
                        self.xr[way, f, pl.ds(at, TILE), :] = zeros
                    for at in (0, TILE + nx):
                        self.yr[way, f, pl.ds(at, TILE), :] = zeros
                return carry

            lax.fori_loop(0, self.n, borders, 0)

            def clear(ref, way, extent):
                def body(f, carry):
                    ref[way, f, pl.ds(TILE, extent), :] = jnp.zeros((extent, LANES), jnp.float32)
                    return carry
                lax.fori_loop(0, self.n, body, 0)

            for way, step in ((0, 1), (1, -1)):
                pl.when(jnp.logical_not(exists(-step, 0)))(functools.partial(clear, self.xr, way, ny))
                pl.when(jnp.logical_not(exists(0, -step)))(functools.partial(clear, self.yr, way, nx))

        def start(self):
            buf, step = self.buf, self.step

            def gather(f, carry):
                for x in range(0, nx, TILE):
                    for way, toward in ((0, 1), (1, -1)):
                        row = self.first_row + x * step + edge_row(toward)
                        self.ys[way, f, pl.ds(x, TILE), :] = buf[f, pl.ds(row, TILE, stride=step), :]
                for k, (dx, dy) in enumerate(WAYS[4:]):
                    row = self.first_row + (nx - 1 if dx > 0 else 0) * step + edge_row(dy)
                    self.cs[k, pl.ds(f, 1), :] = buf[f, pl.ds(row, 1), :]
                return carry

            for k in range(2):
                pl.when(exists(*WAYS[k]))(self.copies[k].start)
            lax.fori_loop(0, self.n, gather, 0)
            for k in range(2, 8):
                pl.when(exists(*WAYS[k]))(self.copies[k].start)

        def receive(self):
            for k, (dx, dy) in enumerate(WAYS):
                pl.when(exists(-dx, -dy))(self.copies[k].wait_recv)

            def corner(k, dx, dy):
                way = 0 if dy > 0 else 1
                at = TILE - 1 if dx > 0 else TILE + nx

                def body(f, carry):
                    self.yr[way, f, pl.ds(at, 1), :] = self.cr[k, pl.ds(f, 1), :]
                    return carry
                lax.fori_loop(0, self.n, body, 0)

            for k, (dx, dy) in enumerate(WAYS[4:]):
                pl.when(exists(-dx, -dy))(functools.partial(corner, k, dx, dy))

        def finish(self):
            for k, (dx, dy) in enumerate(WAYS):
                pl.when(exists(dx, dy))(self.copies[k].wait_send)

    def pad_zeros(buf, n):
        zeros = jnp.zeros((TILE, LANES), jnp.float32)

        def body(f, carry):
            for p in range(nx + 3):
                buf[f, pl.ds(p * pitch, TILE), :] = zeros
            for p in (0, nx + 1):
                for k in range(tiles):
                    buf[f, pl.ds(first(p) + k * TILE, TILE), :] = zeros
            return carry

        lax.fori_loop(0, n, body, 0)

    code_z = Depth(0, edge, zl_i, zr_i, codes, 1)
    code_own = Unit(0, codes, 0, 1, ys_i, yr_i, cs_i, cr_i, 0)
    code_packed = Unit(1, codes, 1, 2, ys_i, yr_i, cs_i, cr_i, 1)
    raw_z = Depth(1, zs_f.at[0], zl_f.at[0], zr_f.at[0], packed, 0)
    raw_all = Faces(2, raw, fields, 0, ny, (xr_r, ys_r, yr_r, cs_r, cr_r))
    raw_packed = Unit(3, packed, 0, 1, ys_p, yr_p, cs_p, cr_p, 0)
    w_z = Depth(2, zs_f.at[1], zl_f.at[1], zr_f.at[1], packed, 1)
    w_all = Faces(4, weights, 1, 0, ny, (xr_w, ys_w, yr_w, cs_w, cr_w))
    w_packed = Unit(5, packed, 1, 2, ys_p, yr_p, cs_p, cr_p, 1)
    q_z = Depth(3, zs_f.at[2], zl_f.at[2], zr_f.at[2], packed, 2)
    q_all = Faces(6, qbuf, nspec, first(1), pitch, (xr_q, ys_q, yr_q, cs_q, cr_q))
    q_packed = Unit(7, packed, 2, 3, ys_p, yr_p, cs_p, cr_p, 2)
    everything = [
        code_z, code_own, code_packed, raw_z, raw_all, raw_packed, w_z, w_all, w_packed, q_z, q_all, q_packed,
    ]

    def total_over(value):
        for number, axis in enumerate(AXES):
            n, me = size[axis], here[axis]
            peers[number, me] = value
            for k in range(1, n):
                def copy(way, slot):
                    block = peers.at[number, lax.max(lax.min(slot, n - 1), 0)]
                    return pltpu.make_async_remote_copy(
                        src_ref=block, dst_ref=block,
                        send_sem=peer_send.at[number, k, way], recv_sem=peer_recv.at[number, k, way],
                        device_id={axis: moved(axis, 1 if way == 0 else -1)}, device_id_type=MESH,
                    )

                up, down = me - k + 1, me + k - 1
                sends = [(jnp.logical_and(up >= 0, me < n - 1), copy(0, up)), (jnp.logical_and(down < n, me > 0), copy(1, down))]
                lands = [(me - k >= 0, copy(0, me - k)), (me + k < n, copy(1, me + k))]
                for there, block in sends:
                    pl.when(there)(block.start)
                yield
                for there, block in lands:
                    pl.when(there)(block.wait_recv)
                for there, block in sends:
                    pl.when(there)(block.wait_send)
            value = peers[number, 0]
            for k in range(1, n):
                value = value + peers[number, k]
        change[...] = jnp.broadcast_to(jnp.sum(value, axis=1, keepdims=True) * scale, change.shape)

    def fractions(own):
        is_cut = flag[own, :] == 1
        volume = jnp.where(is_cut, vol[own, :], 256).astype(jnp.float32) * (1.0 / 256.0)
        face = jnp.where(is_cut, area[own, :], 256).astype(jnp.float32) * (1.0 / 256.0)
        return volume, face

    def fill(x, carry):
        for k in range(tiles):
            row, at = own_tile(x, k)
            own = pl.ds(at, TILE)
            value = jnp.where(flag[own, :] == 1, code[own, :] | CENTER, CENTER)
            codes[0, pl.ds(row, TILE), :] = value
            low = jnp.broadcast_to(value[:, :1], (TILE, LANES))
            high = lax.shift_right_logical(jnp.broadcast_to(value[:, LANES - 1:], (TILE, LANES)), 2)
            edge[own, :] = jnp.where(odd, low, high)
        return carry

    def shift(x, carry):
        for k in range(tiles):
            row, at = own_tile(x, k)
            own = pl.ds(at, TILE)
            value = codes[0, pl.ds(row, TILE), :]
            shifted[0, own, :] = jnp.where(first_lane, 0, pltpu.roll(value, 1, 1))
            shifted[1, own, :] = jnp.where(last_lane, 0, pltpu.roll(value, LANES - 1, 1))
        return carry

    def prepare(x, totals):
        for k in range(tiles):
            _, at = own_tile(x, k)
            own = pl.ds(at, TILE)
            volume, face = fractions(own)
            volumes[own, :] = volume
            raw[nspec, own, :] = face
            totals = tuple(totals[s] + volume * raw[s, own, :] for s in range(nspec))
        return totals

    def raw_pack(x, carry):
        for k in range(tiles):
            _, at = own_tile(x, k)
            own = pl.ds(at, TILE)
            zs_f[0, own, :] = pack([raw[f, own, :] for f in range(fields)], 0)
        return carry

    def masked_sums(taps, low, high):
        zero = jnp.zeros((TILE, LANES), jnp.float32)
        sums = [[None] * (high - low) for _ in range(3)]
        for sources, position, value_of in taps:
            present = [
                None if source is None else (source & (1 << (position + k))) != 0 for k, source in enumerate(sources)
            ]
            for f in range(low, high):
                value = value_of(f)
                for k in range(3):
                    term = value if present[k] is None else jnp.where(present[k], value, zero)
                    old = sums[k][f - low]
                    sums[k][f - low] = term if old is None else old + term
        return sums

    def keep_sums(slot, sums, low):
        for m in range(3):
            for f, value in enumerate(sums[m]):
                parts_f[slot, m, low + f] = value

    def merged(slot, f, wrap):
        if wrap:
            up, down = pltpu.roll(parts_f[slot, 2, f], 1, 1), pltpu.roll(parts_f[slot, 0, f], LANES - 1, 1)
            up, down = jnp.where(first_lane, 0.0, up), jnp.where(last_lane, 0.0, down)
        else:
            up, down = pltpu.roll(parts_f[slot, 2, f], LANES - 1, 1), pltpu.roll(parts_f[slot, 0, f], 1, 1)
        return parts_f[slot, 1, f] + up + down

    def packed_taps(row, step, source, value_of):
        zero = jnp.zeros((TILE, LANES), jnp.float32)
        total = None
        for a, b, position in BLOCK:
            near = pl.ds(row + step * (a * pitch + b), TILE)
            term = jnp.where((source(near) & (1 << position)) != 0, value_of(near), zero)
            total = term if total is None else total + term
        return total

    def pack(values, lowest):
        packed = jnp.zeros((TILE, LANES), jnp.float32)
        for k, value in enumerate(values):
            f = lowest + k
            packed = jnp.where((lane == 2 * f) | (lane == 2 * f + 1), pltpu.roll(value, 2 * f + 1, 1), packed)
        return packed

    quad = 2
    members = [(k, k // tiles, k % tiles) for k in range(quad * tiles)]

    def count_taps(g):
        for k, x, y in members:
            row, at = own_tile(g * quad + x, y)
            sums = [None] * 3
            total = None
            for a, b, position in BLOCK:
                near = pl.ds(row - a * pitch - b, TILE)
                value = codes[0, near, :]
                value = value if position == 0 else lax.shift_right_logical(value, position)
                for m in range(3):
                    term = value & (1 << m)
                    sums[m] = term if sums[m] is None else sums[m] + term
                value = codes[1, near, :]
                value = value if position == 0 else lax.shift_right_logical(value, position)
                total = value & 1 if total is None else total + (value & 1)
            for m in range(3):
                parts_i[k, m] = sums[m]
            parts_i[k, 3] = total

    def weigh(g):
        for k, x, y in members:
            row, at = own_tile(g * quad + x, y)
            own = pl.ds(at, TILE)
            from_end = pltpu.roll(parts_i[k, 3], LANES - 1, 1)
            from_left = pltpu.roll(lax.shift_right_logical(parts_i[k, 2], 2), 1, 1)
            from_right = pltpu.roll(parts_i[k, 0], LANES - 1, 1)
            counted = lax.shift_right_logical(parts_i[k, 1], 1)
            counted = counted + jnp.where(first_lane, from_end, from_left) + jnp.where(last_lane, from_end, from_right)
            share = 1.0 / counted.astype(jnp.float32)
            scaling[own, :] = raw[nspec, own, :] * share
            weight = volumes[own, :] * share
            weights[0, own, :] = weight
            for f in range(fields):
                wbuf[f, pl.ds(row, TILE), :] = weight * raw[f, own, :]

    def weigh_pack(g):
        for k, x, y in members:
            row, at = own_tile(g * quad + x, y)
            own = pl.ds(at, TILE)
            value = weights[0, own, :]
            low = jnp.broadcast_to(value[:, :1], (TILE, LANES))
            high = jnp.broadcast_to(value[:, LANES - 1:], (TILE, LANES))
            zs_f[1, own, :] = jnp.where(odd, low, high)

    def own_row(t):
        x, k = lax.div(t, tiles), lax.rem(t, tiles)
        row = (TILE + pitch) + x * pitch + k * TILE
        if isinstance(t, int):
            return int(row), t * TILE
        return pl.multiple_of(row, TILE), pl.multiple_of(t * TILE, TILE)

    def reader(buf, near):
        return lambda f: buf[f, near, :]

    def weighed(buf, factors, near):
        factor = factors[0, near, :]
        return lambda f: buf[f, near, :] * factor

    def gather_main(t):
        row, at = own_tile(t // tiles, t % tiles) if isinstance(t, int) else own_row(t)
        own = pl.ds(at, TILE)
        right, left, middle = shifted[0, own, :], shifted[1, own, :], codes[0, pl.ds(row, TILE), :]
        taps = []
        for a, b, position in BLOCK:
            center = None if position == 12 else middle
            taps.append(((left, center, right), position, reader(wbuf, pl.ds(row + a * pitch + b, TILE))))
        keep_sums(0, masked_sums(taps, 0, fields), 0)

    def gather_close(t):
        row, at = own_tile(t // tiles, t % tiles) if isinstance(t, int) else own_row(t)
        for f in range(nspec):
            qbuf[f, pl.ds(row, TILE), :] = merged(0, f, False)
        gathered[pl.ds(at, TILE), :] = merged(0, flux, False)

    def gather_strip(j):
        x = j * TILE
        for way, (b, y) in enumerate(((-1, 0), (1, ny - 1))):
            where = pl.ds(x * ny + y, TILE, stride=ny)
            right, left = shifted[0, where, :], shifted[1, where, :]
            middle = codes[0, pl.ds(first(1) + x * pitch + y, TILE, stride=pitch), :]
            taps = []
            for a in (-1, 0, 1):
                near = pl.ds(TILE + x + a, TILE)
                taps.append(((left, middle, right), 9 * (a + 1) + 3 * (b + 1), weighed(yr_r.at[way], yr_w.at[way], near)))
            keep_sums(way, masked_sums(taps, 0, fields), 0)

    def gather_strip_close(j):
        x = j * TILE
        for way, y in enumerate((0, ny - 1)):
            rows = pl.ds(first(1) + x * pitch + y, TILE, stride=pitch)
            for f in range(nspec):
                qbuf[f, rows, :] = qbuf[f, rows, :] + merged(way, f, False)
            where = pl.ds(x * ny + y, TILE, stride=ny)
            gathered[where, :] = gathered[where, :] + merged(way, flux, False)

    def gather_plane(way):
        a, x = ((-1, 0), (1, nx - 1))[way]
        for k in range(tiles):
            row, at = own_tile(x, k)
            own = pl.ds(at, TILE)
            right, left, middle = shifted[0, own, :], shifted[1, own, :], codes[0, pl.ds(row, TILE), :]
            taps = []
            for b in (-1, 0, 1):
                near = pl.ds(TILE + k * TILE + b, TILE)
                taps.append(((left, middle, right), 9 * (a + 1) + 3 * (b + 1), weighed(xr_r.at[way], xr_w.at[way], near)))
            keep_sums(way * tiles + k, masked_sums(taps, 0, fields), 0)

    def gather_plane_close(way):
        x = (0, nx - 1)[way]
        for k in range(tiles):
            row, at = own_tile(x, k)
            for f in range(nspec):
                qbuf[f, pl.ds(row, TILE), :] = qbuf[f, pl.ds(row, TILE), :] + merged(way * tiles + k, f, False)
            own = pl.ds(at, TILE)
            gathered[own, :] = gathered[own, :] + merged(way * tiles + k, flux, False)

    def gather_ends(g):
        for k, x, y in members:
            row, at = own_tile(g * quad + x, y)
            value = edge[pl.ds(at, TILE), :]
            parts_e[k] = packed_taps(
                row, 1, lambda near: value, lambda near: packed[0, near, :] * packed[1, near, :])

    def quotas(g):
        for k, x, y in members:
            row, at = own_tile(g * quad + x, y)
            value = parts_e[k]

            def spread(f):
                return jnp.where(both_ends, pltpu.roll(value, LANES - 1 - 2 * f, 1), 0.0)

            inverted = 1.0 / (gathered[pl.ds(at, TILE), :] + spread(flux))
            for f in range(nspec):
                qbuf[f, pl.ds(row, TILE), :] = (qbuf[f, pl.ds(row, TILE), :] + spread(f)) * inverted

    def quota_pack(g):
        for k, x, y in members:
            row, at = own_tile(g * quad + x, y)
            zs_f[2, pl.ds(at, TILE), :] = pack([qbuf[f, pl.ds(row, TILE), :] for f in range(nspec)], 0)

    def scatter_main(t):
        row, at = own_tile(t // tiles, t % tiles) if isinstance(t, int) else own_row(t)
        taps = []
        for a, b, position in BLOCK:
            near = pl.ds(row - a * pitch - b, TILE)
            source = codes[0, near, :]
            center = None if position == 12 else source
            taps.append(((source, center, source), position, reader(qbuf, near)))
        keep_sums(0, masked_sums(taps, 0, nspec), 0)

    def scatter_close(t):
        row, at = own_tile(t // tiles, t % tiles) if isinstance(t, int) else own_row(t)
        for f in range(nspec):
            out[f, pl.ds(at, TILE), :] = merged(0, f, True)

    def scatter_strip(j):
        x = j * TILE
        for way, (b, y) in enumerate(((1, -1), (-1, ny))):
            taps = []
            for a in (-1, 0, 1):
                source = codes[0, pl.ds(first(1) + (x - a) * pitch + y, TILE, stride=pitch), :]
                taps.append(((source, source, source), 9 * (a + 1) + 3 * (b + 1), reader(yr_q.at[way], pl.ds(TILE + x - a, TILE))))
            keep_sums(way, masked_sums(taps, 0, nspec), 0)

    def scatter_strip_close(j):
        for way, y in enumerate((0, ny - 1)):
            where = pl.ds(j * TILE * ny + y, TILE, stride=ny)
            for f in range(nspec):
                out[f, where, :] = out[f, where, :] + merged(way, f, True)

    def scatter_plane(way):
        a, x = ((1, 0), (-1, nx + 1))[way]
        for k in range(tiles):
            taps = []
            for b in (-1, 0, 1):
                source = codes[0, pl.ds(first(x) + k * TILE - b, TILE), :]
                taps.append(((source, source, source), 9 * (a + 1) + 3 * (b + 1), reader(xr_q.at[way], pl.ds(TILE + k * TILE - b, TILE))))
            keep_sums(way * tiles + k, masked_sums(taps, 0, nspec), 0)

    def scatter_plane_close(way):
        x = (0, nx - 1)[way]
        for k in range(tiles):
            row, at = own_tile(x, k)
            for f in range(nspec):
                out[f, pl.ds(at, TILE), :] = out[f, pl.ds(at, TILE), :] + merged(way * tiles + k, f, True)

    def scatter_ends(g):
        for k, x, y in members:
            row, at = own_tile(g * quad + x, y)
            parts_e[k] = packed_taps(row, -1, lambda near: codes[1, near, :], lambda near: packed[2, near, :])

    def finals(g):
        for k, x, y in members:
            row, at = own_tile(g * quad + x, y)
            own = pl.ds(at, TILE)
            value, factor = parts_e[k], scaling[own, :]
            for f in range(nspec):
                spread = jnp.where(both_ends, pltpu.roll(value, LANES - 1 - 2 * f, 1), 0.0)
                out[f, own, :] = factor * (out[f, own, :] + spread)

    blank(codes, 0, 2)
    loads[0].wait()
    loads[1].wait()
    lax.fori_loop(0, nx, fill, 0, unroll=8)
    pl.semaphore_wait(barrier, greeted)
    code_z.start()
    code_own.start()
    for copy in loads[2:]:
        copy.wait()
    totals = tuple(jnp.zeros((TILE, LANES), jnp.float32) for _ in range(nspec))
    totals = lax.fori_loop(0, nx, prepare, totals, unroll=2)
    local = jnp.concatenate(
        [jnp.sum(total, axis=0, keepdims=True) for total in totals]
        + [jnp.zeros((peers.shape[2] - nspec, LANES), jnp.float32)],
        axis=0,
    )
    reduction = total_over(local)
    code_z.receive()
    code_packed.start()
    raw_all.start()
    next(reduction, None)
    lax.fori_loop(0, nx, raw_pack, 0, unroll=4)
    raw_z.start()
    lax.fori_loop(0, nx, shift, 0, unroll=8)
    blank(packed, 0, 3)
    raw_all.blank()
    w_all.blank()
    q_all.blank()
    pad_zeros(wbuf, fields)
    pad_zeros(qbuf, nspec)
    code_own.receive()
    code_packed.receive()
    raw_z.receive()
    raw_packed.start()
    next(reduction, None)
    pipelined([count_taps, weigh, weigh_pack], nx // quad)
    w_z.start()
    w_all.start()
    next(reduction, None)

    def relay_w():
        w_z.receive()
        w_packed.start()
        next(reduction, None)

    pipelined([gather_main, gather_close], nx * tiles, (nx * tiles // 4, relay_w))
    raw_all.receive()
    raw_packed.receive()
    w_all.receive()
    w_packed.receive()
    next(reduction, None)
    pipelined([gather_strip, gather_strip_close], nx // TILE)
    for stage in (gather_plane, gather_plane_close):
        stage(0)
        stage(1)
    pipelined([gather_ends, quotas, quota_pack], nx // quad)
    q_z.start()
    q_all.start()
    next(reduction, None)

    def relay_q():
        q_z.receive()
        q_packed.start()
        next(reduction, None)

    pipelined([scatter_main, scatter_close], nx * tiles, (nx * tiles // 4, relay_q))
    for _ in reduction:
        pass
    q_all.receive()
    q_packed.receive()
    pipelined([scatter_strip, scatter_strip_close], nx // TILE)
    for stage in (scatter_plane, scatter_plane_close):
        stage(0)
        stage(1)
    pipelined([scatter_ends, finals], nx // quad)
    for part in everything:
        part.finish()


def per_device(provisional, cut_flag, cut_code, volume_level, area_level):
    nspec, nx, ny, nz = provisional.shape
    assert nz == LANES and ny % TILE == 0 and nx % TILE == 0
    own = nx * ny
    tiles = ny // TILE
    rows = 2 * TILE + (nx + 2) * (ny + TILE)
    most = max(lax.axis_size(axis) for axis in AXES)
    cells = own * nz * math.prod(lax.axis_size(axis) for axis in AXES)
    fields = nspec + 1
    f32, i32 = jnp.float32, jnp.int32
    vmem = pl.BlockSpec(memory_space=pltpu.VMEM)
    hbm = pl.BlockSpec(memory_space=pltpu.HBM)
    shapes = [
        ((fields, own, nz), f32), ((own, nz), i32), ((own, nz), i32), ((own, nz), i32), ((own, nz), i32),
        ((2, rows, nz), i32), ((fields, rows, nz), f32), ((nspec, rows, nz), f32), ((3, rows, nz), f32),
        ((2, own, nz), i32), ((own, nz), i32),
        ((own, nz), i32), ((own, nz), i32),
        ((3, own, nz), f32), ((3, own, nz), f32), ((3, own, nz), f32),
        ((2, 2, nx, nz), i32), ((2, 2, nx, nz), i32), ((2, 4, TILE, nz), i32), ((2, 4, TILE, nz), i32),
        ((2, 3, nx, nz), f32), ((2, 3, nx, nz), f32), ((3, 4, TILE, nz), f32), ((3, 4, TILE, nz), f32),
    ]
    for n in (fields, 1, nspec):
        high = -(-n // TILE) * TILE
        shapes += [
            ((2, n, ny + 2 * TILE, nz), f32), ((2, n, nx, nz), f32), ((2, n, nx + 2 * TILE, nz), f32),
            ((4, high, nz), f32), ((4, high, nz), f32),
        ]
    high = -(-nspec // TILE) * TILE
    shapes += [
        ((own, nz), f32), ((1, own, nz), f32), ((own, nz), f32), ((own, nz), f32),
        ((2 * tiles, 4, TILE, nz), i32), ((2 * tiles, 3, fields, TILE, nz), f32), ((2 * tiles, TILE, nz), f32),
        ((3, most, high, nz), f32),
    ]
    dma = pltpu.SemaphoreType.DMA
    out, change = pl.pallas_call(
        functools.partial(kernel, nx, ny, 1.0 / math.sqrt(cells)),
        out_shape=(
            jax.ShapeDtypeStruct((nspec, own, nz), f32),
            jax.ShapeDtypeStruct((high, nz), f32),
        ),
        in_specs=[hbm] * 5,
        out_specs=(vmem, vmem),
        scratch_shapes=[pltpu.VMEM(shape, kind) for shape, kind in shapes]
        + [
            dma((5,)), dma((4, 2)), dma((4, 2)), dma((8, 8)), dma((8, 8)), dma((3, most, 2)), dma((3, most, 2)),
        ],
        compiler_params=pltpu.CompilerParams(
            collective_id=0, has_side_effects=True, vmem_limit_bytes=26 * 1024 * 1024
        ),
    )(
        *[pltpu.with_memory_space_constraint(x, pltpu.HBM) for x in (
        provisional.reshape(nspec, own, nz),
        cut_flag.reshape(own, nz),
        cut_code.reshape(own, nz),
        volume_level.reshape(own, nz),
        area_level.reshape(own, nz))]
    )
    return out.reshape(provisional.shape), change[:nspec, 0]


def solution(mesh):
    spec = P("gx", "gy", "gz")
    wide = P(None, "gx", "gy", "gz")
    return jax.shard_map(
        per_device, mesh=mesh, in_specs=(wide, spec, spec, spec, spec), out_specs=(wide, P()), check_vma=False
    )
```

```python
import functools
import math

import jax
import jax.numpy as jnp
from jax import lax
from jax.experimental import pallas as pl
from jax.experimental.pallas import tpu as pltpu
from jax.sharding import PartitionSpec as P

CENTER = 8192
BLOCK = [(a, b, 9 * (a + 1) + 3 * (b + 1)) for a in (-1, 0, 1) for b in (-1, 0, 1)]
AXES = ("gx", "gy", "gz")
WAYS = [(1, 0), (-1, 0), (0, 1), (0, -1), (1, 1), (1, -1), (-1, 1), (-1, -1)]
MESH = pl.DeviceIdType.MESH
LANES = 128
TILE = 8


def pipelined(stages, count, hook=None):
    depth = len(stages)

    def step(i, lowest, highest):
        for k in reversed(range(lowest, highest)):
            stages[k](i - k)

    for i in range(min(depth - 1, count)):
        step(i, 0, i + 1)

    def body(i, carry):
        step(i, 0, depth)
        return carry

    low = depth - 1
    if hook is not None:
        at, action = hook
        lax.fori_loop(low, at, body, 0)
        action()
        low = at
    lax.fori_loop(low, count, body, 0)
    for i in range(count, count + depth - 1):
        step(i, i - count + 1, depth)


def kernel(
    nx, ny, scale,
    prov_h, flag_h, code_h, vol_h, area_h,
    out, change,
    raw, flag, code, vol, area,
    codes, wbuf, qbuf, packed, shifted, edge,
    zl_i, zr_i, zs_f, zl_f, zr_f,
    ys_i, yr_i, cs_i, cr_i, ys_p, yr_p, cs_p, cr_p,
    xr_r, ys_r, yr_r, cs_r, cr_r, xr_w, ys_w, yr_w, cs_w, cr_w, xr_q, ys_q, yr_q, cs_q, cr_q,
    volumes, weights, gathered, scaling, parts_i, parts_f, parts_e, peers,
    load, z_send, z_recv, send, recv, peer_send, peer_recv,
):
    nspec = prov_h.shape[0]
    pitch = ny + TILE
    tiles = ny // TILE
    here = {axis: lax.axis_index(axis) for axis in AXES}
    size = {axis: lax.axis_size(axis) for axis in AXES}
    lane = lax.broadcasted_iota(jnp.int32, (TILE, LANES), 1)
    odd = (lane & 1) == 1
    first_lane = lane == 0
    last_lane = lane == LANES - 1
    both_ends = first_lane | last_lane
    fields = nspec + 1
    flux = nspec

    inputs = [(flag_h, flag), (code_h, code), (vol_h, vol), (area_h, area), (prov_h, raw.at[pl.ds(0, nspec)])]
    loads = [pltpu.make_async_copy(src, dst, load.at[k]) for k, (src, dst) in enumerate(inputs)]
    for copy in loads:
        copy.start()

    def moved(axis, step):
        return lax.rem(here[axis] + (step + size[axis]), size[axis])

    barrier = pltpu.get_barrier_semaphore()
    near_x = lax.min(here["gx"], 1) + lax.min(size["gx"] - 1 - here["gx"], 1)
    near_y = lax.min(here["gy"], 1) + lax.min(size["gy"] - 1 - here["gy"], 1)
    near_z = lax.min(here["gz"], 1) + lax.min(size["gz"] - 1 - here["gz"], 1)
    greeted = (near_x + 1) * (near_y + 1) - 1 + near_z
    for axis, near in (("gx", near_x), ("gy", near_y), ("gz", near_z)):
        if size[axis] > 4:
            greeted = greeted + (size[axis] - 1 - near)

    def greet(target):
        pl.semaphore_signal(barrier, inc=1, device_id=target, device_id_type=MESH)

    def first(x):
        return TILE + x * pitch

    def own_tile(x, k):
        row = (TILE + pitch + k * TILE) + x * pitch
        at = x * ny + k * TILE
        if isinstance(x, int):
            return row, at
        return pl.multiple_of(row, TILE), pl.multiple_of(at, TILE)

    def side(axis, step):
        return here[axis] < size[axis] - 1 if step > 0 else here[axis] > 0

    def exists(dx, dy):
        found = None
        for axis, step in (("gx", dx), ("gy", dy)):
            if step:
                there = side(axis, step)
                found = there if found is None else jnp.logical_and(found, there)
        return found

    below_z, above_z = side("gz", -1), side("gz", 1)
    for dx, dy in WAYS:
        pl.when(exists(dx, dy))(functools.partial(greet, {"gx": moved("gx", dx), "gy": moved("gy", dy)}))
    pl.when(below_z)(functools.partial(greet, {"gz": moved("gz", -1)}))
    pl.when(above_z)(functools.partial(greet, {"gz": moved("gz", 1)}))
    for axis in AXES:
        if size[axis] > 4:
            for k in range(2, size[axis]):
                pl.when(here[axis] >= k)(functools.partial(greet, {axis: moved(axis, -k)}))
                pl.when(here[axis] + k < size[axis])(functools.partial(greet, {axis: moved(axis, k)}))

    def edge_row(step):
        return ny - 1 if step > 0 else 0

    def halo_row(step):
        return ny if step > 0 else -1

    def blank(buf, low, high):
        zeros = jnp.zeros((ny, LANES), buf.dtype)
        row_zeros = jnp.zeros((TILE, LANES), buf.dtype)
        one = jnp.zeros((1, LANES), buf.dtype)

        def plane(step):
            def body(f, carry):
                buf[f, pl.ds(first(nx + 1 if step > 0 else 0), ny), :] = zeros
                return carry
            lax.fori_loop(low, high, body, 0)

        def row(step):
            def body(f, carry):
                for x in range(0, nx, TILE):
                    buf[f, pl.ds(first(x + 1) + halo_row(step), TILE, stride=pitch), :] = row_zeros
                return carry
            lax.fori_loop(low, high, body, 0)

        def corner(dx, dy):
            def body(f, carry):
                buf[f, pl.ds(first(nx + 1 if dx > 0 else 0) + halo_row(dy), 1), :] = one
                return carry
            lax.fori_loop(low, high, body, 0)

        for dx, dy in WAYS:
            action = functools.partial(plane, dx) if dy == 0 else (
                functools.partial(row, dy) if dx == 0 else functools.partial(corner, dx, dy))
            pl.when(jnp.logical_not(exists(dx, dy)))(action)

    class Unit:
        def __init__(self, number, buf, low, high, ys, yr, cs, cr, corner):
            self.buf, self.low, self.high = buf, low, high
            self.ys, self.yr, self.cs, self.cr, self.corner = ys, yr, cs, cr, corner
            n = high - low
            ends_of = {1: (nx, 0), -1: (1, nx + 1)}
            self.copies = []
            for k, (dx, dy) in enumerate(WAYS):
                if dy == 0:
                    here_x, there_x = ends_of[dx]
                    source = buf.at[pl.ds(low, n), pl.ds(first(here_x), ny), :]
                    landing = buf.at[pl.ds(low, n), pl.ds(first(there_x), ny), :]
                elif dx == 0:
                    way = 0 if dy > 0 else 1
                    source, landing = ys.at[way, pl.ds(low, n)], yr.at[way, pl.ds(low, n)]
                else:
                    source, landing = cs.at[corner, k - 4], cr.at[corner, k - 4]
                self.copies.append(
                    pltpu.make_async_remote_copy(
                        src_ref=source, dst_ref=landing,
                        send_sem=send.at[number, k], recv_sem=recv.at[number, k],
                        device_id={"gx": moved("gx", dx), "gy": moved("gy", dy)}, device_id_type=MESH,
                    )
                )

        def start(self):
            buf = self.buf
            for k, (dx, dy) in enumerate(WAYS):
                if dy == 0:
                    pl.when(exists(dx, dy))(self.copies[k].start)

            def gather(f, carry):
                for x in range(0, nx, TILE):
                    for way, step in ((0, 1), (1, -1)):
                        self.ys[way, f, pl.ds(x, TILE), :] = buf[f, pl.ds(first(x + 1) + edge_row(step), TILE, stride=pitch), :]
                for k, (dx, dy) in enumerate(WAYS[4:]):
                    row = first(nx if dx > 0 else 1) + edge_row(dy)
                    self.cs[self.corner, k, pl.ds(f - self.low, 1), :] = buf[f, pl.ds(row, 1), :]
                return carry

            lax.fori_loop(self.low, self.high, gather, 0)
            for k, (dx, dy) in enumerate(WAYS):
                if dy != 0:
                    pl.when(exists(dx, dy))(self.copies[k].start)

        def receive(self):
            buf = self.buf
            for k, (dx, dy) in enumerate(WAYS):
                pl.when(exists(-dx, -dy))(self.copies[k].wait_recv)

            def rows(way, step):
                def body(f, carry):
                    for x in range(0, nx, TILE):
                        buf[f, pl.ds(first(x + 1) + halo_row(-step), TILE, stride=pitch), :] = self.yr[way, f, pl.ds(x, TILE), :]
                    return carry
                lax.fori_loop(self.low, self.high, body, 0)

            def corner(k, dx, dy):
                def body(f, carry):
                    row = first(0 if dx > 0 else nx + 1) + halo_row(-dy)
                    buf[f, pl.ds(row, 1), :] = self.cr[self.corner, k, pl.ds(f - self.low, 1), :]
                    return carry
                lax.fori_loop(self.low, self.high, body, 0)

            for way, step in ((0, 1), (1, -1)):
                pl.when(exists(0, -step))(functools.partial(rows, way, step))
            for k, (dx, dy) in enumerate(WAYS[4:]):
                pl.when(exists(-dx, -dy))(functools.partial(corner, k, dx, dy))

        def finish(self):
            for k, (dx, dy) in enumerate(WAYS):
                pl.when(exists(dx, dy))(self.copies[k].wait_send)

    class Depth:
        def __init__(self, number, zs, zl, zr, buf, plane):
            self.zl, self.zr, self.buf, self.plane = zl, zr, buf, plane
            self.copies = [
                pltpu.make_async_remote_copy(
                    src_ref=zs, dst_ref=landing,
                    send_sem=z_send.at[number, way], recv_sem=z_recv.at[number, way],
                    device_id={"gz": moved("gz", step)}, device_id_type=MESH,
                )
                for way, (landing, step) in enumerate(((zl, 1), (zr, -1)))
            ]

        def start(self):
            pl.when(above_z)(self.copies[0].start)
            pl.when(below_z)(self.copies[1].start)

        def receive(self):
            pl.when(below_z)(self.copies[0].wait_recv)
            pl.when(above_z)(self.copies[1].wait_recv)
            zero = jnp.zeros((TILE, LANES), self.buf.dtype)

            def place(x, carry):
                for k in range(tiles):
                    row, at = own_tile(x, k)
                    low = jnp.where(below_z, pltpu.roll(self.zl[pl.ds(at, TILE), :], 1, 1), zero)
                    high = jnp.where(above_z, pltpu.roll(self.zr[pl.ds(at, TILE), :], LANES - 1, 1), zero)
                    self.buf[self.plane, pl.ds(row, TILE), :] = jnp.where(odd, low, high)
                return carry

            lax.fori_loop(0, nx, place, 0, unroll=8)

        def finish(self):
            pl.when(above_z)(self.copies[0].wait_send)
            pl.when(below_z)(self.copies[1].wait_send)

    class Faces:
        def __init__(self, number, buf, n, start, step, landing):
            self.buf, self.n, self.first_row, self.step = buf, n, start, step
            self.xr, self.ys, self.yr, self.cs, self.cr = landing
            self.copies = []
            for k, (dx, dy) in enumerate(WAYS):
                way = 0 if dx + dy > 0 else 1
                if dy == 0:
                    source = buf.at[pl.ds(0, n), pl.ds(start + (nx - 1 if dx > 0 else 0) * step, ny), :]
                    target = self.xr.at[way, pl.ds(0, n), pl.ds(TILE, ny), :]
                elif dx == 0:
                    source, target = self.ys.at[way], self.yr.at[way, pl.ds(0, n), pl.ds(TILE, nx), :]
                else:
                    source, target = self.cs.at[k - 4], self.cr.at[k - 4]
                self.copies.append(
                    pltpu.make_async_remote_copy(
                        src_ref=source, dst_ref=target,
                        send_sem=send.at[number, k], recv_sem=recv.at[number, k],
                        device_id={"gx": moved("gx", dx), "gy": moved("gy", dy)}, device_id_type=MESH,
                    )
                )

        def blank(self):
            zeros = jnp.zeros((TILE, LANES), jnp.float32)

            def borders(f, carry):
                for way in range(2):
                    for at in (0, TILE + ny):
                        self.xr[way, f, pl.ds(at, TILE), :] = zeros
                    for at in (0, TILE + nx):
                        self.yr[way, f, pl.ds(at, TILE), :] = zeros
                return carry

            lax.fori_loop(0, self.n, borders, 0)

            def clear(ref, way, extent):
                def body(f, carry):
                    ref[way, f, pl.ds(TILE, extent), :] = jnp.zeros((extent, LANES), jnp.float32)
                    return carry
                lax.fori_loop(0, self.n, body, 0)

            for way, step in ((0, 1), (1, -1)):
                pl.when(jnp.logical_not(exists(-step, 0)))(functools.partial(clear, self.xr, way, ny))
                pl.when(jnp.logical_not(exists(0, -step)))(functools.partial(clear, self.yr, way, nx))

        def start(self):
            buf, step = self.buf, self.step

            def gather(f, carry):
                for x in range(0, nx, TILE):
                    for way, toward in ((0, 1), (1, -1)):
                        row = self.first_row + x * step + edge_row(toward)
                        self.ys[way, f, pl.ds(x, TILE), :] = buf[f, pl.ds(row, TILE, stride=step), :]
                for k, (dx, dy) in enumerate(WAYS[4:]):
                    row = self.first_row + (nx - 1 if dx > 0 else 0) * step + edge_row(dy)
                    self.cs[k, pl.ds(f, 1), :] = buf[f, pl.ds(row, 1), :]
                return carry

            for k in range(2):
                pl.when(exists(*WAYS[k]))(self.copies[k].start)
            lax.fori_loop(0, self.n, gather, 0)
            for k in range(2, 8):
                pl.when(exists(*WAYS[k]))(self.copies[k].start)

        def receive(self):
            for k, (dx, dy) in enumerate(WAYS):
                pl.when(exists(-dx, -dy))(self.copies[k].wait_recv)

            def corner(k, dx, dy):
                way = 0 if dy > 0 else 1
                at = TILE - 1 if dx > 0 else TILE + nx

                def body(f, carry):
                    self.yr[way, f, pl.ds(at, 1), :] = self.cr[k, pl.ds(f, 1), :]
                    return carry
                lax.fori_loop(0, self.n, body, 0)

            for k, (dx, dy) in enumerate(WAYS[4:]):
                pl.when(exists(-dx, -dy))(functools.partial(corner, k, dx, dy))

        def finish(self):
            for k, (dx, dy) in enumerate(WAYS):
                pl.when(exists(dx, dy))(self.copies[k].wait_send)

    def pad_zeros(buf, n):
        zeros = jnp.zeros((TILE, LANES), jnp.float32)

        def body(f, carry):
            for p in range(nx + 3):
                buf[f, pl.ds(p * pitch, TILE), :] = zeros
            for p in (0, nx + 1):
                for k in range(tiles):
                    buf[f, pl.ds(first(p) + k * TILE, TILE), :] = zeros
            return carry

        lax.fori_loop(0, n, body, 0)

    code_z = Depth(0, edge, zl_i, zr_i, codes, 1)
    code_own = Unit(0, codes, 0, 1, ys_i, yr_i, cs_i, cr_i, 0)
    code_packed = Unit(1, codes, 1, 2, ys_i, yr_i, cs_i, cr_i, 1)
    raw_z = Depth(1, zs_f.at[0], zl_f.at[0], zr_f.at[0], packed, 0)
    raw_all = Faces(2, raw, fields, 0, ny, (xr_r, ys_r, yr_r, cs_r, cr_r))
    raw_packed = Unit(3, packed, 0, 1, ys_p, yr_p, cs_p, cr_p, 0)
    w_z = Depth(2, zs_f.at[1], zl_f.at[1], zr_f.at[1], packed, 1)
    w_all = Faces(4, weights, 1, 0, ny, (xr_w, ys_w, yr_w, cs_w, cr_w))
    w_packed = Unit(5, packed, 1, 2, ys_p, yr_p, cs_p, cr_p, 1)
    q_z = Depth(3, zs_f.at[2], zl_f.at[2], zr_f.at[2], packed, 2)
    q_all = Faces(6, qbuf, nspec, first(1), pitch, (xr_q, ys_q, yr_q, cs_q, cr_q))
    q_packed = Unit(7, packed, 2, 3, ys_p, yr_p, cs_p, cr_p, 2)
    everything = [
        code_z, code_own, code_packed, raw_z, raw_all, raw_packed, w_z, w_all, w_packed, q_z, q_all, q_packed,
    ]

    def total_over(value):
        for number, axis in enumerate(AXES):
            n, me = size[axis], here[axis]
            peers[number, me] = value
            copies = [
                pltpu.make_async_remote_copy(
                    src_ref=peers.at[number, me], dst_ref=peers.at[number, me],
                    send_sem=peer_send.at[number, k], recv_sem=peer_recv.at[number, k],
                    device_id={axis: lax.rem(me + k, n)}, device_id_type=MESH,
                )
                for k in range(1, n)
            ]
            for copy in copies:
                copy.start()
            yield
            for copy in copies:
                copy.wait()
            value = peers[number, 0]
            for k in range(1, n):
                value = value + peers[number, k]
        change[...] = jnp.broadcast_to(jnp.sum(value, axis=1, keepdims=True) * scale, change.shape)

    def fractions(own):
        is_cut = flag[own, :] == 1
        volume = jnp.where(is_cut, vol[own, :], 256).astype(jnp.float32) * (1.0 / 256.0)
        face = jnp.where(is_cut, area[own, :], 256).astype(jnp.float32) * (1.0 / 256.0)
        return volume, face

    def fill(x, carry):
        for k in range(tiles):
            row, at = own_tile(x, k)
            own = pl.ds(at, TILE)
            value = jnp.where(flag[own, :] == 1, code[own, :] | CENTER, CENTER)
            codes[0, pl.ds(row, TILE), :] = value
            low = jnp.broadcast_to(value[:, :1], (TILE, LANES))
            high = lax.shift_right_logical(jnp.broadcast_to(value[:, LANES - 1:], (TILE, LANES)), 2)
            edge[own, :] = jnp.where(odd, low, high)
        return carry

    def shift(x, carry):
        for k in range(tiles):
            row, at = own_tile(x, k)
            own = pl.ds(at, TILE)
            value = codes[0, pl.ds(row, TILE), :]
            shifted[0, own, :] = jnp.where(first_lane, 0, pltpu.roll(value, 1, 1))
            shifted[1, own, :] = jnp.where(last_lane, 0, pltpu.roll(value, LANES - 1, 1))
        return carry

    def prepare(x, totals):
        for k in range(tiles):
            _, at = own_tile(x, k)
            own = pl.ds(at, TILE)
            volume, face = fractions(own)
            volumes[own, :] = volume
            raw[nspec, own, :] = face
            totals = tuple(totals[s] + volume * raw[s, own, :] for s in range(nspec))
        return totals

    def raw_pack(x, carry):
        for k in range(tiles):
            _, at = own_tile(x, k)
            own = pl.ds(at, TILE)
            zs_f[0, own, :] = pack([raw[f, own, :] for f in range(fields)], 0)
        return carry

    def masked_sums(taps, low, high):
        zero = jnp.zeros((TILE, LANES), jnp.float32)
        sums = [[None] * (high - low) for _ in range(3)]
        for sources, position, value_of in taps:
            present = [
                None if source is None else (source & (1 << (position + k))) != 0 for k, source in enumerate(sources)
            ]
            for f in range(low, high):
                value = value_of(f)
                for k in range(3):
                    term = value if present[k] is None else jnp.where(present[k], value, zero)
                    old = sums[k][f - low]
                    sums[k][f - low] = term if old is None else old + term
        return sums

    def keep_sums(slot, sums, low):
        for m in range(3):
            for f, value in enumerate(sums[m]):
                parts_f[slot, m, low + f] = value

    def merged(slot, f, wrap):
        if wrap:
            up, down = pltpu.roll(parts_f[slot, 2, f], 1, 1), pltpu.roll(parts_f[slot, 0, f], LANES - 1, 1)
            up, down = jnp.where(first_lane, 0.0, up), jnp.where(last_lane, 0.0, down)
        else:
            up, down = pltpu.roll(parts_f[slot, 2, f], LANES - 1, 1), pltpu.roll(parts_f[slot, 0, f], 1, 1)
        return parts_f[slot, 1, f] + up + down

    def packed_taps(row, step, source, value_of):
        zero = jnp.zeros((TILE, LANES), jnp.float32)
        total = None
        for a, b, position in BLOCK:
            near = pl.ds(row + step * (a * pitch + b), TILE)
            term = jnp.where((source(near) & (1 << position)) != 0, value_of(near), zero)
            total = term if total is None else total + term
        return total

    def pack(values, lowest):
        packed = jnp.zeros((TILE, LANES), jnp.float32)
        for k, value in enumerate(values):
            f = lowest + k
            packed = jnp.where((lane == 2 * f) | (lane == 2 * f + 1), pltpu.roll(value, 2 * f + 1, 1), packed)
        return packed

    quad = 2
    members = [(k, k // tiles, k % tiles) for k in range(quad * tiles)]

    def count_taps(g):
        for k, x, y in members:
            row, at = own_tile(g * quad + x, y)
            sums = [None] * 3
            total = None
            for a, b, position in BLOCK:
                near = pl.ds(row - a * pitch - b, TILE)
                value = codes[0, near, :]
                value = value if position == 0 else lax.shift_right_logical(value, position)
                for m in range(3):
                    term = value & (1 << m)
                    sums[m] = term if sums[m] is None else sums[m] + term
                value = codes[1, near, :]
                value = value if position == 0 else lax.shift_right_logical(value, position)
                total = value & 1 if total is None else total + (value & 1)
            for m in range(3):
                parts_i[k, m] = sums[m]
            parts_i[k, 3] = total

    def weigh(g):
        for k, x, y in members:
            row, at = own_tile(g * quad + x, y)
            own = pl.ds(at, TILE)
            from_end = pltpu.roll(parts_i[k, 3], LANES - 1, 1)
            from_left = pltpu.roll(lax.shift_right_logical(parts_i[k, 2], 2), 1, 1)
            from_right = pltpu.roll(parts_i[k, 0], LANES - 1, 1)
            counted = lax.shift_right_logical(parts_i[k, 1], 1)
            counted = counted + jnp.where(first_lane, from_end, from_left) + jnp.where(last_lane, from_end, from_right)
            share = 1.0 / counted.astype(jnp.float32)
            scaling[own, :] = raw[nspec, own, :] * share
            weight = volumes[own, :] * share
            weights[0, own, :] = weight
            for f in range(fields):
                wbuf[f, pl.ds(row, TILE), :] = weight * raw[f, own, :]

    def weigh_pack(g):
        for k, x, y in members:
            row, at = own_tile(g * quad + x, y)
            own = pl.ds(at, TILE)
            value = weights[0, own, :]
            low = jnp.broadcast_to(value[:, :1], (TILE, LANES))
            high = jnp.broadcast_to(value[:, LANES - 1:], (TILE, LANES))
            zs_f[1, own, :] = jnp.where(odd, low, high)

    def own_row(t):
        x, k = lax.div(t, tiles), lax.rem(t, tiles)
        row = (TILE + pitch) + x * pitch + k * TILE
        if isinstance(t, int):
            return int(row), t * TILE
        return pl.multiple_of(row, TILE), pl.multiple_of(t * TILE, TILE)

    def reader(buf, near):
        return lambda f: buf[f, near, :]

    def weighed(buf, factors, near):
        factor = factors[0, near, :]
        return lambda f: buf[f, near, :] * factor

    def gather_main(t):
        row, at = own_tile(t // tiles, t % tiles) if isinstance(t, int) else own_row(t)
        own = pl.ds(at, TILE)
        right, left, middle = shifted[0, own, :], shifted[1, own, :], codes[0, pl.ds(row, TILE), :]
        taps = []
        for a, b, position in BLOCK:
            center = None if position == 12 else middle
            taps.append(((left, center, right), position, reader(wbuf, pl.ds(row + a * pitch + b, TILE))))
        keep_sums(0, masked_sums(taps, 0, fields), 0)

    def gather_close(t):
        row, at = own_tile(t // tiles, t % tiles) if isinstance(t, int) else own_row(t)
        for f in range(nspec):
            qbuf[f, pl.ds(row, TILE), :] = merged(0, f, False)
        gathered[pl.ds(at, TILE), :] = merged(0, flux, False)

    def gather_strip(j):
        x = j * TILE
        for way, (b, y) in enumerate(((-1, 0), (1, ny - 1))):
            where = pl.ds(x * ny + y, TILE, stride=ny)
            right, left = shifted[0, where, :], shifted[1, where, :]
            middle = codes[0, pl.ds(first(1) + x * pitch + y, TILE, stride=pitch), :]
            taps = []
            for a in (-1, 0, 1):
                near = pl.ds(TILE + x + a, TILE)
                taps.append(((left, middle, right), 9 * (a + 1) + 3 * (b + 1), weighed(yr_r.at[way], yr_w.at[way], near)))
            keep_sums(way, masked_sums(taps, 0, fields), 0)

    def gather_strip_close(j):
        x = j * TILE
        for way, y in enumerate((0, ny - 1)):
            rows = pl.ds(first(1) + x * pitch + y, TILE, stride=pitch)
            for f in range(nspec):
                qbuf[f, rows, :] = qbuf[f, rows, :] + merged(way, f, False)
            where = pl.ds(x * ny + y, TILE, stride=ny)
            gathered[where, :] = gathered[where, :] + merged(way, flux, False)

    def gather_plane(way):
        a, x = ((-1, 0), (1, nx - 1))[way]
        for k in range(tiles):
            row, at = own_tile(x, k)
            own = pl.ds(at, TILE)
            right, left, middle = shifted[0, own, :], shifted[1, own, :], codes[0, pl.ds(row, TILE), :]
            taps = []
            for b in (-1, 0, 1):
                near = pl.ds(TILE + k * TILE + b, TILE)
                taps.append(((left, middle, right), 9 * (a + 1) + 3 * (b + 1), weighed(xr_r.at[way], xr_w.at[way], near)))
            keep_sums(way * tiles + k, masked_sums(taps, 0, fields), 0)

    def gather_plane_close(way):
        x = (0, nx - 1)[way]
        for k in range(tiles):
            row, at = own_tile(x, k)
            for f in range(nspec):
                qbuf[f, pl.ds(row, TILE), :] = qbuf[f, pl.ds(row, TILE), :] + merged(way * tiles + k, f, False)
            own = pl.ds(at, TILE)
            gathered[own, :] = gathered[own, :] + merged(way * tiles + k, flux, False)

    def gather_ends(g):
        for k, x, y in members:
            row, at = own_tile(g * quad + x, y)
            value = edge[pl.ds(at, TILE), :]
            parts_e[k] = packed_taps(
                row, 1, lambda near: value, lambda near: packed[0, near, :] * packed[1, near, :])

    def quotas(g):
        for k, x, y in members:
            row, at = own_tile(g * quad + x, y)
            value = parts_e[k]

            def spread(f):
                return jnp.where(both_ends, pltpu.roll(value, LANES - 1 - 2 * f, 1), 0.0)

            inverted = 1.0 / (gathered[pl.ds(at, TILE), :] + spread(flux))
            for f in range(nspec):
                qbuf[f, pl.ds(row, TILE), :] = (qbuf[f, pl.ds(row, TILE), :] + spread(f)) * inverted

    def quota_pack(g):
        for k, x, y in members:
            row, at = own_tile(g * quad + x, y)
            zs_f[2, pl.ds(at, TILE), :] = pack([qbuf[f, pl.ds(row, TILE), :] for f in range(nspec)], 0)

    def scatter_main(t):
        row, at = own_tile(t // tiles, t % tiles) if isinstance(t, int) else own_row(t)
        taps = []
        for a, b, position in BLOCK:
            near = pl.ds(row - a * pitch - b, TILE)
            source = codes[0, near, :]
            center = None if position == 12 else source
            taps.append(((source, center, source), position, reader(qbuf, near)))
        keep_sums(0, masked_sums(taps, 0, nspec), 0)

    def scatter_close(t):
        row, at = own_tile(t // tiles, t % tiles) if isinstance(t, int) else own_row(t)
        for f in range(nspec):
            wbuf[f, pl.ds(row, TILE), :] = merged(0, f, True)

    def scatter_strip(j):
        x = j * TILE
        for way, (b, y) in enumerate(((1, -1), (-1, ny))):
            taps = []
            for a in (-1, 0, 1):
                source = codes[0, pl.ds(first(1) + (x - a) * pitch + y, TILE, stride=pitch), :]
                taps.append(((source, source, source), 9 * (a + 1) + 3 * (b + 1), reader(yr_q.at[way], pl.ds(TILE + x - a, TILE))))
            keep_sums(way, masked_sums(taps, 0, nspec), 0)

    def scatter_strip_close(j):
        for way, y in enumerate((0, ny - 1)):
            where = pl.ds(first(1) + j * TILE * pitch + y, TILE, stride=pitch)
            for f in range(nspec):
                wbuf[f, where, :] = wbuf[f, where, :] + merged(way, f, True)

    def scatter_plane(way):
        a, x = ((1, 0), (-1, nx + 1))[way]
        for k in range(tiles):
            taps = []
            for b in (-1, 0, 1):
                source = codes[0, pl.ds(first(x) + k * TILE - b, TILE), :]
                taps.append(((source, source, source), 9 * (a + 1) + 3 * (b + 1), reader(xr_q.at[way], pl.ds(TILE + k * TILE - b, TILE))))
            keep_sums(way * tiles + k, masked_sums(taps, 0, nspec), 0)

    def scatter_plane_close(way):
        x = (0, nx - 1)[way]
        for k in range(tiles):
            row, at = own_tile(x, k)
            for f in range(nspec):
                wbuf[f, pl.ds(row, TILE), :] = wbuf[f, pl.ds(row, TILE), :] + merged(way * tiles + k, f, True)

    def scatter_ends(g):
        for k, x, y in members:
            row, at = own_tile(g * quad + x, y)
            parts_e[k] = packed_taps(row, -1, lambda near: codes[1, near, :], lambda near: packed[2, near, :])

    def finals(g):
        for k, x, y in members:
            row, at = own_tile(g * quad + x, y)
            own = pl.ds(at, TILE)
            value, factor = parts_e[k], scaling[own, :]
            for f in range(nspec):
                spread = jnp.where(both_ends, pltpu.roll(value, LANES - 1 - 2 * f, 1), 0.0)
                out[f, own, :] = factor * (wbuf[f, pl.ds(row, TILE), :] + spread)

    blank(codes, 0, 2)
    loads[0].wait()
    loads[1].wait()
    lax.fori_loop(0, nx, fill, 0, unroll=8)
    pl.semaphore_wait(barrier, greeted)
    code_z.start()
    code_own.start()
    for copy in loads[2:]:
        copy.wait()
    totals = tuple(jnp.zeros((TILE, LANES), jnp.float32) for _ in range(nspec))
    totals = lax.fori_loop(0, nx, prepare, totals, unroll=2)
    local = jnp.concatenate(
        [jnp.sum(total, axis=0, keepdims=True) for total in totals]
        + [jnp.zeros((peers.shape[2] - nspec, LANES), jnp.float32)],
        axis=0,
    )
    reduction = total_over(local)
    code_z.receive()
    code_packed.start()
    raw_all.start()
    lax.fori_loop(0, nx, raw_pack, 0, unroll=4)
    raw_z.start()
    lax.fori_loop(0, nx, shift, 0, unroll=8)
    blank(packed, 0, 3)
    raw_all.blank()
    w_all.blank()
    q_all.blank()
    pad_zeros(wbuf, fields)
    pad_zeros(qbuf, nspec)
    code_own.receive()
    code_packed.receive()
    raw_z.receive()
    raw_packed.start()
    pipelined([count_taps, weigh, weigh_pack], nx // quad)
    w_z.start()
    w_all.start()

    def relay_w():
        w_z.receive()
        w_packed.start()

    pipelined([gather_main, gather_close], nx * tiles, (nx * tiles // 4, relay_w))
    raw_all.receive()
    raw_packed.receive()
    w_all.receive()
    w_packed.receive()
    next(reduction)
    pipelined([gather_strip, gather_strip_close], nx // TILE)
    for stage in (gather_plane, gather_plane_close):
        stage(0)
        stage(1)
    pipelined([gather_ends, quotas, quota_pack], nx // quad)
    q_z.start()
    q_all.start()

    def relay_q():
        q_z.receive()
        q_packed.start()
        next(reduction)

    pipelined([scatter_main, scatter_close], nx * tiles, (nx * tiles // 4, relay_q))
    q_all.receive()
    q_packed.receive()
    next(reduction)
    pipelined([scatter_strip, scatter_strip_close], nx // TILE)
    for stage in (scatter_plane, scatter_plane_close):
        stage(0)
        stage(1)
    pipelined([scatter_ends, finals], nx // quad)
    next(reduction, None)
    for part in everything:
        part.finish()


def per_device(provisional, cut_flag, cut_code, volume_level, area_level):
    nspec, nx, ny, nz = provisional.shape
    assert nz == LANES and ny % TILE == 0 and nx % TILE == 0
    own = nx * ny
    tiles = ny // TILE
    rows = 2 * TILE + (nx + 2) * (ny + TILE)
    most = max(lax.axis_size(axis) for axis in AXES)
    cells = own * nz * math.prod(lax.axis_size(axis) for axis in AXES)
    fields = nspec + 1
    f32, i32 = jnp.float32, jnp.int32
    vmem = pl.BlockSpec(memory_space=pltpu.VMEM)
    hbm = pl.BlockSpec(memory_space=pltpu.HBM)
    shapes = [
        ((fields, own, nz), f32), ((own, nz), i32), ((own, nz), i32), ((own, nz), i32), ((own, nz), i32),
        ((2, rows, nz), i32), ((fields, rows, nz), f32), ((nspec, rows, nz), f32), ((3, rows, nz), f32),
        ((2, own, nz), i32), ((own, nz), i32),
        ((own, nz), i32), ((own, nz), i32),
        ((3, own, nz), f32), ((3, own, nz), f32), ((3, own, nz), f32),
        ((2, 2, nx, nz), i32), ((2, 2, nx, nz), i32), ((2, 4, TILE, nz), i32), ((2, 4, TILE, nz), i32),
        ((2, 3, nx, nz), f32), ((2, 3, nx, nz), f32), ((3, 4, TILE, nz), f32), ((3, 4, TILE, nz), f32),
    ]
    for n in (fields, 1, nspec):
        high = -(-n // TILE) * TILE
        shapes += [
            ((2, n, ny + 2 * TILE, nz), f32), ((2, n, nx, nz), f32), ((2, n, nx + 2 * TILE, nz), f32),
            ((4, high, nz), f32), ((4, high, nz), f32),
        ]
    high = -(-nspec // TILE) * TILE
    shapes += [
        ((own, nz), f32), ((1, own, nz), f32), ((own, nz), f32), ((own, nz), f32),
        ((2 * tiles, 4, TILE, nz), i32), ((2 * tiles, 3, fields, TILE, nz), f32), ((2 * tiles, TILE, nz), f32),
        ((3, most, high, nz), f32),
    ]
    dma = pltpu.SemaphoreType.DMA
    out, change = pl.pallas_call(
        functools.partial(kernel, nx, ny, 1.0 / math.sqrt(cells)),
        out_shape=(
            jax.ShapeDtypeStruct((nspec, own, nz), f32),
            jax.ShapeDtypeStruct((high, nz), f32),
        ),
        in_specs=[hbm] * 5,
        out_specs=(vmem, vmem),
        scratch_shapes=[pltpu.VMEM(shape, kind) for shape, kind in shapes]
        + [
            dma((5,)), dma((4, 2)), dma((4, 2)), dma((8, 8)), dma((8, 8)), dma((3, most)), dma((3, most)),
        ],
        compiler_params=pltpu.CompilerParams(
            collective_id=0, has_side_effects=True, vmem_limit_bytes=26 * 1024 * 1024
        ),
    )(
        *[pltpu.with_memory_space_constraint(x, pltpu.HBM) for x in (
        provisional.reshape(nspec, own, nz),
        cut_flag.reshape(own, nz),
        cut_code.reshape(own, nz),
        volume_level.reshape(own, nz),
        area_level.reshape(own, nz))]
    )
    return out.reshape(provisional.shape), change[:nspec, 0]


def solution(mesh):
    spec = P("gx", "gy", "gz")
    wide = P(None, "gx", "gy", "gz")
    return jax.shard_map(
        per_device, mesh=mesh, in_specs=(wide, spec, spec, spec, spec), out_specs=(wide, P()), check_vma=False
    )
```

```python
import functools
import math

import jax
import jax.numpy as jnp
from jax import lax
from jax.experimental import pallas as pl
from jax.experimental.pallas import tpu as pltpu
from jax.sharding import PartitionSpec as P

CENTER = 8192
BLOCK = [(a, b, 9 * (a + 1) + 3 * (b + 1)) for a in (-1, 0, 1) for b in (-1, 0, 1)]
AXES = ("gx", "gy", "gz")
WAYS = [(1, 0), (-1, 0), (0, 1), (0, -1), (1, 1), (1, -1), (-1, 1), (-1, -1)]
MESH = pl.DeviceIdType.MESH
LANES = 128
TILE = 8


def pipelined(stages, count, hook=None):
    depth = len(stages)

    def step(i, lowest, highest):
        for k in reversed(range(lowest, highest)):
            stages[k](i - k)

    for i in range(min(depth - 1, count)):
        step(i, 0, i + 1)

    def body(i, carry):
        step(i, 0, depth)
        return carry

    low = depth - 1
    if hook is not None:
        at, action = hook
        lax.fori_loop(low, at, body, 0)
        action()
        low = at
    lax.fori_loop(low, count, body, 0)
    for i in range(count, count + depth - 1):
        step(i, i - count + 1, depth)


def kernel(
    nx, ny, scale,
    prov_h, flag_h, code_h, vol_h, area_h,
    out, change,
    raw, flag, code, vol, area,
    codes, wbuf, qbuf, packed, shifted, edge,
    zl_i, zr_i, zs_f, zl_f, zr_f,
    ys_i, yr_i, cs_i, cr_i, ys_p, yr_p, cs_p, cr_p,
    xr_r, ys_r, yr_r, cs_r, cr_r, xr_w, ys_w, yr_w, cs_w, cr_w, xr_q, ys_q, yr_q, cs_q, cr_q, xs_q,
    volumes, weights, gathered, scaling, parts_i, parts_f, parts_e, peers,
    load, z_send, z_recv, send, recv, peer_send, peer_recv,
):
    nspec = prov_h.shape[0]
    pitch = ny + TILE
    tiles = ny // TILE
    here = {axis: lax.axis_index(axis) for axis in AXES}
    size = {axis: lax.axis_size(axis) for axis in AXES}
    lane = lax.broadcasted_iota(jnp.int32, (TILE, LANES), 1)
    odd = (lane & 1) == 1
    first_lane = lane == 0
    last_lane = lane == LANES - 1
    both_ends = first_lane | last_lane
    fields = nspec + 1
    flux = nspec

    inputs = [(flag_h, flag), (code_h, code), (vol_h, vol), (area_h, area), (prov_h, raw.at[pl.ds(0, nspec)])]
    loads = [pltpu.make_async_copy(src, dst, load.at[k]) for k, (src, dst) in enumerate(inputs)]
    for copy in loads:
        copy.start()

    def moved(axis, step):
        return lax.rem(here[axis] + (step + size[axis]), size[axis])

    barrier = pltpu.get_barrier_semaphore()
    near_x = lax.min(here["gx"], 1) + lax.min(size["gx"] - 1 - here["gx"], 1)
    near_y = lax.min(here["gy"], 1) + lax.min(size["gy"] - 1 - here["gy"], 1)
    near_z = lax.min(here["gz"], 1) + lax.min(size["gz"] - 1 - here["gz"], 1)
    greeted = (near_x + 1) * (near_y + 1) - 1 + near_z
    for axis, near in (("gx", near_x), ("gy", near_y), ("gz", near_z)):
        if size[axis] > 4:
            greeted = greeted + (size[axis] - 1 - near)

    def greet(target):
        pl.semaphore_signal(barrier, inc=1, device_id=target, device_id_type=MESH)

    def first(x):
        return TILE + x * pitch

    def own_tile(x, k):
        row = (TILE + pitch + k * TILE) + x * pitch
        at = x * ny + k * TILE
        if isinstance(x, int):
            return row, at
        return pl.multiple_of(row, TILE), pl.multiple_of(at, TILE)

    def side(axis, step):
        return here[axis] < size[axis] - 1 if step > 0 else here[axis] > 0

    def exists(dx, dy):
        found = None
        for axis, step in (("gx", dx), ("gy", dy)):
            if step:
                there = side(axis, step)
                found = there if found is None else jnp.logical_and(found, there)
        return found

    below_z, above_z = side("gz", -1), side("gz", 1)
    for dx, dy in WAYS:
        pl.when(exists(dx, dy))(functools.partial(greet, {"gx": moved("gx", dx), "gy": moved("gy", dy)}))
    pl.when(below_z)(functools.partial(greet, {"gz": moved("gz", -1)}))
    pl.when(above_z)(functools.partial(greet, {"gz": moved("gz", 1)}))
    for axis in AXES:
        if size[axis] > 4:
            for k in range(2, size[axis]):
                pl.when(here[axis] >= k)(functools.partial(greet, {axis: moved(axis, -k)}))
                pl.when(here[axis] + k < size[axis])(functools.partial(greet, {axis: moved(axis, k)}))

    def edge_row(step):
        return ny - 1 if step > 0 else 0

    def halo_row(step):
        return ny if step > 0 else -1

    def blank(buf, low, high):
        zeros = jnp.zeros((ny, LANES), buf.dtype)
        row_zeros = jnp.zeros((TILE, LANES), buf.dtype)
        one = jnp.zeros((1, LANES), buf.dtype)

        def plane(step):
            def body(f, carry):
                buf[f, pl.ds(first(nx + 1 if step > 0 else 0), ny), :] = zeros
                return carry
            lax.fori_loop(low, high, body, 0)

        def row(step):
            def body(f, carry):
                for x in range(0, nx, TILE):
                    buf[f, pl.ds(first(x + 1) + halo_row(step), TILE, stride=pitch), :] = row_zeros
                return carry
            lax.fori_loop(low, high, body, 0)

        def corner(dx, dy):
            def body(f, carry):
                buf[f, pl.ds(first(nx + 1 if dx > 0 else 0) + halo_row(dy), 1), :] = one
                return carry
            lax.fori_loop(low, high, body, 0)

        for dx, dy in WAYS:
            action = functools.partial(plane, dx) if dy == 0 else (
                functools.partial(row, dy) if dx == 0 else functools.partial(corner, dx, dy))
            pl.when(jnp.logical_not(exists(dx, dy)))(action)

    class Unit:
        def __init__(self, number, buf, low, high, ys, yr, cs, cr, corner):
            self.buf, self.low, self.high = buf, low, high
            self.ys, self.yr, self.cs, self.cr, self.corner = ys, yr, cs, cr, corner
            n = high - low
            ends_of = {1: (nx, 0), -1: (1, nx + 1)}
            self.copies = []
            for k, (dx, dy) in enumerate(WAYS):
                if dy == 0:
                    here_x, there_x = ends_of[dx]
                    source = buf.at[pl.ds(low, n), pl.ds(first(here_x), ny), :]
                    landing = buf.at[pl.ds(low, n), pl.ds(first(there_x), ny), :]
                elif dx == 0:
                    way = 0 if dy > 0 else 1
                    source, landing = ys.at[way, pl.ds(low, n)], yr.at[way, pl.ds(low, n)]
                else:
                    source, landing = cs.at[corner, k - 4], cr.at[corner, k - 4]
                self.copies.append(
                    pltpu.make_async_remote_copy(
                        src_ref=source, dst_ref=landing,
                        send_sem=send.at[number, k], recv_sem=recv.at[number, k],
                        device_id={"gx": moved("gx", dx), "gy": moved("gy", dy)}, device_id_type=MESH,
                    )
                )

        def start(self):
            buf = self.buf
            for k, (dx, dy) in enumerate(WAYS):
                if dy == 0:
                    pl.when(exists(dx, dy))(self.copies[k].start)

            def gather(f, carry):
                for x in range(0, nx, TILE):
                    for way, step in ((0, 1), (1, -1)):
                        self.ys[way, f, pl.ds(x, TILE), :] = buf[f, pl.ds(first(x + 1) + edge_row(step), TILE, stride=pitch), :]
                for k, (dx, dy) in enumerate(WAYS[4:]):
                    row = first(nx if dx > 0 else 1) + edge_row(dy)
                    self.cs[self.corner, k, pl.ds(f - self.low, 1), :] = buf[f, pl.ds(row, 1), :]
                return carry

            lax.fori_loop(self.low, self.high, gather, 0)
            for k, (dx, dy) in enumerate(WAYS):
                if dy != 0:
                    pl.when(exists(dx, dy))(self.copies[k].start)

        def receive(self):
            buf = self.buf
            for k, (dx, dy) in enumerate(WAYS):
                pl.when(exists(-dx, -dy))(self.copies[k].wait_recv)

            def rows(way, step):
                def body(f, carry):
                    for x in range(0, nx, TILE):
                        buf[f, pl.ds(first(x + 1) + halo_row(-step), TILE, stride=pitch), :] = self.yr[way, f, pl.ds(x, TILE), :]
                    return carry
                lax.fori_loop(self.low, self.high, body, 0)

            def corner(k, dx, dy):
                def body(f, carry):
                    row = first(0 if dx > 0 else nx + 1) + halo_row(-dy)
                    buf[f, pl.ds(row, 1), :] = self.cr[self.corner, k, pl.ds(f - self.low, 1), :]
                    return carry
                lax.fori_loop(self.low, self.high, body, 0)

            for way, step in ((0, 1), (1, -1)):
                pl.when(exists(0, -step))(functools.partial(rows, way, step))
            for k, (dx, dy) in enumerate(WAYS[4:]):
                pl.when(exists(-dx, -dy))(functools.partial(corner, k, dx, dy))

        def finish(self):
            for k, (dx, dy) in enumerate(WAYS):
                pl.when(exists(dx, dy))(self.copies[k].wait_send)

    class Depth:
        def __init__(self, number, zs, zl, zr, buf, plane):
            self.zl, self.zr, self.buf, self.plane = zl, zr, buf, plane
            self.copies = [
                pltpu.make_async_remote_copy(
                    src_ref=zs, dst_ref=landing,
                    send_sem=z_send.at[number, way], recv_sem=z_recv.at[number, way],
                    device_id={"gz": moved("gz", step)}, device_id_type=MESH,
                )
                for way, (landing, step) in enumerate(((zl, 1), (zr, -1)))
            ]

        def start(self):
            pl.when(above_z)(self.copies[0].start)
            pl.when(below_z)(self.copies[1].start)

        def receive(self):
            pl.when(below_z)(self.copies[0].wait_recv)
            pl.when(above_z)(self.copies[1].wait_recv)
            zero = jnp.zeros((TILE, LANES), self.buf.dtype)

            def place(x, carry):
                for k in range(tiles):
                    row, at = own_tile(x, k)
                    low = jnp.where(below_z, pltpu.roll(self.zl[pl.ds(at, TILE), :], 1, 1), zero)
                    high = jnp.where(above_z, pltpu.roll(self.zr[pl.ds(at, TILE), :], LANES - 1, 1), zero)
                    self.buf[self.plane, pl.ds(row, TILE), :] = jnp.where(odd, low, high)
                return carry

            lax.fori_loop(0, nx, place, 0, unroll=8)

        def finish(self):
            pl.when(above_z)(self.copies[0].wait_send)
            pl.when(below_z)(self.copies[1].wait_send)

    class Faces:
        def __init__(self, number, buf, n, start, step, landing, xs=None):
            self.buf, self.n, self.first_row, self.step, self.xs = buf, n, start, step, xs
            self.xr, self.ys, self.yr, self.cs, self.cr = landing
            self.copies = []
            for k, (dx, dy) in enumerate(WAYS):
                way = 0 if dx + dy > 0 else 1
                if dy == 0:
                    if xs is None:
                        source = buf.at[pl.ds(0, n), pl.ds(start + (nx - 1 if dx > 0 else 0) * step, ny), :]
                    else:
                        source = xs.at[way]
                    target = self.xr.at[way, pl.ds(0, n), pl.ds(TILE, ny), :]
                elif dx == 0:
                    source, target = self.ys.at[way], self.yr.at[way, pl.ds(0, n), pl.ds(TILE, nx), :]
                else:
                    source, target = self.cs.at[k - 4], self.cr.at[k - 4]
                self.copies.append(
                    pltpu.make_async_remote_copy(
                        src_ref=source, dst_ref=target,
                        send_sem=send.at[number, k], recv_sem=recv.at[number, k],
                        device_id={"gx": moved("gx", dx), "gy": moved("gy", dy)}, device_id_type=MESH,
                    )
                )

        def blank(self):
            zeros = jnp.zeros((TILE, LANES), jnp.float32)

            def borders(f, carry):
                for way in range(2):
                    for at in (0, TILE + ny):
                        self.xr[way, f, pl.ds(at, TILE), :] = zeros
                    for at in (0, TILE + nx):
                        self.yr[way, f, pl.ds(at, TILE), :] = zeros
                return carry

            lax.fori_loop(0, self.n, borders, 0)

            def clear(ref, way, extent):
                def body(f, carry):
                    ref[way, f, pl.ds(TILE, extent), :] = jnp.zeros((extent, LANES), jnp.float32)
                    return carry
                lax.fori_loop(0, self.n, body, 0)

            for way, step in ((0, 1), (1, -1)):
                pl.when(jnp.logical_not(exists(-step, 0)))(functools.partial(clear, self.xr, way, ny))
                pl.when(jnp.logical_not(exists(0, -step)))(functools.partial(clear, self.yr, way, nx))

        def start(self):
            buf, step = self.buf, self.step

            def gather(f, carry):
                for x in range(0, nx, TILE):
                    for way, toward in ((0, 1), (1, -1)):
                        row = self.first_row + x * step + edge_row(toward)
                        self.ys[way, f, pl.ds(x, TILE), :] = buf[f, pl.ds(row, TILE, stride=step), :]
                for k, (dx, dy) in enumerate(WAYS[4:]):
                    row = self.first_row + (nx - 1 if dx > 0 else 0) * step + edge_row(dy)
                    self.cs[k, pl.ds(f, 1), :] = buf[f, pl.ds(row, 1), :]
                return carry

            for k in range(2):
                pl.when(exists(*WAYS[k]))(self.copies[k].start)
            lax.fori_loop(0, self.n, gather, 0)
            for k in range(2, 8):
                pl.when(exists(*WAYS[k]))(self.copies[k].start)

        def start_filled(self):
            def corners(f, carry):
                for k, (dx, dy) in enumerate(WAYS[4:]):
                    self.cs[k, pl.ds(f, 1), :] = self.xs[0 if dx > 0 else 1, f, pl.ds(edge_row(dy), 1), :]
                return carry

            for k in range(4):
                pl.when(exists(*WAYS[k]))(self.copies[k].start)
            lax.fori_loop(0, self.n, corners, 0)
            for k in range(4, 8):
                pl.when(exists(*WAYS[k]))(self.copies[k].start)

        def receive(self):
            for k, (dx, dy) in enumerate(WAYS):
                pl.when(exists(-dx, -dy))(self.copies[k].wait_recv)

            def corner(k, dx, dy):
                way = 0 if dy > 0 else 1
                at = TILE - 1 if dx > 0 else TILE + nx

                def body(f, carry):
                    self.yr[way, f, pl.ds(at, 1), :] = self.cr[k, pl.ds(f, 1), :]
                    return carry
                lax.fori_loop(0, self.n, body, 0)

            for k, (dx, dy) in enumerate(WAYS[4:]):
                pl.when(exists(-dx, -dy))(functools.partial(corner, k, dx, dy))

        def finish(self):
            for k, (dx, dy) in enumerate(WAYS):
                pl.when(exists(dx, dy))(self.copies[k].wait_send)

    def pad_zeros(buf, n):
        zeros = jnp.zeros((TILE, LANES), jnp.float32)

        def body(f, carry):
            for p in range(nx + 3):
                buf[f, pl.ds(p * pitch, TILE), :] = zeros
            for p in (0, nx + 1):
                for k in range(tiles):
                    buf[f, pl.ds(first(p) + k * TILE, TILE), :] = zeros
            return carry

        lax.fori_loop(0, n, body, 0)

    code_z = Depth(0, edge, zl_i, zr_i, codes, 1)
    code_own = Unit(0, codes, 0, 1, ys_i, yr_i, cs_i, cr_i, 0)
    code_packed = Unit(1, codes, 1, 2, ys_i, yr_i, cs_i, cr_i, 1)
    raw_z = Depth(1, zs_f.at[0], zl_f.at[0], zr_f.at[0], packed, 0)
    raw_all = Faces(2, raw, fields, 0, ny, (xr_r, ys_r, yr_r, cs_r, cr_r))
    raw_packed = Unit(3, packed, 0, 1, ys_p, yr_p, cs_p, cr_p, 0)
    w_z = Depth(2, zs_f.at[1], zl_f.at[1], zr_f.at[1], packed, 1)
    w_all = Faces(4, weights, 1, 0, ny, (xr_w, ys_w, yr_w, cs_w, cr_w))
    w_packed = Unit(5, packed, 1, 2, ys_p, yr_p, cs_p, cr_p, 1)
    q_z = Depth(3, zs_f.at[2], zl_f.at[2], zr_f.at[2], packed, 2)
    q_all = Faces(6, qbuf, nspec, first(1), pitch, (xr_q, ys_q, yr_q, cs_q, cr_q), xs_q)
    q_packed = Unit(7, packed, 2, 3, ys_p, yr_p, cs_p, cr_p, 2)
    everything = [
        code_z, code_own, code_packed, raw_z, raw_all, raw_packed, w_z, w_all, w_packed, q_z, q_all, q_packed,
    ]

    def total_over(value):
        for number, axis in enumerate(AXES):
            n, me = size[axis], here[axis]
            peers[number, me] = value
            copies = [
                pltpu.make_async_remote_copy(
                    src_ref=peers.at[number, me], dst_ref=peers.at[number, me],
                    send_sem=peer_send.at[number, k], recv_sem=peer_recv.at[number, k],
                    device_id={axis: lax.rem(me + k, n)}, device_id_type=MESH,
                )
                for k in range(1, n)
            ]
            for copy in copies:
                copy.start()
            yield
            for copy in copies:
                copy.wait()
            value = peers[number, 0]
            for k in range(1, n):
                value = value + peers[number, k]
        change[...] = jnp.broadcast_to(jnp.sum(value, axis=1, keepdims=True) * scale, change.shape)

    def fractions(own):
        is_cut = flag[own, :] == 1
        volume = jnp.where(is_cut, vol[own, :], 256).astype(jnp.float32) * (1.0 / 256.0)
        face = jnp.where(is_cut, area[own, :], 256).astype(jnp.float32) * (1.0 / 256.0)
        return volume, face

    def fill(x, carry):
        for k in range(tiles):
            row, at = own_tile(x, k)
            own = pl.ds(at, TILE)
            value = jnp.where(flag[own, :] == 1, code[own, :] | CENTER, CENTER)
            codes[0, pl.ds(row, TILE), :] = value
            low = jnp.broadcast_to(value[:, :1], (TILE, LANES))
            high = lax.shift_right_logical(jnp.broadcast_to(value[:, LANES - 1:], (TILE, LANES)), 2)
            edge[own, :] = jnp.where(odd, low, high)
        return carry

    def shift(x, carry):
        for k in range(tiles):
            row, at = own_tile(x, k)
            own = pl.ds(at, TILE)
            value = codes[0, pl.ds(row, TILE), :]
            shifted[0, own, :] = jnp.where(first_lane, 0, pltpu.roll(value, 1, 1))
            shifted[1, own, :] = jnp.where(last_lane, 0, pltpu.roll(value, LANES - 1, 1))
        return carry

    def prepare(x, totals):
        for k in range(tiles):
            _, at = own_tile(x, k)
            own = pl.ds(at, TILE)
            volume, face = fractions(own)
            volumes[own, :] = volume
            raw[nspec, own, :] = face
            totals = tuple(totals[s] + volume * raw[s, own, :] for s in range(nspec))
        return totals

    def raw_pack(x, carry):
        for k in range(tiles):
            _, at = own_tile(x, k)
            own = pl.ds(at, TILE)
            zs_f[0, own, :] = pack([raw[f, own, :] for f in range(fields)], 0)
        return carry

    def masked_sums(taps, low, high):
        zero = jnp.zeros((TILE, LANES), jnp.float32)
        sums = [[None] * (high - low) for _ in range(3)]
        for sources, position, value_of in taps:
            present = [
                None if source is None else (source & (1 << (position + k))) != 0 for k, source in enumerate(sources)
            ]
            for f in range(low, high):
                value = value_of(f)
                for k in range(3):
                    term = value if present[k] is None else jnp.where(present[k], value, zero)
                    old = sums[k][f - low]
                    sums[k][f - low] = term if old is None else old + term
        return sums

    def keep_sums(slot, sums, low):
        for m in range(3):
            for f, value in enumerate(sums[m]):
                parts_f[slot, m, low + f] = value

    def merged(slot, f, wrap):
        if wrap:
            up, down = pltpu.roll(parts_f[slot, 2, f], 1, 1), pltpu.roll(parts_f[slot, 0, f], LANES - 1, 1)
            up, down = jnp.where(first_lane, 0.0, up), jnp.where(last_lane, 0.0, down)
        else:
            up, down = pltpu.roll(parts_f[slot, 2, f], LANES - 1, 1), pltpu.roll(parts_f[slot, 0, f], 1, 1)
        return parts_f[slot, 1, f] + up + down

    def packed_taps(row, step, source, value_of):
        zero = jnp.zeros((TILE, LANES), jnp.float32)
        total = None
        row = row - (pitch + TILE)
        for a, b, position in BLOCK:
            near = pl.ds(row + (pitch + TILE + step * (a * pitch + b)), TILE)
            term = jnp.where((source(near) & (1 << position)) != 0, value_of(near), zero)
            total = term if total is None else total + term
        return total

    def pack(values, lowest):
        packed = jnp.zeros((TILE, LANES), jnp.float32)
        for k, value in enumerate(values):
            f = lowest + k
            packed = jnp.where((lane == 2 * f) | (lane == 2 * f + 1), pltpu.roll(value, 2 * f + 1, 1), packed)
        return packed

    quad = 4
    members = [(k, k // tiles, k % tiles) for k in range(quad * tiles)]

    def count_taps(g):
        for k, x, y in members:
            row, at = own_tile(g * quad + x, y)
            sums = [None] * 3
            total = None
            row = row - (pitch + TILE)
            for a, b, position in BLOCK:
                near = pl.ds(row + (pitch + TILE - a * pitch - b), TILE)
                value = codes[0, near, :]
                value = value if position == 0 else lax.shift_right_logical(value, position)
                for m in range(3):
                    term = value & (1 << m)
                    sums[m] = term if sums[m] is None else sums[m] + term
                value = codes[1, near, :]
                value = value if position == 0 else lax.shift_right_logical(value, position)
                total = value & 1 if total is None else total + (value & 1)
            for m in range(3):
                parts_i[k, m] = sums[m]
            parts_i[k, 3] = total

    def weigh(g):
        for k, x, y in members:
            row, at = own_tile(g * quad + x, y)
            own = pl.ds(at, TILE)
            from_end = pltpu.roll(parts_i[k, 3], LANES - 1, 1)
            from_left = pltpu.roll(lax.shift_right_logical(parts_i[k, 2], 2), 1, 1)
            from_right = pltpu.roll(parts_i[k, 0], LANES - 1, 1)
            counted = lax.shift_right_logical(parts_i[k, 1], 1)
            counted = counted + jnp.where(first_lane, from_end, from_left) + jnp.where(last_lane, from_end, from_right)
            share = 1.0 / counted.astype(jnp.float32)
            scaling[own, :] = raw[nspec, own, :] * share
            weight = volumes[own, :] * share
            weights[0, own, :] = weight
            for f in range(fields):
                wbuf[f, pl.ds(row, TILE), :] = weight * raw[f, own, :]

    def weigh_pack(g):
        for k, x, y in members:
            row, at = own_tile(g * quad + x, y)
            own = pl.ds(at, TILE)
            value = weights[0, own, :]
            low = jnp.broadcast_to(value[:, :1], (TILE, LANES))
            high = jnp.broadcast_to(value[:, LANES - 1:], (TILE, LANES))
            zs_f[1, own, :] = jnp.where(odd, low, high)

    def own_row(t):
        x, k = lax.div(t, tiles), lax.rem(t, tiles)
        row = (TILE + pitch) + x * pitch + k * TILE
        if isinstance(t, int):
            return int(row), t * TILE
        return pl.multiple_of(row, TILE), pl.multiple_of(t * TILE, TILE)

    def reader(buf, near):
        return lambda f: buf[f, near, :]

    def weighed(buf, factors, near):
        factor = factors[0, near, :]
        return lambda f: buf[f, near, :] * factor

    def gather_main(t):
        row, at = own_tile(t // tiles, t % tiles) if isinstance(t, int) else own_row(t)
        own = pl.ds(at, TILE)
        right, left, middle = shifted[0, own, :], shifted[1, own, :], codes[0, pl.ds(row, TILE), :]
        taps = []
        base = row - (pitch + TILE)
        for a, b, position in BLOCK:
            center = None if position == 12 else middle
            near = pl.ds(base + (pitch + TILE + a * pitch + b), TILE)
            taps.append(((left, center, right), position, reader(wbuf, near)))
        keep_sums(0, masked_sums(taps, 0, fields), 0)

    def gather_close(t):
        row, at = own_tile(t // tiles, t % tiles) if isinstance(t, int) else own_row(t)
        for f in range(nspec):
            qbuf[f, pl.ds(row, TILE), :] = merged(0, f, False)
        gathered[pl.ds(at, TILE), :] = merged(0, flux, False)

    def gather_strip(j):
        x = j * TILE
        for way, (b, y) in enumerate(((-1, 0), (1, ny - 1))):
            where = pl.ds(x * ny + y, TILE, stride=ny)
            right, left = shifted[0, where, :], shifted[1, where, :]
            middle = codes[0, pl.ds(first(1) + x * pitch + y, TILE, stride=pitch), :]
            taps = []
            for a in (-1, 0, 1):
                near = pl.ds(TILE + x + a, TILE)
                taps.append(((left, middle, right), 9 * (a + 1) + 3 * (b + 1), weighed(yr_r.at[way], yr_w.at[way], near)))
            keep_sums(way, masked_sums(taps, 0, fields), 0)

    def gather_strip_close(j):
        x = j * TILE
        for way, y in enumerate((0, ny - 1)):
            rows = pl.ds(first(1) + x * pitch + y, TILE, stride=pitch)
            for f in range(nspec):
                qbuf[f, rows, :] = qbuf[f, rows, :] + merged(way, f, False)
            where = pl.ds(x * ny + y, TILE, stride=ny)
            gathered[where, :] = gathered[where, :] + merged(way, flux, False)

    def gather_plane(way):
        a, x = ((-1, 0), (1, nx - 1))[way]
        for k in range(tiles):
            row, at = own_tile(x, k)
            own = pl.ds(at, TILE)
            right, left, middle = shifted[0, own, :], shifted[1, own, :], codes[0, pl.ds(row, TILE), :]
            taps = []
            for b in (-1, 0, 1):
                near = pl.ds(TILE + k * TILE + b, TILE)
                taps.append(((left, middle, right), 9 * (a + 1) + 3 * (b + 1), weighed(xr_r.at[way], xr_w.at[way], near)))
            keep_sums(way * tiles + k, masked_sums(taps, 0, fields), 0)

    def gather_plane_close(way):
        x = (0, nx - 1)[way]
        for k in range(tiles):
            row, at = own_tile(x, k)
            for f in range(nspec):
                qbuf[f, pl.ds(row, TILE), :] = qbuf[f, pl.ds(row, TILE), :] + merged(way * tiles + k, f, False)
            own = pl.ds(at, TILE)
            gathered[own, :] = gathered[own, :] + merged(way * tiles + k, flux, False)

    def edge_tiles():
        for way, y in enumerate((ny - 1, 0)):
            for x in range(0, nx, TILE):
                row = first(x + 1) + y
                yield (
                    lambda start: pl.ds(start, TILE, stride=pitch), row,
                    pl.ds(x * ny + y, TILE, stride=ny), ys_q.at[way], pl.ds(x, TILE),
                )
        for way, x in enumerate((nx - 1, 0)):
            for k in range(tiles):
                row, at = own_tile(x, k)
                yield lambda start: pl.ds(start, TILE), row, pl.ds(at, TILE), xs_q.at[way], pl.ds(k * TILE, TILE)

    def edge_ends():
        zero = jnp.zeros((TILE, LANES), jnp.float32)
        for n, (rows, row, own, _, _) in enumerate(edge_tiles()):
            bits = edge[own, :]
            total = None
            for a, b, position in BLOCK:
                near = rows(row + a * pitch + b)
                term = jnp.where((bits & (1 << position)) != 0, packed[0, near, :] * packed[1, near, :], zero)
                total = term if total is None else total + term
            parts_e[n] = total

    def edge_quotas():
        for n, (rows, row, own, ref, where) in enumerate(edge_tiles()):
            value = parts_e[n]

            def spread(f):
                return jnp.where(both_ends, pltpu.roll(value, LANES - 1 - 2 * f, 1), 0.0)

            inverted = 1.0 / (gathered[own, :] + spread(flux))
            for f in range(nspec):
                ref[f, where, :] = (qbuf[f, rows(row), :] + spread(f)) * inverted

    def gather_ends(g):
        for k, x, y in members:
            row, at = own_tile(g * quad + x, y)
            value = edge[pl.ds(at, TILE), :]
            parts_e[k] = packed_taps(
                row, 1, lambda near: value, lambda near: packed[0, near, :] * packed[1, near, :])

    def quotas(g):
        for k, x, y in members:
            row, at = own_tile(g * quad + x, y)
            value = parts_e[k]

            def spread(f):
                return jnp.where(both_ends, pltpu.roll(value, LANES - 1 - 2 * f, 1), 0.0)

            inverted = 1.0 / (gathered[pl.ds(at, TILE), :] + spread(flux))
            for f in range(nspec):
                qbuf[f, pl.ds(row, TILE), :] = (qbuf[f, pl.ds(row, TILE), :] + spread(f)) * inverted

    def quota_pack(g):
        for k, x, y in members:
            row, at = own_tile(g * quad + x, y)
            zs_f[2, pl.ds(at, TILE), :] = pack([qbuf[f, pl.ds(row, TILE), :] for f in range(nspec)], 0)

    def scatter_main(t):
        row, at = own_tile(t // tiles, t % tiles) if isinstance(t, int) else own_row(t)
        row = row - (pitch + TILE)
        taps = []
        for a, b, position in BLOCK:
            near = pl.ds(row + (pitch + TILE - a * pitch - b), TILE)
            source = codes[0, near, :]
            center = None if position == 12 else source
            taps.append(((source, center, source), position, reader(qbuf, near)))
        keep_sums(0, masked_sums(taps, 0, nspec), 0)

    def scatter_close(t):
        row, at = own_tile(t // tiles, t % tiles) if isinstance(t, int) else own_row(t)
        for f in range(nspec):
            wbuf[f, pl.ds(row, TILE), :] = merged(0, f, True)

    def scatter_strip(j):
        x = j * TILE
        for way, (b, y) in enumerate(((1, -1), (-1, ny))):
            taps = []
            for a in (-1, 0, 1):
                source = codes[0, pl.ds(first(1) + (x - a) * pitch + y, TILE, stride=pitch), :]
                taps.append(((source, source, source), 9 * (a + 1) + 3 * (b + 1), reader(yr_q.at[way], pl.ds(TILE + x - a, TILE))))
            keep_sums(way, masked_sums(taps, 0, nspec), 0)

    def scatter_strip_close(j):
        for way, y in enumerate((0, ny - 1)):
            where = pl.ds(first(1) + j * TILE * pitch + y, TILE, stride=pitch)
            for f in range(nspec):
                wbuf[f, where, :] = wbuf[f, where, :] + merged(way, f, True)

    def scatter_plane(way):
        a, x = ((1, 0), (-1, nx + 1))[way]
        for k in range(tiles):
            taps = []
            for b in (-1, 0, 1):
                source = codes[0, pl.ds(first(x) + k * TILE - b, TILE), :]
                taps.append(((source, source, source), 9 * (a + 1) + 3 * (b + 1), reader(xr_q.at[way], pl.ds(TILE + k * TILE - b, TILE))))
            keep_sums(way * tiles + k, masked_sums(taps, 0, nspec), 0)

    def scatter_plane_close(way):
        x = (0, nx - 1)[way]
        for k in range(tiles):
            row, at = own_tile(x, k)
            for f in range(nspec):
                wbuf[f, pl.ds(row, TILE), :] = wbuf[f, pl.ds(row, TILE), :] + merged(way * tiles + k, f, True)

    def scatter_ends(g):
        for k, x, y in members:
            row, at = own_tile(g * quad + x, y)
            parts_e[k] = packed_taps(row, -1, lambda near: codes[1, near, :], lambda near: packed[2, near, :])

    def finals(g):
        for k, x, y in members:
            row, at = own_tile(g * quad + x, y)
            own = pl.ds(at, TILE)
            value, factor = parts_e[k], scaling[own, :]
            for f in range(nspec):
                spread = jnp.where(both_ends, pltpu.roll(value, LANES - 1 - 2 * f, 1), 0.0)
                out[f, own, :] = factor * (wbuf[f, pl.ds(row, TILE), :] + spread)

    blank(codes, 0, 2)
    loads[0].wait()
    loads[1].wait()
    lax.fori_loop(0, nx, fill, 0, unroll=8)
    pl.semaphore_wait(barrier, greeted)
    code_z.start()
    code_own.start()
    for copy in loads[2:]:
        copy.wait()
    totals = tuple(jnp.zeros((TILE, LANES), jnp.float32) for _ in range(nspec))
    totals = lax.fori_loop(0, nx, prepare, totals, unroll=2)
    local = jnp.concatenate(
        [jnp.sum(total, axis=0, keepdims=True) for total in totals]
        + [jnp.zeros((peers.shape[2] - nspec, LANES), jnp.float32)],
        axis=0,
    )
    reduction = total_over(local)
    code_z.receive()
    code_packed.start()
    raw_all.start()
    lax.fori_loop(0, nx, raw_pack, 0, unroll=4)
    raw_z.start()
    lax.fori_loop(0, nx, shift, 0, unroll=8)
    blank(packed, 0, 3)
    raw_all.blank()
    w_all.blank()
    q_all.blank()
    pad_zeros(wbuf, fields)
    pad_zeros(qbuf, nspec)
    code_own.receive()
    code_packed.receive()
    raw_z.receive()
    raw_packed.start()
    pipelined([count_taps, weigh, weigh_pack], nx // quad)
    w_z.start()
    w_all.start()

    def relay_w():
        w_z.receive()
        w_packed.start()

    pipelined([gather_main, gather_close], nx * tiles, (nx * tiles // 4, relay_w))
    raw_all.receive()
    raw_packed.receive()
    w_all.receive()
    w_packed.receive()
    next(reduction)
    pipelined([gather_strip, gather_strip_close], nx // TILE)
    for stage in (gather_plane, gather_plane_close):
        stage(0)
        stage(1)
    edge_ends()
    edge_quotas()
    q_all.start_filled()
    pipelined([gather_ends, quotas, quota_pack], nx // quad)
    q_z.start()

    def relay_q():
        q_z.receive()
        q_packed.start()
        next(reduction)

    pipelined([scatter_main, scatter_close], nx * tiles, (nx * tiles // 5, relay_q))
    q_all.receive()
    q_packed.receive()
    next(reduction)
    pipelined([scatter_strip, scatter_strip_close], nx // TILE)
    for stage in (scatter_plane, scatter_plane_close):
        stage(0)
        stage(1)
    pipelined([scatter_ends, finals], nx // quad)
    next(reduction, None)
    flat = [part for part in everything if not isinstance(part, Depth)]
    deep = [part for part in everything if isinstance(part, Depth)]

    def drain(copies):
        for copy in copies:
            copy.wait_send()

    for k, (dx, dy) in enumerate(WAYS):
        pl.when(exists(dx, dy))(functools.partial(drain, [part.copies[k] for part in flat]))
    pl.when(above_z)(functools.partial(drain, [part.copies[0] for part in deep]))
    pl.when(below_z)(functools.partial(drain, [part.copies[1] for part in deep]))


def per_device(provisional, cut_flag, cut_code, volume_level, area_level):
    nspec, nx, ny, nz = provisional.shape
    assert nz == LANES and ny % TILE == 0 and nx % TILE == 0
    own = nx * ny
    tiles = ny // TILE
    rows = 2 * TILE + (nx + 2) * (ny + TILE)
    most = max(lax.axis_size(axis) for axis in AXES)
    cells = own * nz * math.prod(lax.axis_size(axis) for axis in AXES)
    fields = nspec + 1
    f32, i32 = jnp.float32, jnp.int32
    vmem = pl.BlockSpec(memory_space=pltpu.VMEM)
    hbm = pl.BlockSpec(memory_space=pltpu.HBM)
    shapes = [
        ((fields, own, nz), f32), ((own, nz), i32), ((own, nz), i32), ((own, nz), i32), ((own, nz), i32),
        ((2, rows, nz), i32), ((fields, rows, nz), f32), ((nspec, rows, nz), f32), ((3, rows, nz), f32),
        ((2, own, nz), i32), ((own, nz), i32),
        ((own, nz), i32), ((own, nz), i32),
        ((3, own, nz), f32), ((3, own, nz), f32), ((3, own, nz), f32),
        ((2, 2, nx, nz), i32), ((2, 2, nx, nz), i32), ((2, 4, TILE, nz), i32), ((2, 4, TILE, nz), i32),
        ((2, 3, nx, nz), f32), ((2, 3, nx, nz), f32), ((3, 4, TILE, nz), f32), ((3, 4, TILE, nz), f32),
    ]
    for n in (fields, 1, nspec):
        high = -(-n // TILE) * TILE
        shapes += [
            ((2, n, ny + 2 * TILE, nz), f32), ((2, n, nx, nz), f32), ((2, n, nx + 2 * TILE, nz), f32),
            ((4, high, nz), f32), ((4, high, nz), f32),
        ]
    high = -(-nspec // TILE) * TILE
    shapes += [
        ((2, nspec, ny, nz), f32), ((own, nz), f32), ((1, own, nz), f32), ((own, nz), f32), ((own, nz), f32),
        ((4 * tiles, 4, TILE, nz), i32), ((2 * tiles, 3, fields, TILE, nz), f32), ((max(4 * tiles, 2 * (tiles + nx // TILE)), TILE, nz), f32),
        ((3, most, high, nz), f32),
    ]
    dma = pltpu.SemaphoreType.DMA
    out, change = pl.pallas_call(
        functools.partial(kernel, nx, ny, 1.0 / math.sqrt(cells)),
        out_shape=(
            jax.ShapeDtypeStruct((nspec, own, nz), f32),
            jax.ShapeDtypeStruct((high, nz), f32),
        ),
        in_specs=[hbm] * 5,
        out_specs=(vmem, vmem),
        scratch_shapes=[pltpu.VMEM(shape, kind) for shape, kind in shapes]
        + [
            dma((5,)), dma((4, 2)), dma((4, 2)), dma((8, 8)), dma((8, 8)), dma((3, most)), dma((3, most)),
        ],
        compiler_params=pltpu.CompilerParams(
            collective_id=0, has_side_effects=True, vmem_limit_bytes=26 * 1024 * 1024
        ),
    )(
        *[pltpu.with_memory_space_constraint(x, pltpu.HBM) for x in (
        provisional.reshape(nspec, own, nz),
        cut_flag.reshape(own, nz),
        cut_code.reshape(own, nz),
        volume_level.reshape(own, nz),
        area_level.reshape(own, nz))]
    )
    return out.reshape(provisional.shape), change[:nspec, 0]


def solution(mesh):
    spec = P("gx", "gy", "gz")
    wide = P(None, "gx", "gy", "gz")
    return jax.shard_map(
        per_device, mesh=mesh, in_specs=(wide, spec, spec, spec, spec), out_specs=(wide, P()), check_vma=False
    )
```

```python
import functools
import math

import jax
import jax.numpy as jnp
from jax import lax
from jax.experimental import pallas as pl
from jax.experimental.pallas import tpu as pltpu
from jax.sharding import PartitionSpec as P

CENTER = 8192
BLOCK = [(a, b, 9 * (a + 1) + 3 * (b + 1)) for a in (-1, 0, 1) for b in (-1, 0, 1)]
AXES = ("gx", "gy", "gz")
WAYS = [(1, 0), (-1, 0), (0, 1), (0, -1), (1, 1), (1, -1), (-1, 1), (-1, -1)]
MESH = pl.DeviceIdType.MESH
LANES = 128
TILE = 8


def pipelined(stages, count, hook=None):
    depth = len(stages)

    def step(i, lowest, highest):
        for k in reversed(range(lowest, highest)):
            stages[k](i - k)

    for i in range(min(depth - 1, count)):
        step(i, 0, i + 1)

    def body(i, carry):
        step(i, 0, depth)
        return carry

    low = depth - 1
    if hook is not None:
        at, action = hook
        lax.fori_loop(low, at, body, 0)
        action()
        low = at
    lax.fori_loop(low, count, body, 0)
    for i in range(count, count + depth - 1):
        step(i, i - count + 1, depth)


def kernel(
    nx, ny, scale,
    prov_h, flag_h, code_h, vol_h, area_h,
    out, change,
    raw, flag, code, vol, area,
    codes, wbuf, qbuf, packed, shifted, edge,
    zl_i, zr_i, zs_f, zl_f, zr_f,
    ys_i, yr_i, cs_i, cr_i, ys_p, yr_p, cs_p, cr_p,
    xr_r, ys_r, yr_r, cs_r, cr_r, xr_w, ys_w, yr_w, cs_w, cr_w, xr_q, ys_q, yr_q, cs_q, cr_q, xs_q, xr_c, ys_c, yr_c, cs_c, cr_c,
    volumes, weights, gathered, scaling, parts_i, parts_f, parts_e, peers,
    load, z_send, z_recv, send, recv, peer_send, peer_recv,
):
    nspec = prov_h.shape[0]
    pitch = ny + TILE
    tiles = ny // TILE
    here = {axis: lax.axis_index(axis) for axis in AXES}
    size = {axis: lax.axis_size(axis) for axis in AXES}
    lane = lax.broadcasted_iota(jnp.int32, (TILE, LANES), 1)
    odd = (lane & 1) == 1
    first_lane = lane == 0
    last_lane = lane == LANES - 1
    both_ends = first_lane | last_lane
    fields = nspec + 1
    flux = nspec

    inputs = [(flag_h, flag), (code_h, code), (vol_h, vol), (area_h, area), (prov_h, raw.at[pl.ds(0, nspec)])]
    loads = [pltpu.make_async_copy(src, dst, load.at[k]) for k, (src, dst) in enumerate(inputs)]
    for copy in loads:
        copy.start()

    def moved(axis, step):
        return lax.rem(here[axis] + (step + size[axis]), size[axis])

    barrier = pltpu.get_barrier_semaphore()
    near_x = lax.min(here["gx"], 1) + lax.min(size["gx"] - 1 - here["gx"], 1)
    near_y = lax.min(here["gy"], 1) + lax.min(size["gy"] - 1 - here["gy"], 1)
    near_z = lax.min(here["gz"], 1) + lax.min(size["gz"] - 1 - here["gz"], 1)
    greeted = (near_x + 1) * (near_y + 1) * (near_z + 1) - 1
    for axis, near in (("gx", near_x), ("gy", near_y), ("gz", near_z)):
        if size[axis] > 4:
            greeted = greeted + (size[axis] - 1 - near)

    def greet(target):
        pl.semaphore_signal(barrier, inc=1, device_id=target, device_id_type=MESH)

    def first(x):
        return TILE + x * pitch

    def own_tile(x, k):
        row = (TILE + pitch + k * TILE) + x * pitch
        at = x * ny + k * TILE
        if isinstance(x, int):
            return row, at
        return pl.multiple_of(row, TILE), pl.multiple_of(at, TILE)

    def side(axis, step):
        return here[axis] < size[axis] - 1 if step > 0 else here[axis] > 0

    def exists(dx, dy):
        found = None
        for axis, step in (("gx", dx), ("gy", dy)):
            if step:
                there = side(axis, step)
                found = there if found is None else jnp.logical_and(found, there)
        return found

    below_z, above_z = side("gz", -1), side("gz", 1)
    for dx, dy in WAYS:
        around = {"gx": moved("gx", dx), "gy": moved("gy", dy)}
        pl.when(exists(dx, dy))(functools.partial(greet, around))
        for dz in (-1, 1):
            there = jnp.logical_and(exists(dx, dy), above_z if dz > 0 else below_z)
            pl.when(there)(functools.partial(greet, {**around, "gz": moved("gz", dz)}))
    pl.when(below_z)(functools.partial(greet, {"gz": moved("gz", -1)}))
    pl.when(above_z)(functools.partial(greet, {"gz": moved("gz", 1)}))
    for axis in AXES:
        if size[axis] > 4:
            for k in range(2, size[axis]):
                pl.when(here[axis] >= k)(functools.partial(greet, {axis: moved(axis, -k)}))
                pl.when(here[axis] + k < size[axis])(functools.partial(greet, {axis: moved(axis, k)}))

    def edge_row(step):
        return ny - 1 if step > 0 else 0

    def halo_row(step):
        return ny if step > 0 else -1

    def blank(buf, low, high):
        zeros = jnp.zeros((ny, LANES), buf.dtype)
        row_zeros = jnp.zeros((TILE, LANES), buf.dtype)
        one = jnp.zeros((1, LANES), buf.dtype)

        def plane(step):
            def body(f, carry):
                buf[f, pl.ds(first(nx + 1 if step > 0 else 0), ny), :] = zeros
                return carry
            lax.fori_loop(low, high, body, 0)

        def row(step):
            def body(f, carry):
                for x in range(0, nx, TILE):
                    buf[f, pl.ds(first(x + 1) + halo_row(step), TILE, stride=pitch), :] = row_zeros
                return carry
            lax.fori_loop(low, high, body, 0)

        def corner(dx, dy):
            def body(f, carry):
                buf[f, pl.ds(first(nx + 1 if dx > 0 else 0) + halo_row(dy), 1), :] = one
                return carry
            lax.fori_loop(low, high, body, 0)

        for dx, dy in WAYS:
            action = functools.partial(plane, dx) if dy == 0 else (
                functools.partial(row, dy) if dx == 0 else functools.partial(corner, dx, dy))
            pl.when(jnp.logical_not(exists(dx, dy)))(action)

    class Unit:
        def __init__(self, number, buf, low, high, ys, yr, cs, cr, corner):
            self.buf, self.low, self.high = buf, low, high
            self.ys, self.yr, self.cs, self.cr, self.corner = ys, yr, cs, cr, corner
            n = high - low
            ends_of = {1: (nx, 0), -1: (1, nx + 1)}
            self.copies = []
            for k, (dx, dy) in enumerate(WAYS):
                if dy == 0:
                    here_x, there_x = ends_of[dx]
                    source = buf.at[pl.ds(low, n), pl.ds(first(here_x), ny), :]
                    landing = buf.at[pl.ds(low, n), pl.ds(first(there_x), ny), :]
                elif dx == 0:
                    way = 0 if dy > 0 else 1
                    source, landing = ys.at[way, pl.ds(low, n)], yr.at[way, pl.ds(low, n)]
                else:
                    source, landing = cs.at[corner, k - 4], cr.at[corner, k - 4]
                self.copies.append(
                    pltpu.make_async_remote_copy(
                        src_ref=source, dst_ref=landing,
                        send_sem=send.at[number, k], recv_sem=recv.at[number, k],
                        device_id={"gx": moved("gx", dx), "gy": moved("gy", dy)}, device_id_type=MESH,
                    )
                )

        def start(self):
            buf = self.buf
            for k, (dx, dy) in enumerate(WAYS):
                if dy == 0:
                    pl.when(exists(dx, dy))(self.copies[k].start)

            def gather(f, carry):
                for x in range(0, nx, TILE):
                    for way, step in ((0, 1), (1, -1)):
                        self.ys[way, f, pl.ds(x, TILE), :] = buf[f, pl.ds(first(x + 1) + edge_row(step), TILE, stride=pitch), :]
                for k, (dx, dy) in enumerate(WAYS[4:]):
                    row = first(nx if dx > 0 else 1) + edge_row(dy)
                    self.cs[self.corner, k, pl.ds(f - self.low, 1), :] = buf[f, pl.ds(row, 1), :]
                return carry

            lax.fori_loop(self.low, self.high, gather, 0)
            for k, (dx, dy) in enumerate(WAYS):
                if dy != 0:
                    pl.when(exists(dx, dy))(self.copies[k].start)

        def receive(self):
            buf = self.buf
            for k, (dx, dy) in enumerate(WAYS):
                pl.when(exists(-dx, -dy))(self.copies[k].wait_recv)

            def rows(way, step):
                def body(f, carry):
                    for x in range(0, nx, TILE):
                        buf[f, pl.ds(first(x + 1) + halo_row(-step), TILE, stride=pitch), :] = self.yr[way, f, pl.ds(x, TILE), :]
                    return carry
                lax.fori_loop(self.low, self.high, body, 0)

            def corner(k, dx, dy):
                def body(f, carry):
                    row = first(0 if dx > 0 else nx + 1) + halo_row(-dy)
                    buf[f, pl.ds(row, 1), :] = self.cr[self.corner, k, pl.ds(f - self.low, 1), :]
                    return carry
                lax.fori_loop(self.low, self.high, body, 0)

            for way, step in ((0, 1), (1, -1)):
                pl.when(exists(0, -step))(functools.partial(rows, way, step))
            for k, (dx, dy) in enumerate(WAYS[4:]):
                pl.when(exists(-dx, -dy))(functools.partial(corner, k, dx, dy))

        def finish(self):
            for k, (dx, dy) in enumerate(WAYS):
                pl.when(exists(dx, dy))(self.copies[k].wait_send)

    class Depth:
        def __init__(self, number, zs, zl, zr, buf, plane):
            self.zl, self.zr, self.buf, self.plane = zl, zr, buf, plane
            self.copies = [
                pltpu.make_async_remote_copy(
                    src_ref=zs, dst_ref=landing,
                    send_sem=z_send.at[number, way], recv_sem=z_recv.at[number, way],
                    device_id={"gz": moved("gz", step)}, device_id_type=MESH,
                )
                for way, (landing, step) in enumerate(((zl, 1), (zr, -1)))
            ]

        def start(self):
            pl.when(above_z)(self.copies[0].start)
            pl.when(below_z)(self.copies[1].start)

        def receive(self):
            pl.when(below_z)(self.copies[0].wait_recv)
            pl.when(above_z)(self.copies[1].wait_recv)
            zero = jnp.zeros((TILE, LANES), self.buf.dtype)

            def place(x, carry):
                for k in range(tiles):
                    row, at = own_tile(x, k)
                    low = jnp.where(below_z, pltpu.roll(self.zl[pl.ds(at, TILE), :], 1, 1), zero)
                    high = jnp.where(above_z, pltpu.roll(self.zr[pl.ds(at, TILE), :], LANES - 1, 1), zero)
                    self.buf[self.plane, pl.ds(row, TILE), :] = jnp.where(odd, low, high)
                return carry

            lax.fori_loop(0, nx, place, 0, unroll=8)

        def finish(self):
            pl.when(above_z)(self.copies[0].wait_send)
            pl.when(below_z)(self.copies[1].wait_send)

    class Faces:
        def __init__(self, number, buf, n, start, step, landing, xs=None, dz=0):
            self.dz = dz
            self.buf, self.n, self.first_row, self.step, self.xs = buf, n, start, step, xs
            self.xr, self.ys, self.yr, self.cs, self.cr = landing
            self.copies = []
            for k, (dx, dy) in enumerate(WAYS):
                way = 0 if dx + dy > 0 else 1
                if dy == 0:
                    if xs is None:
                        source = buf.at[pl.ds(0, n), pl.ds(start + (nx - 1 if dx > 0 else 0) * step, ny), :]
                    else:
                        source = xs.at[way]
                    target = self.xr.at[way, pl.ds(0, n), pl.ds(TILE, ny), :]
                elif dx == 0:
                    source, target = self.ys.at[way], self.yr.at[way, pl.ds(0, n), pl.ds(TILE, nx), :]
                else:
                    source, target = self.cs.at[k - 4], self.cr.at[k - 4]
                self.copies.append(
                    pltpu.make_async_remote_copy(
                        src_ref=source, dst_ref=target,
                        send_sem=send.at[number, k], recv_sem=recv.at[number, k],
                        device_id={"gx": moved("gx", dx), "gy": moved("gy", dy), "gz": moved("gz", dz)}, device_id_type=MESH,
                    )
                )

        def there(self, dx, dy):
            if self.dz == 0:
                return exists(dx, dy)
            return jnp.logical_and(exists(dx, dy), above_z if self.dz > 0 else below_z)

        def incoming(self, dx, dy):
            if self.dz == 0:
                return exists(-dx, -dy)
            return jnp.logical_and(exists(-dx, -dy), below_z if self.dz > 0 else above_z)

        def land(self):
            for k, (dx, dy) in enumerate(WAYS):
                pl.when(self.incoming(dx, dy))(self.copies[k].wait_recv)

        def blank(self):
            zeros = jnp.zeros((TILE, LANES), jnp.float32)

            def borders(f, carry):
                for way in range(2):
                    for at in (0, TILE + ny):
                        self.xr[way, f, pl.ds(at, TILE), :] = zeros
                    for at in (0, TILE + nx):
                        self.yr[way, f, pl.ds(at, TILE), :] = zeros
                return carry

            lax.fori_loop(0, self.n, borders, 0)

            def clear(ref, way, extent):
                def body(f, carry):
                    ref[way, f, pl.ds(TILE, extent), :] = jnp.zeros((extent, LANES), jnp.float32)
                    return carry
                lax.fori_loop(0, self.n, body, 0)

            for way, step in ((0, 1), (1, -1)):
                pl.when(jnp.logical_not(exists(-step, 0)))(functools.partial(clear, self.xr, way, ny))
                pl.when(jnp.logical_not(exists(0, -step)))(functools.partial(clear, self.yr, way, nx))

        def collect(self):
            buf, step = self.buf, self.step

            def gather(f, carry):
                for x in range(0, nx, TILE):
                    for way, toward in ((0, 1), (1, -1)):
                        row = self.first_row + x * step + edge_row(toward)
                        self.ys[way, f, pl.ds(x, TILE), :] = buf[f, pl.ds(row, TILE, stride=step), :]
                for k, (dx, dy) in enumerate(WAYS[4:]):
                    row = self.first_row + (nx - 1 if dx > 0 else 0) * step + edge_row(dy)
                    self.cs[k, pl.ds(f, 1), :] = buf[f, pl.ds(row, 1), :]
                return carry

            lax.fori_loop(0, self.n, gather, 0)

        def launch(self):
            for k in range(8):
                pl.when(self.there(*WAYS[k]))(self.copies[k].start)

        def start_filled(self):
            def corners(f, carry):
                for k, (dx, dy) in enumerate(WAYS[4:]):
                    self.cs[k, pl.ds(f, 1), :] = self.xs[0 if dx > 0 else 1, f, pl.ds(edge_row(dy), 1), :]
                return carry

            for k in range(4):
                pl.when(exists(*WAYS[k]))(self.copies[k].start)
            lax.fori_loop(0, self.n, corners, 0)
            for k in range(4, 8):
                pl.when(exists(*WAYS[k]))(self.copies[k].start)

        def receive(self):
            for k, (dx, dy) in enumerate(WAYS):
                pl.when(exists(-dx, -dy))(self.copies[k].wait_recv)

            def corner(k, dx, dy):
                way = 0 if dy > 0 else 1
                at = TILE - 1 if dx > 0 else TILE + nx

                def body(f, carry):
                    self.yr[way, f, pl.ds(at, 1), :] = self.cr[k, pl.ds(f, 1), :]
                    return carry
                lax.fori_loop(0, self.n, body, 0)

            for k, (dx, dy) in enumerate(WAYS[4:]):
                pl.when(exists(-dx, -dy))(functools.partial(corner, k, dx, dy))

        def finish(self):
            for k, (dx, dy) in enumerate(WAYS):
                pl.when(self.there(dx, dy))(self.copies[k].wait_send)

    def pad_zeros(buf, n):
        zeros = jnp.zeros((TILE, LANES), jnp.float32)

        def body(f, carry):
            for p in range(nx + 3):
                buf[f, pl.ds(p * pitch, TILE), :] = zeros
            for p in (0, nx + 1):
                for k in range(tiles):
                    buf[f, pl.ds(first(p) + k * TILE, TILE), :] = zeros
            return carry

        lax.fori_loop(0, n, body, 0)

    code_z = Depth(0, edge.at[0], zl_i, zr_i, codes, 1)
    code_own = Unit(0, codes, 0, 1, ys_i, yr_i, cs_i, cr_i, 0)
    code_up = Faces(1, edge, 1, 0, ny, (xr_c.at[0], ys_c, yr_c.at[0], cs_c, cr_c.at[0]), None, 1)
    code_down = Faces(8, edge, 1, 0, ny, (xr_c.at[1], ys_c, yr_c.at[1], cs_c, cr_c.at[1]), None, -1)
    raw_z = Depth(1, zs_f.at[0], zl_f.at[0], zr_f.at[0], packed, 0)
    raw_all = Faces(2, raw, fields, 0, ny, (xr_r, ys_r, yr_r, cs_r, cr_r))
    raw_packed = Unit(3, packed, 0, 1, ys_p, yr_p, cs_p, cr_p, 0)
    w_z = Depth(2, zs_f.at[1], zl_f.at[1], zr_f.at[1], packed, 1)
    w_all = Faces(4, weights, 1, 0, ny, (xr_w, ys_w, yr_w, cs_w, cr_w))
    w_packed = Unit(5, packed, 1, 2, ys_p, yr_p, cs_p, cr_p, 1)
    q_z = Depth(3, zs_f.at[2], zl_f.at[2], zr_f.at[2], packed, 2)
    q_all = Faces(6, qbuf, nspec, first(1), pitch, (xr_q, ys_q, yr_q, cs_q, cr_q), xs_q)
    q_packed = Unit(7, packed, 2, 3, ys_p, yr_p, cs_p, cr_p, 2)
    everything = [
        code_z, code_own, raw_z, raw_all, raw_packed, w_z, w_all, w_packed, q_z, q_all, q_packed,
    ]

    def join_code_ends():
        code_up.land()
        code_down.land()
        zero = jnp.zeros((TILE, LANES), jnp.int32)

        def mixed(low, high):
            low = jnp.where(below_z, pltpu.roll(low, 1, 1), zero)
            high = jnp.where(above_z, pltpu.roll(high, LANES - 1, 1), zero)
            return jnp.where(odd, low, high)

        def plane(way, step):
            for k in range(tiles):
                near = pl.ds(TILE + k * TILE, TILE)
                row = first(0 if step > 0 else nx + 1) + k * TILE
                codes[1, pl.ds(row, TILE), :] = mixed(xr_c[0, way, 0, near, :], xr_c[1, way, 0, near, :])

        def rows(way, step):
            for x in range(0, nx, TILE):
                near = pl.ds(TILE + x, TILE)
                row = first(x + 1) + halo_row(-step)
                codes[1, pl.ds(row, TILE, stride=pitch), :] = mixed(yr_c[0, way, 0, near, :], yr_c[1, way, 0, near, :])

        def corner(k, dx, dy):
            row = first(0 if dx > 0 else nx + 1) + halo_row(-dy)
            codes[1, pl.ds(row, 1), :] = mixed(cr_c[0, k], cr_c[1, k])[:1]

        for way, step in ((0, 1), (1, -1)):
            pl.when(exists(-step, 0))(functools.partial(plane, way, step))
            pl.when(exists(0, -step))(functools.partial(rows, way, step))
        for k, (dx, dy) in enumerate(WAYS[4:]):
            pl.when(exists(-dx, -dy))(functools.partial(corner, k, dx, dy))

    def total_over(value):
        for number, axis in enumerate(AXES):
            n, me = size[axis], here[axis]
            peers[number, me] = value
            copies = [
                pltpu.make_async_remote_copy(
                    src_ref=peers.at[number, me], dst_ref=peers.at[number, me],
                    send_sem=peer_send.at[number, k], recv_sem=peer_recv.at[number, k],
                    device_id={axis: lax.rem(me + k, n)}, device_id_type=MESH,
                )
                for k in range(1, n)
            ]
            for copy in copies:
                copy.start()
            yield
            for copy in copies:
                copy.wait()
            value = peers[number, 0]
            for k in range(1, n):
                value = value + peers[number, k]
        sums = jnp.broadcast_to(jnp.sum(value, axis=1, keepdims=True) * scale, value.shape)
        places = lax.broadcasted_iota(jnp.int32, value.shape, 1) == lax.broadcasted_iota(jnp.int32, value.shape, 0)
        change[...] = jnp.sum(jnp.where(places, sums, 0.0), axis=0)[:nspec]

    def fractions(own):
        is_cut = flag[own, :] == 1
        volume = jnp.where(is_cut, vol[own, :], 256).astype(jnp.float32) * (1.0 / 256.0)
        face = jnp.where(is_cut, area[own, :], 256).astype(jnp.float32) * (1.0 / 256.0)
        return volume, face

    def fill(x, carry):
        for k in range(tiles):
            row, at = own_tile(x, k)
            own = pl.ds(at, TILE)
            value = jnp.where(flag[own, :] == 1, code[own, :] | CENTER, CENTER)
            codes[0, pl.ds(row, TILE), :] = value
            low = jnp.broadcast_to(value[:, :1], (TILE, LANES))
            high = lax.shift_right_logical(jnp.broadcast_to(value[:, LANES - 1:], (TILE, LANES)), 2)
            edge[0, own, :] = jnp.where(odd, low, high)
        return carry

    def shift(x, carry):
        for k in range(tiles):
            row, at = own_tile(x, k)
            own = pl.ds(at, TILE)
            value = codes[0, pl.ds(row, TILE), :]
            shifted[0, own, :] = jnp.where(first_lane, 0, pltpu.roll(value, 1, 1))
            shifted[1, own, :] = jnp.where(last_lane, 0, pltpu.roll(value, LANES - 1, 1))
        return carry

    def prepare(x, totals):
        for k in range(tiles):
            _, at = own_tile(x, k)
            own = pl.ds(at, TILE)
            volume, face = fractions(own)
            volumes[own, :] = volume
            raw[nspec, own, :] = face
            totals = tuple(totals[s] + volume * raw[s, own, :] for s in range(nspec))
        return totals

    def raw_pack(x, carry):
        for k in range(tiles):
            _, at = own_tile(x, k)
            own = pl.ds(at, TILE)
            zs_f[0, own, :] = pack([raw[f, own, :] for f in range(fields)], 0)
        return carry

    def masked_sums(taps, low, high):
        zero = jnp.zeros((TILE, LANES), jnp.float32)
        sums = [[None] * (high - low) for _ in range(3)]
        for sources, position, value_of in taps:
            present = [
                None if source is None else (source & (1 << (position + k))) != 0 for k, source in enumerate(sources)
            ]
            for f in range(low, high):
                value = value_of(f)
                for k in range(3):
                    term = value if present[k] is None else jnp.where(present[k], value, zero)
                    old = sums[k][f - low]
                    sums[k][f - low] = term if old is None else old + term
        return sums

    def keep_sums(slot, sums, low):
        for m in range(3):
            for f, value in enumerate(sums[m]):
                parts_f[slot, m, low + f] = value

    def merged(slot, f, wrap):
        if wrap:
            up, down = pltpu.roll(parts_f[slot, 2, f], 1, 1), pltpu.roll(parts_f[slot, 0, f], LANES - 1, 1)
            up, down = jnp.where(first_lane, 0.0, up), jnp.where(last_lane, 0.0, down)
        else:
            up, down = pltpu.roll(parts_f[slot, 2, f], LANES - 1, 1), pltpu.roll(parts_f[slot, 0, f], 1, 1)
        return parts_f[slot, 1, f] + up + down

    def packed_taps(row, step, source, value_of):
        zero = jnp.zeros((TILE, LANES), jnp.float32)
        total = None
        row = row - (pitch + TILE)
        for a, b, position in BLOCK:
            near = pl.ds(row + (pitch + TILE + step * (a * pitch + b)), TILE)
            term = jnp.where((source(near) & (1 << position)) != 0, value_of(near), zero)
            total = term if total is None else total + term
        return total

    def pack(values, lowest):
        packed = jnp.zeros((TILE, LANES), jnp.float32)
        for k, value in enumerate(values):
            f = lowest + k
            packed = jnp.where((lane == 2 * f) | (lane == 2 * f + 1), pltpu.roll(value, 2 * f + 1, 1), packed)
        return packed

    quad = 4
    members = [(k, k // tiles, k % tiles) for k in range(quad * tiles)]

    def count_taps(g):
        for k, x, y in members:
            row, at = own_tile(g * quad + x, y)
            sums = [None] * 3
            total = None
            row = row - (pitch + TILE)
            for a, b, position in BLOCK:
                near = pl.ds(row + (pitch + TILE - a * pitch - b), TILE)
                value = codes[0, near, :]
                value = value if position == 0 else lax.shift_right_logical(value, position)
                for m in range(3):
                    term = value & (1 << m)
                    sums[m] = term if sums[m] is None else sums[m] + term
                value = codes[1, near, :]
                value = value if position == 0 else lax.shift_right_logical(value, position)
                total = value & 1 if total is None else total + (value & 1)
            for m in range(3):
                parts_i[k, m] = sums[m]
            parts_i[k, 3] = total

    def weigh(g):
        for k, x, y in members:
            row, at = own_tile(g * quad + x, y)
            own = pl.ds(at, TILE)
            from_end = pltpu.roll(parts_i[k, 3], LANES - 1, 1)
            from_left = pltpu.roll(lax.shift_right_logical(parts_i[k, 2], 2), 1, 1)
            from_right = pltpu.roll(parts_i[k, 0], LANES - 1, 1)
            counted = lax.shift_right_logical(parts_i[k, 1], 1)
            counted = counted + jnp.where(first_lane, from_end, from_left) + jnp.where(last_lane, from_end, from_right)
            share = 1.0 / counted.astype(jnp.float32)
            scaling[own, :] = raw[nspec, own, :] * share
            weight = volumes[own, :] * share
            weights[0, own, :] = weight
            for f in range(fields):
                wbuf[f, pl.ds(row, TILE), :] = weight * raw[f, own, :]

    def weigh_pack(g):
        for k, x, y in members:
            row, at = own_tile(g * quad + x, y)
            own = pl.ds(at, TILE)
            value = weights[0, own, :]
            low = jnp.broadcast_to(value[:, :1], (TILE, LANES))
            high = jnp.broadcast_to(value[:, LANES - 1:], (TILE, LANES))
            zs_f[1, own, :] = jnp.where(odd, low, high)

    def own_row(t):
        x, k = lax.div(t, tiles), lax.rem(t, tiles)
        row = (TILE + pitch) + x * pitch + k * TILE
        if isinstance(t, int):
            return int(row), t * TILE
        return pl.multiple_of(row, TILE), pl.multiple_of(t * TILE, TILE)

    def reader(buf, near):
        return lambda f: buf[f, near, :]

    def weighed(buf, factors, near):
        factor = factors[0, near, :]
        return lambda f: buf[f, near, :] * factor

    def gather_main(t):
        row, at = own_tile(t // tiles, t % tiles) if isinstance(t, int) else own_row(t)
        own = pl.ds(at, TILE)
        right, left, middle = shifted[0, own, :], shifted[1, own, :], codes[0, pl.ds(row, TILE), :]
        taps = []
        base = row - (pitch + TILE)
        for a, b, position in BLOCK:
            center = None if position == 12 else middle
            near = pl.ds(base + (pitch + TILE + a * pitch + b), TILE)
            taps.append(((left, center, right), position, reader(wbuf, near)))
        keep_sums(0, masked_sums(taps, 0, fields), 0)

    def gather_close(t):
        row, at = own_tile(t // tiles, t % tiles) if isinstance(t, int) else own_row(t)
        for f in range(nspec):
            qbuf[f, pl.ds(row, TILE), :] = merged(0, f, False)
        gathered[pl.ds(at, TILE), :] = merged(0, flux, False)

    def gather_strip(j):
        x = j * TILE
        for way, (b, y) in enumerate(((-1, 0), (1, ny - 1))):
            where = pl.ds(x * ny + y, TILE, stride=ny)
            right, left = shifted[0, where, :], shifted[1, where, :]
            middle = codes[0, pl.ds(first(1) + x * pitch + y, TILE, stride=pitch), :]
            taps = []
            for a in (-1, 0, 1):
                near = pl.ds(TILE + x + a, TILE)
                taps.append(((left, middle, right), 9 * (a + 1) + 3 * (b + 1), weighed(yr_r.at[way], yr_w.at[way], near)))
            keep_sums(way, masked_sums(taps, 0, fields), 0)

    def gather_strip_close(j):
        x = j * TILE
        for way, y in enumerate((0, ny - 1)):
            rows = pl.ds(first(1) + x * pitch + y, TILE, stride=pitch)
            for f in range(nspec):
                qbuf[f, rows, :] = qbuf[f, rows, :] + merged(way, f, False)
            where = pl.ds(x * ny + y, TILE, stride=ny)
            gathered[where, :] = gathered[where, :] + merged(way, flux, False)

    def gather_plane(way):
        a, x = ((-1, 0), (1, nx - 1))[way]
        for k in range(tiles):
            row, at = own_tile(x, k)
            own = pl.ds(at, TILE)
            right, left, middle = shifted[0, own, :], shifted[1, own, :], codes[0, pl.ds(row, TILE), :]
            taps = []
            for b in (-1, 0, 1):
                near = pl.ds(TILE + k * TILE + b, TILE)
                taps.append(((left, middle, right), 9 * (a + 1) + 3 * (b + 1), weighed(xr_r.at[way], xr_w.at[way], near)))
            keep_sums(way * tiles + k, masked_sums(taps, 0, fields), 0)

    def gather_plane_close(way):
        x = (0, nx - 1)[way]
        for k in range(tiles):
            row, at = own_tile(x, k)
            for f in range(nspec):
                qbuf[f, pl.ds(row, TILE), :] = qbuf[f, pl.ds(row, TILE), :] + merged(way * tiles + k, f, False)
            own = pl.ds(at, TILE)
            gathered[own, :] = gathered[own, :] + merged(way * tiles + k, flux, False)

    def edge_tiles():
        for way, y in enumerate((ny - 1, 0)):
            for x in range(0, nx, TILE):
                row = first(x + 1) + y
                yield (
                    lambda start: pl.ds(start, TILE, stride=pitch), row,
                    pl.ds(x * ny + y, TILE, stride=ny), ys_q.at[way], pl.ds(x, TILE),
                )
        for way, x in enumerate((nx - 1, 0)):
            for k in range(tiles):
                row, at = own_tile(x, k)
                yield lambda start: pl.ds(start, TILE), row, pl.ds(at, TILE), xs_q.at[way], pl.ds(k * TILE, TILE)

    def edge_ends():
        zero = jnp.zeros((TILE, LANES), jnp.float32)
        for n, (rows, row, own, _, _) in enumerate(edge_tiles()):
            bits = edge[0, own, :]
            total = None
            for a, b, position in BLOCK:
                near = rows(row + a * pitch + b)
                term = jnp.where((bits & (1 << position)) != 0, packed[0, near, :] * packed[1, near, :], zero)
                total = term if total is None else total + term
            parts_e[n] = total

    def edge_quotas():
        for n, (rows, row, own, ref, where) in enumerate(edge_tiles()):
            value = parts_e[n]

            def spread(f):
                return jnp.where(both_ends, pltpu.roll(value, LANES - 1 - 2 * f, 1), 0.0)

            inverted = 1.0 / (gathered[own, :] + spread(flux))
            for f in range(nspec):
                ref[f, where, :] = (qbuf[f, rows(row), :] + spread(f)) * inverted

    def gather_ends(g):
        for k, x, y in members:
            row, at = own_tile(g * quad + x, y)
            value = edge[0, pl.ds(at, TILE), :]
            parts_e[k] = packed_taps(
                row, 1, lambda near: value, lambda near: packed[0, near, :] * packed[1, near, :])

    def quotas(g):
        for k, x, y in members:
            row, at = own_tile(g * quad + x, y)
            value = parts_e[k]

            def spread(f):
                return jnp.where(both_ends, pltpu.roll(value, LANES - 1 - 2 * f, 1), 0.0)

            inverted = 1.0 / (gathered[pl.ds(at, TILE), :] + spread(flux))
            for f in range(nspec):
                qbuf[f, pl.ds(row, TILE), :] = (qbuf[f, pl.ds(row, TILE), :] + spread(f)) * inverted

    def quota_pack(g):
        for k, x, y in members:
            row, at = own_tile(g * quad + x, y)
            zs_f[2, pl.ds(at, TILE), :] = pack([qbuf[f, pl.ds(row, TILE), :] for f in range(nspec)], 0)

    def scatter_main(t):
        row, at = own_tile(t // tiles, t % tiles) if isinstance(t, int) else own_row(t)
        row = row - (pitch + TILE)
        taps = []
        for a, b, position in BLOCK:
            near = pl.ds(row + (pitch + TILE - a * pitch - b), TILE)
            source = codes[0, near, :]
            center = None if position == 12 else source
            taps.append(((source, center, source), position, reader(qbuf, near)))
        keep_sums(0, masked_sums(taps, 0, nspec), 0)

    def scatter_close(t):
        row, at = own_tile(t // tiles, t % tiles) if isinstance(t, int) else own_row(t)
        for f in range(nspec):
            wbuf[f, pl.ds(row, TILE), :] = merged(0, f, True)

    def scatter_strip(j):
        x = j * TILE
        for way, (b, y) in enumerate(((1, -1), (-1, ny))):
            taps = []
            for a in (-1, 0, 1):
                source = codes[0, pl.ds(first(1) + (x - a) * pitch + y, TILE, stride=pitch), :]
                taps.append(((source, source, source), 9 * (a + 1) + 3 * (b + 1), reader(yr_q.at[way], pl.ds(TILE + x - a, TILE))))
            keep_sums(way, masked_sums(taps, 0, nspec), 0)

    def scatter_strip_close(j):
        for way, y in enumerate((0, ny - 1)):
            where = pl.ds(first(1) + j * TILE * pitch + y, TILE, stride=pitch)
            for f in range(nspec):
                wbuf[f, where, :] = wbuf[f, where, :] + merged(way, f, True)

    def scatter_plane(way):
        a, x = ((1, 0), (-1, nx + 1))[way]
        for k in range(tiles):
            taps = []
            for b in (-1, 0, 1):
                source = codes[0, pl.ds(first(x) + k * TILE - b, TILE), :]
                taps.append(((source, source, source), 9 * (a + 1) + 3 * (b + 1), reader(xr_q.at[way], pl.ds(TILE + k * TILE - b, TILE))))
            keep_sums(way * tiles + k, masked_sums(taps, 0, nspec), 0)

    def scatter_plane_close(way):
        x = (0, nx - 1)[way]
        for k in range(tiles):
            row, at = own_tile(x, k)
            for f in range(nspec):
                wbuf[f, pl.ds(row, TILE), :] = wbuf[f, pl.ds(row, TILE), :] + merged(way * tiles + k, f, True)

    def scatter_ends(g):
        for k, x, y in members:
            row, at = own_tile(g * quad + x, y)
            parts_e[k] = packed_taps(row, -1, lambda near: codes[1, near, :], lambda near: packed[2, near, :])

    def finals(g):
        for k, x, y in members:
            row, at = own_tile(g * quad + x, y)
            own = pl.ds(at, TILE)
            value, factor = parts_e[k], scaling[own, :]
            for f in range(nspec):
                spread = jnp.where(both_ends, pltpu.roll(value, LANES - 1 - 2 * f, 1), 0.0)
                out[f, own, :] = factor * (wbuf[f, pl.ds(row, TILE), :] + spread)

    blank(codes, 0, 2)
    loads[0].wait()
    loads[1].wait()
    lax.fori_loop(0, nx, fill, 0, unroll=8)
    pl.semaphore_wait(barrier, greeted)
    code_z.start()
    code_own.start()
    code_up.collect()
    code_up.launch()
    code_down.launch()
    for copy in loads[2:]:
        copy.wait()
    totals = tuple(jnp.zeros((TILE, LANES), jnp.float32) for _ in range(nspec))
    totals = lax.fori_loop(0, nx, prepare, totals, unroll=2)
    local = jnp.concatenate(
        [jnp.sum(total, axis=0, keepdims=True) for total in totals]
        + [jnp.zeros((peers.shape[2] - nspec, LANES), jnp.float32)],
        axis=0,
    )
    reduction = total_over(local)
    raw_all.collect()
    raw_all.launch()
    lax.fori_loop(0, nx, raw_pack, 0, unroll=4)
    raw_z.start()
    lax.fori_loop(0, nx, shift, 0, unroll=8)
    blank(packed, 0, 3)
    raw_all.blank()
    w_all.blank()
    q_all.blank()
    pad_zeros(wbuf, fields)
    pad_zeros(qbuf, nspec)
    raw_z.receive()
    raw_packed.start()
    code_z.receive()
    code_own.receive()
    join_code_ends()
    pipelined([count_taps, weigh, weigh_pack], nx // quad)
    w_z.start()
    w_all.collect()
    w_all.launch()

    def relay_w():
        w_z.receive()
        w_packed.start()

    pipelined([gather_main, gather_close], nx * tiles, (nx * tiles // 4, relay_w))
    raw_all.receive()
    w_all.receive()
    next(reduction)
    pipelined([gather_strip, gather_strip_close], nx // TILE)
    for stage in (gather_plane, gather_plane_close):
        stage(0)
        stage(1)
    raw_packed.receive()
    w_packed.receive()
    edge_ends()
    edge_quotas()
    q_all.start_filled()
    pipelined([gather_ends, quotas, quota_pack], nx // quad)
    q_z.start()

    def relay_q():
        q_z.receive()
        q_packed.start()
        next(reduction)

    pipelined([scatter_main, scatter_close], nx * tiles, (nx * tiles // 5, relay_q))
    q_all.receive()
    next(reduction)
    pipelined([scatter_strip, scatter_strip_close], nx // TILE)
    for stage in (scatter_plane, scatter_plane_close):
        stage(0)
        stage(1)
    q_packed.receive()
    pipelined([scatter_ends, finals], nx // quad)
    next(reduction, None)
    flat = [part for part in everything if not isinstance(part, Depth)]
    deep = [part for part in everything if isinstance(part, Depth)]

    def drain(copies):
        for copy in copies:
            copy.wait_send()

    for k, (dx, dy) in enumerate(WAYS):
        pl.when(exists(dx, dy))(functools.partial(drain, [part.copies[k] for part in flat]))
    code_up.finish()
    code_down.finish()
    pl.when(above_z)(functools.partial(drain, [part.copies[0] for part in deep]))
    pl.when(below_z)(functools.partial(drain, [part.copies[1] for part in deep]))


def per_device(provisional, cut_flag, cut_code, volume_level, area_level):
    nspec, nx, ny, nz = provisional.shape
    assert nz == LANES and ny % TILE == 0 and nx % TILE == 0
    own = nx * ny
    tiles = ny // TILE
    rows = 2 * TILE + (nx + 2) * (ny + TILE)
    most = max(lax.axis_size(axis) for axis in AXES)
    cells = own * nz * math.prod(lax.axis_size(axis) for axis in AXES)
    fields = nspec + 1
    f32, i32 = jnp.float32, jnp.int32
    vmem = pl.BlockSpec(memory_space=pltpu.VMEM)
    hbm = pl.BlockSpec(memory_space=pltpu.HBM)
    shapes = [
        ((fields, own, nz), f32), ((own, nz), i32), ((own, nz), i32), ((own, nz), i32), ((own, nz), i32),
        ((2, rows, nz), i32), ((fields, rows, nz), f32), ((nspec, rows, nz), f32), ((3, rows, nz), f32),
        ((2, own, nz), i32), ((1, own, nz), i32),
        ((own, nz), i32), ((own, nz), i32),
        ((3, own, nz), f32), ((3, own, nz), f32), ((3, own, nz), f32),
        ((2, 2, nx, nz), i32), ((2, 2, nx, nz), i32), ((2, 4, TILE, nz), i32), ((2, 4, TILE, nz), i32),
        ((2, 3, nx, nz), f32), ((2, 3, nx, nz), f32), ((3, 4, TILE, nz), f32), ((3, 4, TILE, nz), f32),
    ]
    for n in (fields, 1, nspec):
        high = -(-n // TILE) * TILE
        shapes += [
            ((2, n, ny + 2 * TILE, nz), f32), ((2, n, nx, nz), f32), ((2, n, nx + 2 * TILE, nz), f32),
            ((4, high, nz), f32), ((4, high, nz), f32),
        ]
    high = -(-nspec // TILE) * TILE
    shapes += [
        ((2, nspec, ny, nz), f32),
        ((2, 2, 1, ny + 2 * TILE, nz), i32), ((2, 1, nx, nz), i32), ((2, 2, 1, nx + 2 * TILE, nz), i32),
        ((4, TILE, nz), i32), ((2, 4, TILE, nz), i32),
        ((own, nz), f32), ((1, own, nz), f32), ((own, nz), f32), ((own, nz), f32),
        ((4 * tiles, 4, TILE, nz), i32), ((2 * tiles, 3, fields, TILE, nz), f32), ((max(4 * tiles, 2 * (tiles + nx // TILE)), TILE, nz), f32),
        ((3, most, high, nz), f32),
    ]
    dma = pltpu.SemaphoreType.DMA
    out, change = pl.pallas_call(
        functools.partial(kernel, nx, ny, 1.0 / math.sqrt(cells)),
        out_shape=(
            jax.ShapeDtypeStruct((nspec, own, nz), f32),
            jax.ShapeDtypeStruct((nspec,), f32),
        ),
        in_specs=[hbm] * 5,
        out_specs=(vmem, vmem),
        scratch_shapes=[pltpu.VMEM(shape, kind) for shape, kind in shapes]
        + [
            dma((5,)), dma((4, 2)), dma((4, 2)), dma((9, 8)), dma((9, 8)), dma((3, most)), dma((3, most)),
        ],
        compiler_params=pltpu.CompilerParams(
            collective_id=0, has_side_effects=True, vmem_limit_bytes=26 * 1024 * 1024
        ),
    )(
        *[pltpu.with_memory_space_constraint(x, pltpu.HBM) for x in (
        provisional.reshape(nspec, own, nz),
        cut_flag.reshape(own, nz),
        cut_code.reshape(own, nz),
        volume_level.reshape(own, nz),
        area_level.reshape(own, nz))]
    )
    return out.reshape(provisional.shape), change


def solution(mesh):
    spec = P("gx", "gy", "gz")
    wide = P(None, "gx", "gy", "gz")
    return jax.shard_map(
        per_device, mesh=mesh, in_specs=(wide, spec, spec, spec, spec), out_specs=(wide, P()), check_vma=False
    )
```

```python
import functools
import math

import jax
import jax.numpy as jnp
from jax import lax
from jax.experimental import pallas as pl
from jax.experimental.pallas import tpu as pltpu
from jax.sharding import PartitionSpec as P

CENTER = 8192
BLOCK = [(a, b, 9 * (a + 1) + 3 * (b + 1)) for a in (-1, 0, 1) for b in (-1, 0, 1)]
AXES = ("gx", "gy", "gz")
WAYS = [(1, 0), (-1, 0), (0, 1), (0, -1), (1, 1), (1, -1), (-1, 1), (-1, -1)]
MESH = pl.DeviceIdType.MESH
LANES = 128
TILE = 8


def pipelined(stages, count, hook=None):
    depth = len(stages)

    def step(i, lowest, highest):
        for k in reversed(range(lowest, highest)):
            stages[k](i - k)

    for i in range(min(depth - 1, count)):
        step(i, 0, i + 1)

    def body(i, carry):
        step(i, 0, depth)
        return carry

    low = depth - 1
    if hook is not None:
        at, action = hook
        lax.fori_loop(low, at, body, 0)
        action()
        low = at
    lax.fori_loop(low, count, body, 0)
    for i in range(count, count + depth - 1):
        step(i, i - count + 1, depth)


def kernel(
    nx, ny, scale,
    prov_h, flag_h, code_h, vol_h, area_h,
    out, change,
    raw, flag, code, vol, area,
    codes, wbuf, qbuf, packed, shifted, edge,
    zl_i, zr_i, zs_f, zl_f, zr_f,
    ys_i, yr_i, cs_i, cr_i, ys_p, yr_p, cs_p, cr_p,
    xr_r, ys_r, yr_r, cs_r, cr_r, xr_w, ys_w, yr_w, cs_w, cr_w, xr_q, ys_q, yr_q, cs_q, cr_q, xs_q, xr_c, ys_c, yr_c, cs_c, cr_c,
    volumes, weights, gathered, scaling, parts_i, parts_f, parts_e, peers,
    load, z_send, z_recv, send, recv, peer_send, peer_recv,
):
    nspec = prov_h.shape[0]
    pitch = ny + TILE
    tiles = ny // TILE
    here = {axis: lax.axis_index(axis) for axis in AXES}
    size = {axis: lax.axis_size(axis) for axis in AXES}
    lane = lax.broadcasted_iota(jnp.int32, (TILE, LANES), 1)
    odd = (lane & 1) == 1
    first_lane = lane == 0
    last_lane = lane == LANES - 1
    both_ends = first_lane | last_lane
    fields = nspec + 1
    flux = nspec

    inputs = [(flag_h, flag), (code_h, code), (vol_h, vol), (area_h, area), (prov_h, raw.at[pl.ds(0, nspec)])]
    loads = [pltpu.make_async_copy(src, dst, load.at[k]) for k, (src, dst) in enumerate(inputs)]
    for copy in loads:
        copy.start()

    def moved(axis, step):
        return lax.rem(here[axis] + (step + size[axis]), size[axis])

    barrier = pltpu.get_barrier_semaphore()
    near_x = lax.min(here["gx"], 1) + lax.min(size["gx"] - 1 - here["gx"], 1)
    near_y = lax.min(here["gy"], 1) + lax.min(size["gy"] - 1 - here["gy"], 1)
    near_z = lax.min(here["gz"], 1) + lax.min(size["gz"] - 1 - here["gz"], 1)
    greeted = (near_x + 1) * (near_y + 1) * (near_z + 1) - 1
    for axis, near in (("gx", near_x), ("gy", near_y), ("gz", near_z)):
        if size[axis] > 4:
            greeted = greeted + (size[axis] - 1 - near)

    def greet(target):
        pl.semaphore_signal(barrier, inc=1, device_id=target, device_id_type=MESH)

    def first(x):
        return TILE + x * pitch

    def own_tile(x, k):
        row = (TILE + pitch + k * TILE) + x * pitch
        at = x * ny + k * TILE
        if isinstance(x, int):
            return row, at
        return pl.multiple_of(row, TILE), pl.multiple_of(at, TILE)

    def side(axis, step):
        return here[axis] < size[axis] - 1 if step > 0 else here[axis] > 0

    def exists(dx, dy):
        found = None
        for axis, step in (("gx", dx), ("gy", dy)):
            if step:
                there = side(axis, step)
                found = there if found is None else jnp.logical_and(found, there)
        return found

    below_z, above_z = side("gz", -1), side("gz", 1)
    for dx, dy in WAYS:
        around = {"gx": moved("gx", dx), "gy": moved("gy", dy)}
        pl.when(exists(dx, dy))(functools.partial(greet, around))
        for dz in (-1, 1):
            there = jnp.logical_and(exists(dx, dy), above_z if dz > 0 else below_z)
            pl.when(there)(functools.partial(greet, {**around, "gz": moved("gz", dz)}))
    pl.when(below_z)(functools.partial(greet, {"gz": moved("gz", -1)}))
    pl.when(above_z)(functools.partial(greet, {"gz": moved("gz", 1)}))
    for axis in AXES:
        if size[axis] > 4:
            for k in range(2, size[axis]):
                pl.when(here[axis] >= k)(functools.partial(greet, {axis: moved(axis, -k)}))
                pl.when(here[axis] + k < size[axis])(functools.partial(greet, {axis: moved(axis, k)}))

    def edge_row(step):
        return ny - 1 if step > 0 else 0

    def halo_row(step):
        return ny if step > 0 else -1

    def blank(buf, low, high):
        zeros = jnp.zeros((ny, LANES), buf.dtype)
        row_zeros = jnp.zeros((TILE, LANES), buf.dtype)
        one = jnp.zeros((1, LANES), buf.dtype)

        def plane(step):
            def body(f, carry):
                buf[f, pl.ds(first(nx + 1 if step > 0 else 0), ny), :] = zeros
                return carry
            lax.fori_loop(low, high, body, 0)

        def row(step):
            def body(f, carry):
                for x in range(0, nx, TILE):
                    buf[f, pl.ds(first(x + 1) + halo_row(step), TILE, stride=pitch), :] = row_zeros
                return carry
            lax.fori_loop(low, high, body, 0)

        def corner(dx, dy):
            def body(f, carry):
                buf[f, pl.ds(first(nx + 1 if dx > 0 else 0) + halo_row(dy), 1), :] = one
                return carry
            lax.fori_loop(low, high, body, 0)

        for dx, dy in WAYS:
            action = functools.partial(plane, dx) if dy == 0 else (
                functools.partial(row, dy) if dx == 0 else functools.partial(corner, dx, dy))
            pl.when(jnp.logical_not(exists(dx, dy)))(action)

    class Unit:
        def __init__(self, number, buf, low, high, ys, yr, cs, cr, corner):
            self.buf, self.low, self.high = buf, low, high
            self.ys, self.yr, self.cs, self.cr, self.corner = ys, yr, cs, cr, corner
            n = high - low
            ends_of = {1: (nx, 0), -1: (1, nx + 1)}
            self.copies = []
            for k, (dx, dy) in enumerate(WAYS):
                if dy == 0:
                    here_x, there_x = ends_of[dx]
                    source = buf.at[pl.ds(low, n), pl.ds(first(here_x), ny), :]
                    landing = buf.at[pl.ds(low, n), pl.ds(first(there_x), ny), :]
                elif dx == 0:
                    way = 0 if dy > 0 else 1
                    source, landing = ys.at[way, pl.ds(low, n)], yr.at[way, pl.ds(low, n)]
                else:
                    source, landing = cs.at[corner, k - 4], cr.at[corner, k - 4]
                self.copies.append(
                    pltpu.make_async_remote_copy(
                        src_ref=source, dst_ref=landing,
                        send_sem=send.at[number, k], recv_sem=recv.at[number, k],
                        device_id={"gx": moved("gx", dx), "gy": moved("gy", dy)}, device_id_type=MESH,
                    )
                )

        def start(self):
            buf = self.buf
            def gather(f, carry):
                for x in range(0, nx, TILE):
                    for way, step in ((0, 1), (1, -1)):
                        self.ys[way, f, pl.ds(x, TILE), :] = buf[f, pl.ds(first(x + 1) + edge_row(step), TILE, stride=pitch), :]
                for k, (dx, dy) in enumerate(WAYS[4:]):
                    row = first(nx if dx > 0 else 1) + edge_row(dy)
                    self.cs[self.corner, k, pl.ds(f - self.low, 1), :] = buf[f, pl.ds(row, 1), :]
                return carry

            lax.fori_loop(self.low, self.high, gather, 0)
            for k in (4, 5, 6, 7, 0, 1, 2, 3):
                pl.when(exists(*WAYS[k]))(self.copies[k].start)

        def receive(self):
            buf = self.buf
            for k, (dx, dy) in enumerate(WAYS):
                pl.when(exists(-dx, -dy))(self.copies[k].wait_recv)

            def rows(way, step):
                def body(f, carry):
                    for x in range(0, nx, TILE):
                        buf[f, pl.ds(first(x + 1) + halo_row(-step), TILE, stride=pitch), :] = self.yr[way, f, pl.ds(x, TILE), :]
                    return carry
                lax.fori_loop(self.low, self.high, body, 0)

            def corner(k, dx, dy):
                def body(f, carry):
                    row = first(0 if dx > 0 else nx + 1) + halo_row(-dy)
                    buf[f, pl.ds(row, 1), :] = self.cr[self.corner, k, pl.ds(f - self.low, 1), :]
                    return carry
                lax.fori_loop(self.low, self.high, body, 0)

            for way, step in ((0, 1), (1, -1)):
                pl.when(exists(0, -step))(functools.partial(rows, way, step))
            for k, (dx, dy) in enumerate(WAYS[4:]):
                pl.when(exists(-dx, -dy))(functools.partial(corner, k, dx, dy))

        def finish(self):
            for k, (dx, dy) in enumerate(WAYS):
                pl.when(exists(dx, dy))(self.copies[k].wait_send)

    class Depth:
        def __init__(self, number, zs, zl, zr, buf, plane):
            self.zl, self.zr, self.buf, self.plane = zl, zr, buf, plane
            self.copies = [
                pltpu.make_async_remote_copy(
                    src_ref=zs, dst_ref=landing,
                    send_sem=z_send.at[number, way], recv_sem=z_recv.at[number, way],
                    device_id={"gz": moved("gz", step)}, device_id_type=MESH,
                )
                for way, (landing, step) in enumerate(((zl, 1), (zr, -1)))
            ]

        def start(self):
            pl.when(above_z)(self.copies[0].start)
            pl.when(below_z)(self.copies[1].start)

        def receive(self):
            pl.when(below_z)(self.copies[0].wait_recv)
            pl.when(above_z)(self.copies[1].wait_recv)
            zero = jnp.zeros((TILE, LANES), self.buf.dtype)

            def place(x, carry):
                for k in range(tiles):
                    row, at = own_tile(x, k)
                    low = jnp.where(below_z, pltpu.roll(self.zl[pl.ds(at, TILE), :], 1, 1), zero)
                    high = jnp.where(above_z, pltpu.roll(self.zr[pl.ds(at, TILE), :], LANES - 1, 1), zero)
                    self.buf[self.plane, pl.ds(row, TILE), :] = jnp.where(odd, low, high)
                return carry

            lax.fori_loop(0, nx, place, 0, unroll=8)

        def finish(self):
            pl.when(above_z)(self.copies[0].wait_send)
            pl.when(below_z)(self.copies[1].wait_send)

    class Faces:
        def __init__(self, number, buf, n, start, step, landing, xs=None, dz=0):
            self.dz = dz
            self.buf, self.n, self.first_row, self.step, self.xs = buf, n, start, step, xs
            self.xr, self.ys, self.yr, self.cs, self.cr = landing
            self.copies = []
            for k, (dx, dy) in enumerate(WAYS):
                way = 0 if dx + dy > 0 else 1
                if dy == 0:
                    if xs is None:
                        source = buf.at[pl.ds(0, n), pl.ds(start + (nx - 1 if dx > 0 else 0) * step, ny), :]
                    else:
                        source = xs.at[way]
                    target = self.xr.at[way, pl.ds(0, n), pl.ds(TILE, ny), :]
                elif dx == 0:
                    source, target = self.ys.at[way], self.yr.at[way, pl.ds(0, n), pl.ds(TILE, nx), :]
                else:
                    source, target = self.cs.at[k - 4], self.cr.at[k - 4]
                self.copies.append(
                    pltpu.make_async_remote_copy(
                        src_ref=source, dst_ref=target,
                        send_sem=send.at[number, k], recv_sem=recv.at[number, k],
                        device_id={"gx": moved("gx", dx), "gy": moved("gy", dy), "gz": moved("gz", dz)}, device_id_type=MESH,
                    )
                )

        def there(self, dx, dy):
            if self.dz == 0:
                return exists(dx, dy)
            return jnp.logical_and(exists(dx, dy), above_z if self.dz > 0 else below_z)

        def incoming(self, dx, dy):
            if self.dz == 0:
                return exists(-dx, -dy)
            return jnp.logical_and(exists(-dx, -dy), below_z if self.dz > 0 else above_z)

        def land(self):
            for k, (dx, dy) in enumerate(WAYS):
                pl.when(self.incoming(dx, dy))(self.copies[k].wait_recv)

        def blank(self):
            zeros = jnp.zeros((TILE, LANES), jnp.float32)

            def borders(f, carry):
                for way in range(2):
                    for at in (0, TILE + ny):
                        self.xr[way, f, pl.ds(at, TILE), :] = zeros
                    for at in (0, TILE + nx):
                        self.yr[way, f, pl.ds(at, TILE), :] = zeros
                return carry

            lax.fori_loop(0, self.n, borders, 0)

            def clear(ref, way, extent):
                def body(f, carry):
                    ref[way, f, pl.ds(TILE, extent), :] = jnp.zeros((extent, LANES), jnp.float32)
                    return carry
                lax.fori_loop(0, self.n, body, 0)

            for way, step in ((0, 1), (1, -1)):
                pl.when(jnp.logical_not(exists(-step, 0)))(functools.partial(clear, self.xr, way, ny))
                pl.when(jnp.logical_not(exists(0, -step)))(functools.partial(clear, self.yr, way, nx))

        def collect(self):
            buf, step = self.buf, self.step

            def gather(f, carry):
                for x in range(0, nx, TILE):
                    for way, toward in ((0, 1), (1, -1)):
                        row = self.first_row + x * step + edge_row(toward)
                        self.ys[way, f, pl.ds(x, TILE), :] = buf[f, pl.ds(row, TILE, stride=step), :]
                for k, (dx, dy) in enumerate(WAYS[4:]):
                    row = self.first_row + (nx - 1 if dx > 0 else 0) * step + edge_row(dy)
                    self.cs[k, pl.ds(f, 1), :] = buf[f, pl.ds(row, 1), :]
                return carry

            lax.fori_loop(0, self.n, gather, 0)

        def launch(self):
            for k in (4, 5, 6, 7, 0, 1, 2, 3):
                pl.when(self.there(*WAYS[k]))(self.copies[k].start)

        def start_filled(self):
            def corners(f, carry):
                for k, (dx, dy) in enumerate(WAYS[4:]):
                    self.cs[k, pl.ds(f, 1), :] = self.xs[0 if dx > 0 else 1, f, pl.ds(edge_row(dy), 1), :]
                return carry

            lax.fori_loop(0, self.n, corners, 0)
            for k in (4, 5, 6, 7, 0, 1, 2, 3):
                pl.when(exists(*WAYS[k]))(self.copies[k].start)

        def receive(self):
            for k, (dx, dy) in enumerate(WAYS):
                pl.when(exists(-dx, -dy))(self.copies[k].wait_recv)

            def corner(k, dx, dy):
                way = 0 if dy > 0 else 1
                at = TILE - 1 if dx > 0 else TILE + nx

                def body(f, carry):
                    self.yr[way, f, pl.ds(at, 1), :] = self.cr[k, pl.ds(f, 1), :]
                    return carry
                lax.fori_loop(0, self.n, body, 0)

            for k, (dx, dy) in enumerate(WAYS[4:]):
                pl.when(exists(-dx, -dy))(functools.partial(corner, k, dx, dy))

        def finish(self):
            for k, (dx, dy) in enumerate(WAYS):
                pl.when(self.there(dx, dy))(self.copies[k].wait_send)

    def pad_zeros(buf, n):
        zeros = jnp.zeros((TILE, LANES), jnp.float32)

        def body(f, carry):
            for p in range(nx + 3):
                buf[f, pl.ds(p * pitch, TILE), :] = zeros
            for p in (0, nx + 1):
                for k in range(tiles):
                    buf[f, pl.ds(first(p) + k * TILE, TILE), :] = zeros
            return carry

        lax.fori_loop(0, n, body, 0)

    code_z = Depth(0, edge.at[0], zl_i, zr_i, codes, 1)
    code_own = Unit(0, codes, 0, 1, ys_i, yr_i, cs_i, cr_i, 0)
    code_up = Faces(1, edge, 1, 0, ny, (xr_c.at[0], ys_c, yr_c.at[0], cs_c, cr_c.at[0]), None, 1)
    code_down = Faces(8, edge, 1, 0, ny, (xr_c.at[1], ys_c, yr_c.at[1], cs_c, cr_c.at[1]), None, -1)
    raw_z = Depth(1, zs_f.at[0], zl_f.at[0], zr_f.at[0], packed, 0)
    raw_all = Faces(2, raw, fields, 0, ny, (xr_r, ys_r, yr_r, cs_r, cr_r))
    raw_packed = Unit(3, packed, 0, 1, ys_p, yr_p, cs_p, cr_p, 0)
    w_z = Depth(2, zs_f.at[1], zl_f.at[1], zr_f.at[1], packed, 1)
    w_all = Faces(4, weights, 1, 0, ny, (xr_w, ys_w, yr_w, cs_w, cr_w))
    w_packed = Unit(5, packed, 1, 2, ys_p, yr_p, cs_p, cr_p, 1)
    q_z = Depth(3, zs_f.at[2], zl_f.at[2], zr_f.at[2], packed, 2)
    q_all = Faces(6, qbuf, nspec, first(1), pitch, (xr_q, ys_q, yr_q, cs_q, cr_q), xs_q)
    q_packed = Unit(7, packed, 2, 3, ys_p, yr_p, cs_p, cr_p, 2)
    everything = [
        code_z, code_own, raw_z, raw_all, raw_packed, w_z, w_all, w_packed, q_z, q_all, q_packed,
    ]

    def join_code_ends():
        code_up.land()
        code_down.land()
        zero = jnp.zeros((TILE, LANES), jnp.int32)

        def mixed(low, high):
            low = jnp.where(below_z, pltpu.roll(low, 1, 1), zero)
            high = jnp.where(above_z, pltpu.roll(high, LANES - 1, 1), zero)
            return jnp.where(odd, low, high)

        def plane(way, step):
            for k in range(tiles):
                near = pl.ds(TILE + k * TILE, TILE)
                row = first(0 if step > 0 else nx + 1) + k * TILE
                codes[1, pl.ds(row, TILE), :] = mixed(xr_c[0, way, 0, near, :], xr_c[1, way, 0, near, :])

        def rows(way, step):
            for x in range(0, nx, TILE):
                near = pl.ds(TILE + x, TILE)
                row = first(x + 1) + halo_row(-step)
                codes[1, pl.ds(row, TILE, stride=pitch), :] = mixed(yr_c[0, way, 0, near, :], yr_c[1, way, 0, near, :])

        def corner(k, dx, dy):
            row = first(0 if dx > 0 else nx + 1) + halo_row(-dy)
            codes[1, pl.ds(row, 1), :] = mixed(cr_c[0, k], cr_c[1, k])[:1]

        for way, step in ((0, 1), (1, -1)):
            pl.when(exists(-step, 0))(functools.partial(plane, way, step))
            pl.when(exists(0, -step))(functools.partial(rows, way, step))
        for k, (dx, dy) in enumerate(WAYS[4:]):
            pl.when(exists(-dx, -dy))(functools.partial(corner, k, dx, dy))

    def total_over(value):
        for number, axis in enumerate(AXES):
            n, me = size[axis], here[axis]
            peers[number, me] = value
            copies = [
                pltpu.make_async_remote_copy(
                    src_ref=peers.at[number, me], dst_ref=peers.at[number, me],
                    send_sem=peer_send.at[number, k], recv_sem=peer_recv.at[number, k],
                    device_id={axis: lax.rem(me + k, n)}, device_id_type=MESH,
                )
                for k in range(1, n)
            ]
            for copy in copies:
                copy.start()
            yield
            for copy in copies:
                copy.wait()
            value = peers[number, 0]
            for k in range(1, n):
                value = value + peers[number, k]
        sums = jnp.broadcast_to(jnp.sum(value, axis=1, keepdims=True) * scale, value.shape)
        places = lax.broadcasted_iota(jnp.int32, value.shape, 1) == lax.broadcasted_iota(jnp.int32, value.shape, 0)
        change[...] = jnp.sum(jnp.where(places, sums, 0.0), axis=0)[:nspec]

    def fractions(own):
        is_cut = flag[own, :] == 1
        volume = jnp.where(is_cut, vol[own, :], 256).astype(jnp.float32) * (1.0 / 256.0)
        face = jnp.where(is_cut, area[own, :], 256).astype(jnp.float32) * (1.0 / 256.0)
        return volume, face

    def fill(x, carry):
        for k in range(tiles):
            row, at = own_tile(x, k)
            own = pl.ds(at, TILE)
            value = jnp.where(flag[own, :] == 1, code[own, :] | CENTER, CENTER)
            codes[0, pl.ds(row, TILE), :] = value
            low = jnp.broadcast_to(value[:, :1], (TILE, LANES))
            high = lax.shift_right_logical(jnp.broadcast_to(value[:, LANES - 1:], (TILE, LANES)), 2)
            edge[0, own, :] = jnp.where(odd, low, high)
        return carry

    def shift(x, carry):
        for k in range(tiles):
            row, at = own_tile(x, k)
            own = pl.ds(at, TILE)
            value = codes[0, pl.ds(row, TILE), :]
            shifted[0, own, :] = jnp.where(first_lane, 0, pltpu.roll(value, 1, 1))
            shifted[1, own, :] = jnp.where(last_lane, 0, pltpu.roll(value, LANES - 1, 1))
        return carry

    def prepare(x, totals):
        for k in range(tiles):
            _, at = own_tile(x, k)
            own = pl.ds(at, TILE)
            volume, face = fractions(own)
            volumes[own, :] = volume
            raw[nspec, own, :] = face
            totals = tuple(totals[s] + volume * raw[s, own, :] for s in range(nspec))
        return totals

    def raw_pack(x, carry):
        for k in range(tiles):
            _, at = own_tile(x, k)
            own = pl.ds(at, TILE)
            zs_f[0, own, :] = pack([raw[f, own, :] for f in range(fields)], 0)
        return carry

    def masked_sums(taps, low, high):
        zero = jnp.zeros((TILE, LANES), jnp.float32)
        sums = [[None] * (high - low) for _ in range(3)]
        for sources, position, value_of in taps:
            present = [
                None if source is None else (source & (1 << (position + k))) != 0 for k, source in enumerate(sources)
            ]
            for f in range(low, high):
                value = value_of(f)
                for k in range(3):
                    term = value if present[k] is None else jnp.where(present[k], value, zero)
                    old = sums[k][f - low]
                    sums[k][f - low] = term if old is None else old + term
        return sums

    def keep_sums(slot, sums, low):
        for m in range(3):
            for f, value in enumerate(sums[m]):
                parts_f[slot, m, low + f] = value

    def merged(slot, f, wrap):
        if wrap:
            up, down = pltpu.roll(parts_f[slot, 2, f], 1, 1), pltpu.roll(parts_f[slot, 0, f], LANES - 1, 1)
            up, down = jnp.where(first_lane, 0.0, up), jnp.where(last_lane, 0.0, down)
        else:
            up, down = pltpu.roll(parts_f[slot, 2, f], LANES - 1, 1), pltpu.roll(parts_f[slot, 0, f], 1, 1)
        return parts_f[slot, 1, f] + up + down

    def packed_taps(row, step, source, value_of):
        zero = jnp.zeros((TILE, LANES), jnp.float32)
        total = None
        row = row - (pitch + TILE)
        for a, b, position in BLOCK:
            near = pl.ds(row + (pitch + TILE + step * (a * pitch + b)), TILE)
            term = jnp.where((source(near) & (1 << position)) != 0, value_of(near), zero)
            total = term if total is None else total + term
        return total

    def pack(values, lowest):
        packed = jnp.zeros((TILE, LANES), jnp.float32)
        for k, value in enumerate(values):
            f = lowest + k
            packed = jnp.where((lane == 2 * f) | (lane == 2 * f + 1), pltpu.roll(value, 2 * f + 1, 1), packed)
        return packed

    quad = 4
    members = [(k, k // tiles, k % tiles) for k in range(quad * tiles)]

    def count_taps(g):
        for k, x, y in members:
            row, at = own_tile(g * quad + x, y)
            sums = [None] * 3
            total = None
            row = row - (pitch + TILE)
            for a, b, position in BLOCK:
                near = pl.ds(row + (pitch + TILE - a * pitch - b), TILE)
                value = codes[0, near, :]
                value = value if position == 0 else lax.shift_right_logical(value, position)
                for m in range(3):
                    term = value & (1 << m)
                    sums[m] = term if sums[m] is None else sums[m] + term
                value = codes[1, near, :]
                value = value if position == 0 else lax.shift_right_logical(value, position)
                total = value & 1 if total is None else total + (value & 1)
            for m in range(3):
                parts_i[k, m] = sums[m]
            parts_i[k, 3] = total

    def weigh(g):
        for k, x, y in members:
            row, at = own_tile(g * quad + x, y)
            own = pl.ds(at, TILE)
            from_end = pltpu.roll(parts_i[k, 3], LANES - 1, 1)
            from_left = pltpu.roll(lax.shift_right_logical(parts_i[k, 2], 2), 1, 1)
            from_right = pltpu.roll(parts_i[k, 0], LANES - 1, 1)
            counted = lax.shift_right_logical(parts_i[k, 1], 1)
            counted = counted + jnp.where(first_lane, from_end, from_left) + jnp.where(last_lane, from_end, from_right)
            share = 1.0 / counted.astype(jnp.float32)
            scaling[own, :] = raw[nspec, own, :] * share
            weight = volumes[own, :] * share
            weights[0, own, :] = weight
            for f in range(fields):
                wbuf[f, pl.ds(row, TILE), :] = weight * raw[f, own, :]

    def weigh_pack(g):
        for k, x, y in members:
            row, at = own_tile(g * quad + x, y)
            own = pl.ds(at, TILE)
            value = weights[0, own, :]
            low = jnp.broadcast_to(value[:, :1], (TILE, LANES))
            high = jnp.broadcast_to(value[:, LANES - 1:], (TILE, LANES))
            zs_f[1, own, :] = jnp.where(odd, low, high)

    def own_row(t):
        x, k = lax.div(t, tiles), lax.rem(t, tiles)
        row = (TILE + pitch) + x * pitch + k * TILE
        if isinstance(t, int):
            return int(row), t * TILE
        return pl.multiple_of(row, TILE), pl.multiple_of(t * TILE, TILE)

    def reader(buf, near):
        return lambda f: buf[f, near, :]

    def weighed(buf, factors, near):
        factor = factors[0, near, :]
        return lambda f: buf[f, near, :] * factor

    def gather_main(t):
        row, at = own_tile(t // tiles, t % tiles) if isinstance(t, int) else own_row(t)
        own = pl.ds(at, TILE)
        right, left, middle = shifted[0, own, :], shifted[1, own, :], codes[0, pl.ds(row, TILE), :]
        taps = []
        base = row - (pitch + TILE)
        for a, b, position in BLOCK:
            center = None if position == 12 else middle
            near = pl.ds(base + (pitch + TILE + a * pitch + b), TILE)
            taps.append(((left, center, right), position, reader(wbuf, near)))
        keep_sums(0, masked_sums(taps, 0, fields), 0)

    def gather_close(t):
        row, at = own_tile(t // tiles, t % tiles) if isinstance(t, int) else own_row(t)
        for f in range(nspec):
            qbuf[f, pl.ds(row, TILE), :] = merged(0, f, False)
        gathered[pl.ds(at, TILE), :] = merged(0, flux, False)

    def gather_strip(j):
        x = j * TILE
        for way, (b, y) in enumerate(((-1, 0), (1, ny - 1))):
            where = pl.ds(x * ny + y, TILE, stride=ny)
            right, left = shifted[0, where, :], shifted[1, where, :]
            middle = codes[0, pl.ds(first(1) + x * pitch + y, TILE, stride=pitch), :]
            taps = []
            for a in (-1, 0, 1):
                near = pl.ds(TILE + x + a, TILE)
                taps.append(((left, middle, right), 9 * (a + 1) + 3 * (b + 1), weighed(yr_r.at[way], yr_w.at[way], near)))
            keep_sums(way, masked_sums(taps, 0, fields), 0)

    def gather_strip_close(j):
        x = j * TILE
        for way, y in enumerate((0, ny - 1)):
            rows = pl.ds(first(1) + x * pitch + y, TILE, stride=pitch)
            for f in range(nspec):
                qbuf[f, rows, :] = qbuf[f, rows, :] + merged(way, f, False)
            where = pl.ds(x * ny + y, TILE, stride=ny)
            gathered[where, :] = gathered[where, :] + merged(way, flux, False)

    def gather_plane(way):
        a, x = ((-1, 0), (1, nx - 1))[way]
        for k in range(tiles):
            row, at = own_tile(x, k)
            own = pl.ds(at, TILE)
            right, left, middle = shifted[0, own, :], shifted[1, own, :], codes[0, pl.ds(row, TILE), :]
            taps = []
            for b in (-1, 0, 1):
                near = pl.ds(TILE + k * TILE + b, TILE)
                taps.append(((left, middle, right), 9 * (a + 1) + 3 * (b + 1), weighed(xr_r.at[way], xr_w.at[way], near)))
            keep_sums(way * tiles + k, masked_sums(taps, 0, fields), 0)

    def gather_plane_close(way):
        x = (0, nx - 1)[way]
        for k in range(tiles):
            row, at = own_tile(x, k)
            for f in range(nspec):
                qbuf[f, pl.ds(row, TILE), :] = qbuf[f, pl.ds(row, TILE), :] + merged(way * tiles + k, f, False)
            own = pl.ds(at, TILE)
            gathered[own, :] = gathered[own, :] + merged(way * tiles + k, flux, False)

    def edge_tiles():
        for way, y in enumerate((ny - 1, 0)):
            for x in range(0, nx, TILE):
                row = first(x + 1) + y
                yield (
                    lambda start: pl.ds(start, TILE, stride=pitch), row,
                    pl.ds(x * ny + y, TILE, stride=ny), ys_q.at[way], pl.ds(x, TILE),
                )
        for way, x in enumerate((nx - 1, 0)):
            for k in range(tiles):
                row, at = own_tile(x, k)
                yield lambda start: pl.ds(start, TILE), row, pl.ds(at, TILE), xs_q.at[way], pl.ds(k * TILE, TILE)

    def edge_ends():
        zero = jnp.zeros((TILE, LANES), jnp.float32)
        for n, (rows, row, own, _, _) in enumerate(edge_tiles()):
            bits = edge[0, own, :]
            total = None
            for a, b, position in BLOCK:
                near = rows(row + a * pitch + b)
                term = jnp.where((bits & (1 << position)) != 0, packed[0, near, :] * packed[1, near, :], zero)
                total = term if total is None else total + term
            parts_e[n] = total

    def edge_quotas():
        for n, (rows, row, own, ref, where) in enumerate(edge_tiles()):
            value = parts_e[n]

            def spread(f):
                return jnp.where(both_ends, pltpu.roll(value, LANES - 1 - 2 * f, 1), 0.0)

            inverted = 1.0 / (gathered[own, :] + spread(flux))
            for f in range(nspec):
                ref[f, where, :] = (qbuf[f, rows(row), :] + spread(f)) * inverted

    def gather_ends(g):
        for k, x, y in members:
            row, at = own_tile(g * quad + x, y)
            value = edge[0, pl.ds(at, TILE), :]
            parts_e[k] = packed_taps(
                row, 1, lambda near: value, lambda near: packed[0, near, :] * packed[1, near, :])

    def quotas(g):
        for k, x, y in members:
            row, at = own_tile(g * quad + x, y)
            value = parts_e[k]

            def spread(f):
                return jnp.where(both_ends, pltpu.roll(value, LANES - 1 - 2 * f, 1), 0.0)

            inverted = 1.0 / (gathered[pl.ds(at, TILE), :] + spread(flux))
            for f in range(nspec):
                qbuf[f, pl.ds(row, TILE), :] = (qbuf[f, pl.ds(row, TILE), :] + spread(f)) * inverted

    def quota_pack(g):
        for k, x, y in members:
            row, at = own_tile(g * quad + x, y)
            zs_f[2, pl.ds(at, TILE), :] = pack([qbuf[f, pl.ds(row, TILE), :] for f in range(nspec)], 0)

    def scatter_main(t):
        row, at = own_tile(t // tiles, t % tiles) if isinstance(t, int) else own_row(t)
        row = row - (pitch + TILE)
        taps = []
        for a, b, position in BLOCK:
            near = pl.ds(row + (pitch + TILE - a * pitch - b), TILE)
            source = codes[0, near, :]
            center = None if position == 12 else source
            taps.append(((source, center, source), position, reader(qbuf, near)))
        keep_sums(0, masked_sums(taps, 0, nspec), 0)

    def scatter_close(t):
        row, at = own_tile(t // tiles, t % tiles) if isinstance(t, int) else own_row(t)
        for f in range(nspec):
            wbuf[f, pl.ds(row, TILE), :] = merged(0, f, True)

    def scatter_strip(j):
        x = j * TILE
        for way, (b, y) in enumerate(((1, -1), (-1, ny))):
            taps = []
            for a in (-1, 0, 1):
                source = codes[0, pl.ds(first(1) + (x - a) * pitch + y, TILE, stride=pitch), :]
                taps.append(((source, source, source), 9 * (a + 1) + 3 * (b + 1), reader(yr_q.at[way], pl.ds(TILE + x - a, TILE))))
            keep_sums(way, masked_sums(taps, 0, nspec), 0)

    def scatter_strip_close(j):
        for way, y in enumerate((0, ny - 1)):
            where = pl.ds(first(1) + j * TILE * pitch + y, TILE, stride=pitch)
            for f in range(nspec):
                wbuf[f, where, :] = wbuf[f, where, :] + merged(way, f, True)

    def scatter_plane(way):
        a, x = ((1, 0), (-1, nx + 1))[way]
        for k in range(tiles):
            taps = []
            for b in (-1, 0, 1):
                source = codes[0, pl.ds(first(x) + k * TILE - b, TILE), :]
                taps.append(((source, source, source), 9 * (a + 1) + 3 * (b + 1), reader(xr_q.at[way], pl.ds(TILE + k * TILE - b, TILE))))
            keep_sums(way * tiles + k, masked_sums(taps, 0, nspec), 0)

    def scatter_plane_close(way):
        x = (0, nx - 1)[way]
        for k in range(tiles):
            row, at = own_tile(x, k)
            for f in range(nspec):
                wbuf[f, pl.ds(row, TILE), :] = wbuf[f, pl.ds(row, TILE), :] + merged(way * tiles + k, f, True)

    def scatter_ends(g):
        for k, x, y in members:
            row, at = own_tile(g * quad + x, y)
            parts_e[k] = packed_taps(row, -1, lambda near: codes[1, near, :], lambda near: packed[2, near, :])

    def finals(g):
        for k, x, y in members:
            row, at = own_tile(g * quad + x, y)
            own = pl.ds(at, TILE)
            value, factor = parts_e[k], scaling[own, :]
            for f in range(nspec):
                spread = jnp.where(both_ends, pltpu.roll(value, LANES - 1 - 2 * f, 1), 0.0)
                out[f, own, :] = factor * (wbuf[f, pl.ds(row, TILE), :] + spread)

    blank(codes, 0, 2)
    loads[0].wait()
    loads[1].wait()
    lax.fori_loop(0, nx, fill, 0, unroll=8)
    pl.semaphore_wait(barrier, greeted)
    code_z.start()
    code_own.start()
    code_up.collect()
    code_up.launch()
    code_down.launch()
    for copy in loads[2:]:
        copy.wait()
    totals = tuple(jnp.zeros((TILE, LANES), jnp.float32) for _ in range(nspec))
    totals = lax.fori_loop(0, nx, prepare, totals, unroll=2)
    local = jnp.concatenate(
        [jnp.sum(total, axis=0, keepdims=True) for total in totals]
        + [jnp.zeros((peers.shape[2] - nspec, LANES), jnp.float32)],
        axis=0,
    )
    reduction = total_over(local)
    raw_all.collect()
    raw_all.launch()
    lax.fori_loop(0, nx, raw_pack, 0, unroll=4)
    raw_z.start()
    lax.fori_loop(0, nx, shift, 0, unroll=8)
    blank(packed, 0, 3)
    raw_all.blank()
    w_all.blank()
    q_all.blank()
    pad_zeros(wbuf, fields)
    pad_zeros(qbuf, nspec)
    raw_z.receive()
    raw_packed.start()
    code_z.receive()
    code_own.receive()
    join_code_ends()
    pipelined([count_taps, weigh, weigh_pack], nx // quad)
    w_z.start()
    w_all.collect()
    w_all.launch()

    def relay_w():
        w_z.receive()
        w_packed.start()

    pipelined([gather_main, gather_close], nx * tiles, (nx * tiles // 4, relay_w))
    raw_all.receive()
    w_all.receive()
    next(reduction)
    pipelined([gather_strip, gather_strip_close], nx // TILE)
    for stage in (gather_plane, gather_plane_close):
        stage(0)
        stage(1)
    raw_packed.receive()
    w_packed.receive()
    edge_ends()
    edge_quotas()
    q_all.start_filled()
    pipelined([gather_ends, quotas, quota_pack], nx // quad)
    q_z.start()

    def relay_q():
        q_z.receive()
        q_packed.start()
        next(reduction)

    pipelined([scatter_main, scatter_close], nx * tiles, (nx * tiles // 5, relay_q))
    q_all.receive()
    next(reduction)
    pipelined([scatter_strip, scatter_strip_close], nx // TILE)
    for stage in (scatter_plane, scatter_plane_close):
        stage(0)
        stage(1)
    q_packed.receive()
    pipelined([scatter_ends, finals], nx // quad)
    next(reduction, None)
    flat = [part for part in everything if not isinstance(part, Depth)]
    deep = [part for part in everything if isinstance(part, Depth)]

    def drain(copies):
        for copy in copies:
            copy.wait_send()

    for k, (dx, dy) in enumerate(WAYS):
        pl.when(exists(dx, dy))(functools.partial(drain, [part.copies[k] for part in flat]))
    code_up.finish()
    code_down.finish()
    pl.when(above_z)(functools.partial(drain, [part.copies[0] for part in deep]))
    pl.when(below_z)(functools.partial(drain, [part.copies[1] for part in deep]))


def per_device(provisional, cut_flag, cut_code, volume_level, area_level):
    nspec, nx, ny, nz = provisional.shape
    assert nz == LANES and ny % TILE == 0 and nx % TILE == 0
    own = nx * ny
    tiles = ny // TILE
    rows = 2 * TILE + (nx + 2) * (ny + TILE)
    most = max(lax.axis_size(axis) for axis in AXES)
    cells = own * nz * math.prod(lax.axis_size(axis) for axis in AXES)
    fields = nspec + 1
    f32, i32 = jnp.float32, jnp.int32
    vmem = pl.BlockSpec(memory_space=pltpu.VMEM)
    hbm = pl.BlockSpec(memory_space=pltpu.HBM)
    shapes = [
        ((fields, own, nz), f32), ((own, nz), i32), ((own, nz), i32), ((own, nz), i32), ((own, nz), i32),
        ((2, rows, nz), i32), ((fields, rows, nz), f32), ((nspec, rows, nz), f32), ((3, rows, nz), f32),
        ((2, own, nz), i32), ((1, own, nz), i32),
        ((own, nz), i32), ((own, nz), i32),
        ((3, own, nz), f32), ((3, own, nz), f32), ((3, own, nz), f32),
        ((2, 2, nx, nz), i32), ((2, 2, nx, nz), i32), ((2, 4, TILE, nz), i32), ((2, 4, TILE, nz), i32),
        ((2, 3, nx, nz), f32), ((2, 3, nx, nz), f32), ((3, 4, TILE, nz), f32), ((3, 4, TILE, nz), f32),
    ]
    for n in (fields, 1, nspec):
        high = -(-n // TILE) * TILE
        shapes += [
            ((2, n, ny + 2 * TILE, nz), f32), ((2, n, nx, nz), f32), ((2, n, nx + 2 * TILE, nz), f32),
            ((4, high, nz), f32), ((4, high, nz), f32),
        ]
    high = -(-nspec // TILE) * TILE
    shapes += [
        ((2, nspec, ny, nz), f32),
        ((2, 2, 1, ny + 2 * TILE, nz), i32), ((2, 1, nx, nz), i32), ((2, 2, 1, nx + 2 * TILE, nz), i32),
        ((4, TILE, nz), i32), ((2, 4, TILE, nz), i32),
        ((own, nz), f32), ((1, own, nz), f32), ((own, nz), f32), ((own, nz), f32),
        ((4 * tiles, 4, TILE, nz), i32), ((2 * tiles, 3, fields, TILE, nz), f32), ((max(4 * tiles, 2 * (tiles + nx // TILE)), TILE, nz), f32),
        ((3, most, high, nz), f32),
    ]
    dma = pltpu.SemaphoreType.DMA
    out, change = pl.pallas_call(
        functools.partial(kernel, nx, ny, 1.0 / math.sqrt(cells)),
        out_shape=(
            jax.ShapeDtypeStruct((nspec, own, nz), f32),
            jax.ShapeDtypeStruct((nspec,), f32),
        ),
        in_specs=[hbm] * 5,
        out_specs=(vmem, vmem),
        scratch_shapes=[pltpu.VMEM(shape, kind) for shape, kind in shapes]
        + [
            dma((5,)), dma((4, 2)), dma((4, 2)), dma((9, 8)), dma((9, 8)), dma((3, most)), dma((3, most)),
        ],
        compiler_params=pltpu.CompilerParams(
            collective_id=0, has_side_effects=True, vmem_limit_bytes=26 * 1024 * 1024
        ),
    )(
        *[pltpu.with_memory_space_constraint(x, pltpu.HBM) for x in (
        provisional.reshape(nspec, own, nz),
        cut_flag.reshape(own, nz),
        cut_code.reshape(own, nz),
        volume_level.reshape(own, nz),
        area_level.reshape(own, nz))]
    )
    return out.reshape(provisional.shape), change


def solution(mesh):
    spec = P("gx", "gy", "gz")
    wide = P(None, "gx", "gy", "gz")
    return jax.shard_map(
        per_device, mesh=mesh, in_specs=(wide, spec, spec, spec, spec), out_specs=(wide, P()), check_vma=False
    )
```
